16 devices in a mesh: dp: 2 (over z), tp: 8 (over y, x, core).
Axes of the slice: x: 2, y: 2, z: 2, core: 2. Of those that a mesh axis runs over, the one named last changes fastest.
Arguments:
- hidden: bfloat16 [2, 4096, 2048], P('dp', 'tp'), parts along dimension 0
- norm_attn: float32 [2, 2048], replicated
- w_q: bfloat16 [2, 2048, 16, 128], P(None, None, 'tp')
- w_kv: bfloat16 [2, 2048, 2, 2, 128], replicated
- w_o: bfloat16 [2, 16, 128, 2048], P(None, 'tp')
- norm_mlp: float32 [2, 2048], replicated
- w_gate: bfloat16 [2, 2048, 11008], P(None, None, 'tp')
- w_up: bfloat16 [2, 2048, 11008], P(None, None, 'tp')
- w_down: bfloat16 [2, 11008, 2048], P(None, 'tp')
Outputs:
- output: bfloat16 [2, 4096, 2048], P('dp', 'tp'), parts along dimension 0
There are 2 independent parts. The reference program is written for one: setup_inputs(seed, part) draws one part's arguments, and reference() takes and returns one part's arrays. A program takes and returns all parts, laid end to end along the dimension named above; an argument that names none is the same for every part.
All inputs are finite; a program needn't handle non-finite values.
Results may differ from the reference program's by a relative error of at most 0.011265.
Values are sent between devices in bfloat16 or wider.
A program may use at most 1 GiB of HBM per device.

```python
import math
import jax
import jax.numpy as jnp
from jax import lax

D = 2048
HEADS = 16
KV_HEADS = 2
HEAD = 128
FF = 11008
BATCH = 1
SEQ = 4096
LAYERS = 2

EPS = 1e-5
ROPE_BASE = 10000.0
GROUP = HEADS // KV_HEADS


def setup_inputs(seed: int = 0, part: int = 0) -> dict:
    root = jax.random.key(seed)
    keys = jax.random.split(root, 9)
    tok_key, scale_key = jax.random.split(jax.random.fold_in(keys[8], part))
    tokens = jax.random.normal(tok_key, (BATCH, SEQ, D), jnp.float32)
    tok_scale = jax.random.uniform(scale_key, (BATCH, SEQ, 1), jnp.float32, 0.5, 2.0)
    hidden = (tokens * tok_scale).astype(jnp.bfloat16)
    qk_gain = math.sqrt(math.sqrt(math.log(max(SEQ / 8.0, 4.0))))
    in_scale = 1.0 / math.sqrt(D)
    out_scale = 1.0 / math.sqrt(HEADS * HEAD)
    ff_scale = 1.0 / math.sqrt(FF)
    norm_attn = 1.0 + 0.3 * jax.random.uniform(keys[0], (LAYERS, D), jnp.float32, -1.0, 1.0)
    w_q = (jax.random.normal(keys[1], (LAYERS, D, HEADS, HEAD), jnp.float32) * (in_scale * qk_gain)).astype(jnp.bfloat16)
    kv_gain = jnp.array([qk_gain, 1.0], jnp.float32).reshape(1, 1, 2, 1, 1)
    w_kv = (jax.random.normal(keys[2], (LAYERS, D, 2, KV_HEADS, HEAD), jnp.float32) * in_scale * kv_gain).astype(jnp.bfloat16)
    w_o = (jax.random.normal(keys[3], (LAYERS, HEADS, HEAD, D), jnp.float32) * out_scale).astype(jnp.bfloat16)
    norm_mlp = 1.0 + 0.3 * jax.random.uniform(keys[4], (LAYERS, D), jnp.float32, -1.0, 1.0)
    w_gate = (jax.random.normal(keys[5], (LAYERS, D, FF), jnp.float32) * in_scale).astype(jnp.bfloat16)
    w_up = (jax.random.normal(keys[6], (LAYERS, D, FF), jnp.float32) * in_scale).astype(jnp.bfloat16)
    w_down = (jax.random.normal(keys[7], (LAYERS, FF, D), jnp.float32) * ff_scale).astype(jnp.bfloat16)
    return {'hidden': hidden, 'norm_attn': norm_attn, 'w_q': w_q, 'w_kv': w_kv, 'w_o': w_o, 'norm_mlp': norm_mlp, 'w_gate': w_gate, 'w_up': w_up, 'w_down': w_down}


def rms_norm(resid, gain):
    mean_sq = jnp.mean(resid * resid, axis=-1, keepdims=True)
    return (resid * lax.rsqrt(mean_sq + EPS) * gain).astype(jnp.bfloat16)


def rope_tables(positions, head_dim):
    half_dim = head_dim // 2
    inv_freq = jnp.power(ROPE_BASE, -2.0 * jnp.arange(half_dim, dtype=jnp.float32) / head_dim)
    angles = positions.astype(jnp.float32)[:, None] * inv_freq[None, :]
    return jnp.cos(angles), jnp.sin(angles)


def apply_rope(proj, cos_t, sin_t):
    half_dim = proj.shape[-1] // 2
    first_half = proj[..., :half_dim]
    second_half = proj[..., half_dim:]
    cos_b = cos_t[:, None, :]
    sin_b = sin_t[:, None, :]
    return jnp.concatenate([first_half * cos_b - second_half * sin_b, second_half * cos_b + first_half * sin_b], axis=-1)


def decoder_layer(resid, layer_w, cos_t, sin_t, causal_mask):
    attn_gain, q_weight, kv_weight, o_weight, mlp_gain, gate_weight, up_weight, down_weight = layer_w
    normed = rms_norm(resid, attn_gain)
    q_proj = jnp.dot(normed, q_weight.reshape(D, HEADS * HEAD), preferred_element_type=jnp.float32).reshape(SEQ, HEADS, HEAD)
    kv_proj = jnp.dot(normed, kv_weight.reshape(D, 2 * KV_HEADS * HEAD), preferred_element_type=jnp.float32).reshape(SEQ, 2, KV_HEADS, HEAD)
    queries = apply_rope(q_proj, cos_t, sin_t).astype(jnp.bfloat16)
    keys = apply_rope(kv_proj[:, 0], cos_t, sin_t).astype(jnp.bfloat16)
    values = kv_proj[:, 1].astype(jnp.bfloat16)
    q_heads = jnp.transpose(queries, (1, 0, 2))
    k_heads = jnp.repeat(jnp.transpose(keys, (1, 0, 2)), GROUP, axis=0)
    v_heads = jnp.repeat(jnp.transpose(values, (1, 0, 2)), GROUP, axis=0)
    inv_sqrt = 1.0 / math.sqrt(HEAD)

    def attend(head_args):
        q_one, k_one, v_one = head_args
        scores = jnp.dot(q_one, k_one.T, preferred_element_type=jnp.float32) * inv_sqrt
        scores = jnp.where(causal_mask, scores, -jnp.inf)
        attn_probs = jax.nn.softmax(scores, axis=-1).astype(jnp.bfloat16)
        return jnp.dot(attn_probs, v_one, preferred_element_type=jnp.float32).astype(jnp.bfloat16)

    context = lax.map(attend, (q_heads, k_heads, v_heads))
    context = jnp.transpose(context, (1, 0, 2)).reshape(SEQ, HEADS * HEAD)
    resid = resid + jnp.dot(context, o_weight.reshape(HEADS * HEAD, D), preferred_element_type=jnp.float32)
    normed = rms_norm(resid, mlp_gain)
    gate_proj = jnp.dot(normed, gate_weight, preferred_element_type=jnp.float32)
    up_proj = jnp.dot(normed, up_weight, preferred_element_type=jnp.float32)
    activated = (jax.nn.silu(gate_proj) * up_proj).astype(jnp.bfloat16)
    return resid + jnp.dot(activated, down_weight, preferred_element_type=jnp.float32)


def reference(hidden, norm_attn, w_q, w_kv, w_o, norm_mlp, w_gate, w_up, w_down):
    positions = jnp.arange(SEQ)
    cos_t, sin_t = rope_tables(positions, HEAD)
    causal_mask = positions[:, None] >= positions[None, :]
    stacked = (norm_attn, w_q, w_kv, w_o, norm_mlp, w_gate, w_up, w_down)

    def one_sequence(seq_tokens):
        def layer_step(resid, layer_w):
            return decoder_layer(resid, layer_w, cos_t, sin_t, causal_mask), None
        final, _ = lax.scan(layer_step, seq_tokens.astype(jnp.float32), stacked)
        return final.astype(jnp.bfloat16)

    return lax.map(one_sequence, hidden)
```

```python
import functools
import math
import jax
import jax.numpy as jnp
from jax import lax
from jax.experimental import pallas as pl
from jax.experimental.pallas import tpu as pltpu
from jax.sharding import PartitionSpec as P

EPS = 1e-5
ROPE_BASE = 10000.0
MESH = pl.DeviceIdType.MESH
VMEM_MAX = 67043328
F32 = jnp.float32
BF16 = jnp.bfloat16


def rms_norm(resid, gain):
    mean_sq = jnp.mean(resid * resid, axis=-1, keepdims=True)
    return (resid * lax.rsqrt(mean_sq + EPS) * gain).astype(BF16)


def rope_tables(positions, head_dim):
    half_dim = head_dim // 2
    inv_freq = jnp.power(ROPE_BASE, -2.0 * jnp.arange(half_dim, dtype=F32) / head_dim)
    angles = positions.astype(F32)[:, None] * inv_freq[None, :]
    return jnp.cos(angles), jnp.sin(angles)


def apply_rope(proj, cos_t, sin_t):
    half_dim = proj.shape[-1] // 2
    first_half = proj[..., :half_dim]
    second_half = proj[..., half_dim:]
    cos_b = cos_t[:, None, :]
    sin_b = sin_t[:, None, :]
    return jnp.concatenate([first_half * cos_b - second_half * sin_b, second_half * cos_b + first_half * sin_b], axis=-1)


def flash_kernel(bq, bk, head_dim, heads, q_ref, k_ref, v_ref, o_ref):
    i = pl.program_id(0)
    scale = math.log2(math.e) / math.sqrt(head_dim)
    rows = lax.broadcasted_iota(jnp.int32, (bq, bk), 0)
    cols = lax.broadcasted_iota(jnp.int32, (bq, bk), 1)
    qs = [q_ref[:, h * head_dim:(h + 1) * head_dim] for h in range(heads)]

    def step(j, carry, masked):
        at = pl.ds(pl.multiple_of(j * bk, bk), bk)
        k_blk = k_ref[at, :]
        v_blk = v_ref[at, :]
        out = []
        for h in range(heads):
            m, l, acc = carry[h]
            s = lax.dot_general(qs[h], k_blk, (((1,), (1,)), ((), ())), preferred_element_type=F32)
            if masked:
                s = jnp.where(i * bq + rows >= j * bk + cols, s, -jnp.inf)
            m_new = jnp.maximum(m, jnp.max(s, axis=-1, keepdims=True))
            p = jnp.exp2((s - m_new) * scale)
            alpha = jnp.exp2((m - m_new) * scale)
            l = l * alpha + jnp.sum(p, axis=-1, keepdims=True)
            acc = acc * alpha + jnp.dot(p.astype(BF16), v_blk, preferred_element_type=F32)
            out.append((m_new, l, acc))
        return tuple(out)

    init = tuple((jnp.full((bq, 1), -jnp.inf, F32), jnp.zeros((bq, 1), F32), jnp.zeros((bq, head_dim), F32)) for _ in range(heads))
    per = bq // bk
    carry = lax.fori_loop(0, i * per, functools.partial(step, masked=False), init)
    for d in range(per):
        carry = step(i * per + d, carry, True)
    for h in range(heads):
        m, l, acc = carry[h]
        o_ref[:, h * head_dim:(h + 1) * head_dim] = (acc / l).astype(BF16)


def flash(q, k, v, heads, head_dim, bq=512, bk=512):
    seq = q.shape[0]
    width = heads * head_dim
    return pl.pallas_call(
        functools.partial(flash_kernel, bq, bk, head_dim, heads),
        grid=(seq // bq,),
        in_specs=[
            pl.BlockSpec((bq, width), lambda i: (i, 0)),
            pl.BlockSpec((seq, head_dim), lambda i: (0, 0)),
            pl.BlockSpec((seq, head_dim), lambda i: (0, 0)),
        ],
        out_specs=pl.BlockSpec((bq, width), lambda i: (i, 0)),
        out_shape=jax.ShapeDtypeStruct((seq, width), BF16),
        compiler_params=pltpu.CompilerParams(dimension_semantics=("arbitrary",)),
        cost_estimate=pl.CostEstimate(flops=2 * seq * seq * width, bytes_accessed=8 * seq * width, transcendentals=seq * seq * heads // 2),
        name="flash",
    )(q, k, v)


def mlp_kernel(layer, r_hbm, gain_ref, wg_hbm, wu_hbm, wd_hbm, out_hbm,
               wg, wu, wd, xbuf, prec, recv, acc, stash, act,
               lsem, sx, sy, ag, fs, fr, ps, pr, rr, ss):
    t = lax.axis_index('tp')
    c = lax.rem(t, 2)
    xx = lax.rem(lax.div(t, 2), 2)
    yy = lax.div(t, 4)
    mate = t + 1 - 2 * c
    dev_x = t + 2 - 4 * xx
    dev_y = t + 4 - 8 * yy
    rows, width = acc.shape
    half = rows // 2
    hid = act.shape[1]
    h0 = pl.ds(0, half)
    h1 = pl.ds(half, half)
    hs = (h0, h1)

    def rcopy(src, dst, ssem, rsem, dev):
        return pltpu.make_async_remote_copy(src_ref=src, dst_ref=dst, send_sem=ssem, recv_sem=rsem,
                                            device_id={'tp': dev}, device_id_type=MESH)

    load_r = pltpu.make_async_copy(r_hbm, acc, lsem.at[0])
    load_g = pltpu.make_async_copy(wg_hbm.at[layer], wg, lsem.at[1])
    load_u = pltpu.make_async_copy(wu_hbm.at[layer], wu, lsem.at[2])
    load_d = pltpu.make_async_copy(wd_hbm.at[layer], wd, lsem.at[3])
    load_r.start()
    load_g.start()
    load_u.start()
    load_d.start()

    barrier = pltpu.get_barrier_semaphore()
    for dev in (mate, dev_x, dev_y):
        pl.semaphore_signal(barrier, inc=1, device_id={'tp': dev}, device_id_type=MESH)

    load_r.wait()
    nb = 64

    @pl.loop(0, rows // nb)
    def _(b):
        at = pl.ds(pl.multiple_of(b * nb, nb), nb)
        r = acc[at, :]
        mean_sq = jnp.mean(r * r, axis=-1, keepdims=True)
        xbuf[0, 0, at, :] = (r * lax.rsqrt(mean_sq + EPS) * gain_ref[...]).astype(BF16)

    pl.semaphore_wait(barrier, 3)

    own = xbuf.at[0, 0]
    send_x = (rcopy(own.at[h0], xbuf.at[1, 0, h0], sx.at[0], ag.at[1, 0], dev_x),
              rcopy(own.at[h1], xbuf.at[2, 0, h1], sx.at[1], ag.at[2, 1], dev_x),
              rcopy(xbuf.at[1, 0, h1], xbuf.at[3, 0, h1], sx.at[2], ag.at[3, 1], dev_x))
    send_y = (rcopy(own.at[h1], xbuf.at[1, 0, h1], sy.at[0], ag.at[1, 1], dev_y),
              rcopy(own.at[h0], xbuf.at[2, 0, h0], sy.at[1], ag.at[2, 0], dev_y),
              rcopy(xbuf.at[1, 0, h0], xbuf.at[3, 0, h0], sy.at[2], ag.at[3, 0], dev_y))
    for k in range(2):
        send_x[k].start()
        send_y[k].start()

    def forward(w):
        return rcopy(xbuf.at[w, 0], xbuf.at[w, 1], fs.at[w], fr.at[w], mate)

    def partial_send(w):
        return rcopy(xbuf.at[w, 1], prec.at[w], ps.at[w], pr.at[w], mate)

    stage = (rcopy(xbuf.at[1, 1, h0], recv.at[0], ss.at[0], rr.at[0], dev_x),
             rcopy(xbuf.at[1, 1, h1], recv.at[1], ss.at[1], rr.at[1], dev_y),
             rcopy(xbuf.at[3, 1, h0], recv.at[2], ss.at[2], rr.at[2], dev_x),
             rcopy(xbuf.at[3, 1, h1], recv.at[3], ss.at[3], rr.at[3], dev_y),
             rcopy(xbuf.at[2, 1, h0], recv.at[4], ss.at[4], rr.at[4], dev_y),
             rcopy(xbuf.at[2, 1, h1], recv.at[5], ss.at[5], rr.at[5], dev_x))

    forward(0).start()
    load_g.wait()
    load_u.wait()
    load_d.wait()

    nc = 256
    n_full = hid // nc
    tail = hid - n_full * nc

    def gate_up(x_at, at):
        g = jnp.dot(x_at[...], wg[:, at], preferred_element_type=F32)
        u = jnp.dot(x_at[...], wu[:, at], preferred_element_type=F32)
        act[:, at] = (g * jax.nn.sigmoid(g) * u).astype(BF16)

    @pl.loop(0, 8)
    def _(s):
        w = lax.div(s, 2)
        rc = 1 - lax.rem(s, 2)

        @pl.when(rc == 1)
        def _():
            @pl.when(w >= 1)
            def _():
                pltpu.make_async_copy(xbuf.at[0, 0, h0], xbuf.at[w, 0, h0], ag.at[w, 0]).wait()
                pltpu.make_async_copy(xbuf.at[0, 0, h1], xbuf.at[w, 0, h1], ag.at[w, 1]).wait()
                forward(w).start()

                @pl.when(w == 1)
                def _():
                    send_x[2].start()
                    send_y[2].start()
            forward(w).wait_recv()

        x_at = xbuf.at[w, rc]

        @pl.loop(0, n_full)
        def _(n):
            gate_up(x_at, pl.ds(pl.multiple_of(n * nc, nc), nc))
        if tail:
            gate_up(x_at, pl.ds(n_full * nc, tail))

        @pl.when(rc == 0)
        def _():
            partial_send(w).wait()

        @pl.loop(0, width // nc)
        def _(n):
            at = pl.ds(pl.multiple_of(n * nc, nc), nc)
            val = jnp.dot(act[...], wd[:, at], preferred_element_type=F32)

            @pl.when(rc == 1)
            def _():
                xbuf[w, 1, :, at] = val.astype(BF16)

            @pl.when(rc == 0)
            def _():
                total = val + prec[w, :, at].astype(F32)

                @pl.when(w == 0)
                def _():
                    acc[:, at] = acc[:, at] + total

                @pl.when(w == 2)
                def _():
                    stash[:, at] = total

                @pl.when(lax.rem(w, 2) == 1)
                def _():
                    xbuf[w, 1, :, at] = total.astype(BF16)

        @pl.when(rc == 1)
        def _():
            partial_send(w).start()

        @pl.when(s == 3)
        def _():
            stage[0].start()
            stage[1].start()

        @pl.when(s == 7)
        def _():
            stage[2].start()
            stage[3].start()

    def add_rows(dst, first, slot):
        @pl.loop(0, half // nb)
        def _(b):
            at = pl.ds(pl.multiple_of(b * nb, nb), nb)
            to = pl.ds(pl.multiple_of(first + b * nb, nb), nb)
            dst[to, :] = dst[to, :] + recv[slot, at, :].astype(F32)

    for k in range(2):
        stage[k].wait_recv()
        add_rows(acc, k * half, k)
    for k in range(2):
        stage[2 + k].wait_recv()

        @pl.loop(0, half // nb)
        def _(b):
            at = pl.ds(pl.multiple_of(b * nb, nb), nb)
            to = pl.ds(pl.multiple_of(k * half + b * nb, nb), nb)
            xbuf[2, 1, to, :] = (stash[to, :] + recv[2 + k, at, :].astype(F32)).astype(BF16)
        stage[4 + k].start()
    outs = []
    for k in range(2):
        stage[4 + k].wait_recv()
        add_rows(acc, k * half, 4 + k)
        outs.append(pltpu.make_async_copy(acc.at[hs[k]], out_hbm.at[hs[k]], lsem.at[k]))
        outs[k].start()
    for copy in send_x + send_y:
        copy.wait_send()
    for w in range(4):
        forward(w).wait_send()
    for copy in stage:
        copy.wait_send()
    for copy in outs:
        copy.wait()


def mlp(layer, resid, gain, w_gate, w_up, w_down):
    rows, width = resid.shape
    hid = w_gate.shape[2]
    half = rows // 2
    any_spec = pl.BlockSpec(memory_space=pl.ANY)
    dma = pltpu.SemaphoreType.DMA
    return pl.pallas_call(
        functools.partial(mlp_kernel, layer),
        out_shape=jax.ShapeDtypeStruct((rows, width), F32),
        in_specs=[any_spec, pl.BlockSpec(memory_space=pltpu.VMEM), any_spec, any_spec, any_spec],
        out_specs=any_spec,
        scratch_shapes=[
            pltpu.VMEM((width, hid), BF16),
            pltpu.VMEM((width, hid), BF16),
            pltpu.VMEM((hid, width), BF16),
            pltpu.VMEM((4, 2, rows, width), BF16),
            pltpu.VMEM((4, rows, width), BF16),
            pltpu.VMEM((6, half, width), BF16),
            pltpu.VMEM((rows, width), F32),
            pltpu.VMEM((rows, width), F32),
            pltpu.VMEM((rows, hid), BF16),
            dma((4,)), dma((3,)), dma((3,)), dma((4, 2)), dma((4,)), dma((4,)), dma((4,)), dma((4,)), dma((6,)), dma((6,)),
        ],
        compiler_params=pltpu.CompilerParams(collective_id=1 + layer, has_side_effects=True, vmem_limit_bytes=VMEM_MAX),
        cost_estimate=pl.CostEstimate(flops=6 * 8 * rows * width * hid, bytes_accessed=6 * width * hid, transcendentals=8 * rows * hid),
        name="mlp" + str(layer),
    )(resid, gain, w_gate, w_up, w_down)


def solution(mesh):
    n_tp = mesh.shape['tp']
    tok_spec = P('dp', 'tp', None)
    in_specs = (tok_spec, P(), P(None, None, 'tp', None), P(), P(None, 'tp', None, None), P(), P(None, None, 'tp'), P(None, None, 'tp'), P(None, 'tp', None))

    def body(hidden, norm_attn, w_q, w_kv, w_o, norm_mlp, w_gate, w_up, w_down):
        n_layers, width, heads, head_dim = w_q.shape
        n_kv = w_kv.shape[3]
        rows = hidden.shape[1]
        seq = rows * n_tp
        kv_head = (lax.axis_index('tp') * n_kv) // n_tp
        cos_t, sin_t = rope_tables(jnp.arange(seq), head_dim)
        resid = hidden[0].astype(F32)
        for layer in range(n_layers):
            o_full = lax.all_gather(w_o[layer], 'tp', axis=0, tiled=True)
            gathered = lax.all_gather(rms_norm(resid, norm_attn[layer]), 'tp', axis=0, tiled=True)
            kv_weight = lax.dynamic_index_in_dim(w_kv[layer], kv_head, axis=2, keepdims=False)
            q_proj = jnp.einsum('sd,dhe->she', gathered, w_q[layer], preferred_element_type=F32)
            kv_proj = jnp.einsum('sd,dce->sce', gathered, kv_weight, preferred_element_type=F32)
            queries = apply_rope(q_proj, cos_t, sin_t).astype(BF16).reshape(seq, heads * head_dim)
            keys = apply_rope(kv_proj[:, :1], cos_t, sin_t).astype(BF16)[:, 0]
            values = kv_proj[:, 1].astype(BF16)
            context = flash(queries, keys, values, heads, head_dim)
            blocks = lax.all_to_all(context.reshape(n_tp, rows, heads * head_dim), 'tp', 0, 0)
            blocks = jnp.transpose(blocks, (1, 0, 2)).reshape(rows, n_tp * heads * head_dim)
            resid = resid + jnp.dot(blocks, o_full.reshape(-1, width), preferred_element_type=F32)
            resid = mlp(layer, resid, norm_mlp[layer][None], w_gate, w_up, w_down)
        return resid.astype(BF16)[None]

    return jax.shard_map(body, mesh=mesh, in_specs=in_specs, out_specs=tok_spec, check_vma=False)
```

```python
import functools
import math
import jax
import jax.numpy as jnp
from jax import lax
from jax.experimental import pallas as pl
from jax.experimental.pallas import tpu as pltpu
from jax.sharding import PartitionSpec as P

EPS = 1e-5
ROPE_BASE = 10000.0
MESH = pl.DeviceIdType.MESH
VMEM_MAX = 67043328
F32 = jnp.float32
BF16 = jnp.bfloat16


def rope_tables(seq, head_dim):
    half_dim = head_dim // 2
    inv_freq = jnp.power(ROPE_BASE, -2.0 * jnp.arange(half_dim, dtype=F32) / head_dim)
    angles = jnp.arange(seq).astype(F32)[:, None] * inv_freq[None, :]
    cos_t, sin_t = jnp.cos(angles), jnp.sin(angles)
    return jnp.concatenate([cos_t, cos_t], axis=1), jnp.concatenate([-sin_t, sin_t], axis=1)


def coords():
    t = lax.axis_index('tp')
    c = lax.rem(t, 2)
    xx = lax.rem(lax.div(t, 2), 2)
    yy = lax.div(t, 4)
    return t, (yy, xx, c), (t + 1 - 2 * c, t + 2 - 4 * xx, t + 4 - 8 * yy)


def rcopy(src, dst, ssem, rsem, dev):
    return pltpu.make_async_remote_copy(src_ref=src, dst_ref=dst, send_sem=ssem, recv_sem=rsem,
                                        device_id={'tp': dev}, device_id_type=MESH)


def greet(devices):
    for dev in devices:
        pl.semaphore_signal(pltpu.get_barrier_semaphore(), inc=1, device_id={'tp': dev}, device_id_type=MESH)


class RowGather:
    def __init__(self, xbuf, sx, sy, ag, fs, fr, partners):
        mate, dev_x, dev_y = partners
        rows = xbuf.shape[2]
        half = rows // 2
        lead = half // 4
        h0, h1 = pl.ds(0, half), pl.ds(half, half)
        own = xbuf.at[0, 0]
        self.xbuf, self.ag, self.fs, self.fr, self.mate = xbuf, ag, fs, fr, mate
        self.halves = (h0, h1)

        def piece(k, sem, dev, first, size, window, slot):
            at = pl.ds(first, size)
            return rcopy(own.at[at], xbuf.at[window, 0, at], sem.at[k], ag.at[window, slot], dev)

        self.first = (piece(0, sx, dev_x, 0, half, 1, 0), piece(0, sy, dev_y, half, half, 1, 1))
        self.lead = (piece(1, sx, dev_x, half, lead, 3, 1), piece(1, sy, dev_y, 0, lead, 3, 0))
        self.rest = (piece(2, sx, dev_x, half + lead, half - lead, 3, 1), piece(2, sy, dev_y, lead, half - lead, 3, 0))
        self.relay = (rcopy(xbuf.at[1, 0, h1], xbuf.at[2, 0, h1], sx.at[3], ag.at[2, 1], dev_x),
                      rcopy(xbuf.at[1, 0, h0], xbuf.at[2, 0, h0], sy.at[3], ag.at[2, 0], dev_y))

    def forward(self, w):
        return rcopy(self.xbuf.at[w, 0], self.xbuf.at[w, 1], self.fs.at[w], self.fr.at[w], self.mate)

    def start(self, norm_half):
        norm_half(0)
        pl.semaphore_wait(pltpu.get_barrier_semaphore(), 3)
        self.first[0].start()
        norm_half(1)
        self.first[1].start()
        self.lead[0].start()
        self.lead[1].start()
        self.forward(0).start()

    def arrive(self, w):
        for k in range(2):
            at = self.halves[k]
            pltpu.make_async_copy(self.xbuf.at[0, 0, at], self.xbuf.at[w, 0, at], self.ag.at[w, k]).wait()

        @pl.when(w == 1)
        def _():
            for copy in self.relay + self.rest:
                copy.start()
        self.forward(w).start()

    def finish(self):
        for copy in self.first + self.lead + self.relay + self.rest:
            copy.wait_send()
        for w in range(4):
            self.forward(w).wait_send()


def gather_sems():
    dma = pltpu.SemaphoreType.DMA
    return [dma((4,)), dma((4,)), dma((4, 2)), dma((4,)), dma((4,))]


def norm_rows(src, gain_ref, dst, first, count):
    nb = 64

    @pl.loop(0, count // nb)
    def _(b):
        at = pl.ds(pl.multiple_of(first + b * nb, nb), nb)
        r = src[at, :].astype(F32)
        mean_sq = jnp.mean(r * r, axis=-1, keepdims=True)
        dst[at, :] = (r * lax.rsqrt(mean_sq + EPS) * gain_ref[...]).astype(BF16)


def qkv_kernel(heads, head_dim, r_ref, gain_ref, w_ref, cos_ref, sin_ref, out_ref, xbuf, sx, sy, ag, fs, fr):
    _, (yy, xx, c), partners = coords()
    rows = xbuf.shape[2]
    half = rows // 2
    greet(partners)
    gather = RowGather(xbuf, sx, sy, ag, fs, fr, partners)
    gather.start(lambda k: norm_rows(r_ref, gain_ref, xbuf.at[0, 0], k * half, half))

    @pl.loop(0, 8)
    def _(s):
        w = lax.div(s, 2)
        rc = lax.rem(s, 2)

        @pl.when((rc == 0) & (w >= 1))
        def _():
            gather.arrive(w)

        @pl.when(rc == 1)
        def _():
            gather.forward(w).wait_recv()
        proj = jnp.dot(xbuf[w, rc], w_ref[...], preferred_element_type=F32)
        core = c + rc - 2 * c * rc
        one = lax.rem(lax.div(w + 1, 2), 2)
        two = lax.div(w, 2)
        for k in range(2):
            flip_x, flip_y = (one, two) if k == 0 else (two, one)
            chip = 2 * (yy + flip_y - 2 * yy * flip_y) + xx + flip_x - 2 * xx * flip_x
            at = pl.ds(pl.multiple_of((chip * 2 + core) * rows + k * half, half), half)
            part = proj[k * half:(k + 1) * half]
            cos_b = cos_ref[at, :]
            sin_b = sin_ref[at, :]
            for h in range(heads + 1):
                cols = slice(h * head_dim, (h + 1) * head_dim)
                z = part[:, cols]
                out_ref[at, cols] = (z * cos_b + pltpu.roll(z, head_dim // 2, 1) * sin_b).astype(BF16)
            cols = slice((heads + 1) * head_dim, (heads + 2) * head_dim)
            out_ref[at, cols] = part[:, cols].astype(BF16)
    gather.finish()


def qkv(layer, resid, gain, w_qkv, cos_t, sin_t, heads, head_dim, n_tp):
    rows, width = resid.shape
    cols = w_qkv.shape[1]
    seq = rows * n_tp
    vmem = pl.BlockSpec(memory_space=pltpu.VMEM)
    return pl.pallas_call(
        functools.partial(qkv_kernel, heads, head_dim),
        out_shape=jax.ShapeDtypeStruct((seq, cols), BF16),
        in_specs=[vmem] * 5,
        out_specs=vmem,
        scratch_shapes=[pltpu.VMEM((4, 2, rows, width), BF16)] + gather_sems(),
        compiler_params=pltpu.CompilerParams(collective_id=1 + layer, has_side_effects=True, vmem_limit_bytes=VMEM_MAX),
        cost_estimate=pl.CostEstimate(flops=2 * seq * width * cols, bytes_accessed=4 * seq * cols, transcendentals=0),
        name="qkv" + str(layer),
    )(resid, gain, w_qkv, cos_t, sin_t)


def attend(qkv_ref, block, bq, bk, heads, head_dim):
    scale = math.log2(math.e) / math.sqrt(head_dim)
    rows = lax.broadcasted_iota(jnp.int32, (bq, bk), 0)
    cols = lax.broadcasted_iota(jnp.int32, (bq, bk), 1)
    q_at = pl.ds(pl.multiple_of(block * bq, bq), bq)
    qs = [qkv_ref[q_at, h * head_dim:(h + 1) * head_dim] for h in range(heads)]

    def step(j, carry, masked):
        at = pl.ds(pl.multiple_of(j * bk, bk), bk)
        k_blk = qkv_ref[at, heads * head_dim:(heads + 1) * head_dim]
        v_blk = qkv_ref[at, (heads + 1) * head_dim:(heads + 2) * head_dim]
        out = []
        for h in range(heads):
            m, l, acc = carry[h]
            s = lax.dot_general(qs[h], k_blk, (((1,), (1,)), ((), ())), preferred_element_type=F32)
            if masked:
                s = jnp.where(block * bq + rows >= j * bk + cols, s, -jnp.inf)
            m_new = jnp.maximum(m, jnp.max(s, axis=-1, keepdims=True))
            p = jnp.exp2((s - m_new) * scale)
            alpha = jnp.exp2((m - m_new) * scale)
            l = l * alpha + jnp.sum(p, axis=-1, keepdims=True)
            acc = acc * alpha + jnp.dot(p.astype(BF16), v_blk, preferred_element_type=F32)
            out.append((m_new, l, acc))
        return tuple(out)

    init = tuple((jnp.full((bq, 1), -jnp.inf, F32), jnp.zeros((bq, 1), F32), jnp.zeros((bq, head_dim), F32)) for _ in range(heads))
    last = lax.div(block * bq, bk)
    carry = lax.fori_loop(0, last, functools.partial(step, masked=False), init)
    carry = step(last, carry, True)
    return [(acc / l).astype(BF16) for _, l, acc in carry]


def attn_kernel(layer, n_tp, heads, head_dim, bk, qkv_ref, r_ref, wo_hbm, out_ref,
                wo, ctx, ctx_out, lsem, sx, sy, ag, fs, fr, cs, cr):
    t, (yy, xx, c), partners = coords()
    mate, dev_x, dev_y = partners
    rows = out_ref.shape[0]
    width = out_ref.shape[1]
    cols = heads * head_dim
    load_o = pltpu.make_async_copy(wo_hbm.at[layer], wo.at[pl.ds(pl.multiple_of(t * cols, cols), cols)], lsem.at[0])
    load_o.start()
    others = [lax.rem(t + k, n_tp) for k in range(1, n_tp)]
    greet(others)
    load_o.wait()
    pl.semaphore_wait(pltpu.get_barrier_semaphore(), n_tp - 1)

    def span(dev, k):
        return pl.ds(pl.multiple_of(dev * cols + k * head_dim, head_dim), head_dim)

    def same(at, ssem, rsem, dev):
        return rcopy(wo.at[at], wo.at[at], ssem, rsem, dev)

    send = (same(span(t, 0), sx.at[0], ag.at[0], dev_x), same(span(t, 1), sy.at[0], ag.at[1], dev_y),
            same(span(t, 1), sx.at[1], ag.at[2], dev_x), same(span(t, 0), sy.at[1], ag.at[3], dev_y))
    relay = (same(span(dev_y, 1), sx.at[2], ag.at[4], dev_x), same(span(dev_x, 0), sy.at[2], ag.at[5], dev_y))
    dev_d = dev_x + dev_y - t
    landed = (span(dev_x, 0), span(dev_y, 1), span(dev_x, 1), span(dev_y, 0), span(dev_d, 1), span(dev_d, 0))
    own = pl.ds(pl.multiple_of(t * cols, cols), cols)
    to_mate = tuple(same(landed[k], fs.at[k], fr.at[k], mate) for k in range(6)) + (same(own, fs.at[6], fr.at[6], mate),)

    def take(k):
        pltpu.make_async_copy(wo.at[landed[k]], wo.at[landed[k]], ag.at[k]).wait()

    for copy in send:
        copy.start()
    to_mate[6].start()

    mine = pl.ds(pl.multiple_of(t * cols, cols), cols)

    def ctx_send(i, dev):
        return rcopy(ctx_out.at[i], ctx.at[:, mine], cs.at[i], cr.at[t], dev)

    @pl.loop(0, n_tp)
    def _(i):
        block = lax.rem(t + 1 + i, n_tp)

        @pl.when(i == 3)
        def _():
            take(0)
            take(1)
            for copy in relay:
                copy.start()

        @pl.when(i == 6)
        def _():
            for k in range(2, 6):
                take(k)
            for k in range(6):
                to_mate[k].start()
        for h, val in enumerate(attend(qkv_ref, block, rows, bk, heads, head_dim)):
            ctx_out[i, :, h * head_dim:(h + 1) * head_dim] = val

        @pl.when(i < n_tp - 1)
        def _():
            ctx_send(i, block).start()

    ctx[:, mine] = ctx_out[n_tp - 1]
    for copy in to_mate:
        copy.wait_recv()
    for dev in others:
        at = pl.ds(pl.multiple_of(dev * cols, cols), cols)
        pltpu.make_async_copy(ctx_out.at[0], ctx.at[:, at], cr.at[dev]).wait()
    nc = 512

    @pl.loop(0, width // nc)
    def _(n):
        at = pl.ds(pl.multiple_of(n * nc, nc), nc)
        out_ref[:, at] = r_ref[:, at].astype(F32) + jnp.dot(ctx[...], wo[:, at], preferred_element_type=F32)
    for copy in send + relay + to_mate:
        copy.wait_send()
    for i in range(n_tp - 1):
        ctx_send(i, mate).wait_send()


def attention(layer, qkv_all, resid, w_o, heads, head_dim, n_tp, bk=1024):
    rows, width = resid.shape
    cols = heads * head_dim
    seq = rows * n_tp
    vmem = pl.BlockSpec(memory_space=pltpu.VMEM)
    dma = pltpu.SemaphoreType.DMA
    return pl.pallas_call(
        functools.partial(attn_kernel, layer, n_tp, heads, head_dim, bk),
        out_shape=jax.ShapeDtypeStruct((rows, width), F32),
        in_specs=[vmem, vmem, pl.BlockSpec(memory_space=pl.ANY)],
        out_specs=vmem,
        scratch_shapes=[
            pltpu.VMEM((n_tp * cols, width), BF16),
            pltpu.VMEM((rows, n_tp * cols), BF16),
            pltpu.VMEM((n_tp, rows, cols), BF16),
            dma((1,)), dma((3,)), dma((3,)), dma((6,)), dma((7,)), dma((7,)), dma((n_tp,)), dma((n_tp,)),
        ],
        compiler_params=pltpu.CompilerParams(collective_id=3 + layer, has_side_effects=True, vmem_limit_bytes=VMEM_MAX),
        cost_estimate=pl.CostEstimate(flops=2 * seq * seq * cols, bytes_accessed=4 * seq * cols, transcendentals=seq * seq),
        name="attention" + str(layer),
    )(qkv_all, resid, w_o)


def mlp_kernel(layer, r_hbm, gain_ref, wg_hbm, wu_hbm, wd_hbm, out_hbm,
               wg, wu, wd, xbuf, prec, recv, acc, stash, act,
               lsem, sx, sy, ag, fs, fr, ps, pr, rr, ss):
    _, _, partners = coords()
    mate, dev_x, dev_y = partners
    rows, width = acc.shape
    half = rows // 2
    hid = act.shape[1]
    h0, h1 = pl.ds(0, half), pl.ds(half, half)
    hs = (h0, h1)
    nb = 64

    load_r = pltpu.make_async_copy(r_hbm, acc, lsem.at[0])
    load_r.start()
    greet(partners)
    loads = [pltpu.make_async_copy(src.at[layer], dst, lsem.at[k + 1]) for k, (src, dst) in enumerate(((wg_hbm, wg), (wu_hbm, wu), (wd_hbm, wd)))]
    load_r.wait()
    for copy in loads:
        copy.start()
    gather = RowGather(xbuf, sx, sy, ag, fs, fr, partners)
    gather.start(lambda k: norm_rows(acc, gain_ref, xbuf.at[0, 0], k * half, half))

    def partial_send(w):
        return rcopy(xbuf.at[w, 1], prec.at[w], ps.at[w], pr.at[w], mate)

    stage = (rcopy(xbuf.at[1, 1, h0], recv.at[0], ss.at[0], rr.at[0], dev_x),
             rcopy(xbuf.at[1, 1, h1], recv.at[1], ss.at[1], rr.at[1], dev_y),
             rcopy(xbuf.at[2, 1, h0], recv.at[2], ss.at[2], rr.at[2], dev_x),
             rcopy(xbuf.at[2, 1, h1], recv.at[3], ss.at[3], rr.at[3], dev_y),
             rcopy(xbuf.at[3, 1, h0], recv.at[4], ss.at[4], rr.at[4], dev_y),
             rcopy(xbuf.at[3, 1, h1], recv.at[5], ss.at[5], rr.at[5], dev_x))

    for copy in loads:
        copy.wait()
    cut = 768
    nd = 1024

    def gate_up(x_at, at):
        g = lax.dot_general(x_at[...], wg[at, :], (((1,), (1,)), ((), ())), preferred_element_type=F32)
        u = lax.dot_general(x_at[...], wu[at, :], (((1,), (1,)), ((), ())), preferred_element_type=F32)
        act[:, at] = (g * jax.nn.sigmoid(g) * u).astype(BF16)

    @pl.loop(0, 8)
    def _(s):
        w = lax.div(s, 2)
        rc = 1 - lax.rem(s, 2)

        @pl.when(rc == 1)
        def _():
            gather.forward(w).wait_recv()
        x_at = xbuf.at[w, rc]
        gate_up(x_at, pl.ds(0, cut))
        gate_up(x_at, pl.ds(cut, hid - cut))

        @pl.when(rc == 0)
        def _():
            @pl.when(w < 3)
            def _():
                gather.arrive(w + 1)
            partial_send(w).wait()

        @pl.loop(0, width // nd)
        def _(n):
            at = pl.ds(pl.multiple_of(n * nd, nd), nd)
            val = jnp.dot(act[...], wd[:, at], preferred_element_type=F32)

            @pl.when(rc == 1)
            def _():
                xbuf[w, 1, :, at] = val.astype(BF16)

            @pl.when(rc == 0)
            def _():
                total = val + prec[w, :, at].astype(F32)

                @pl.when(w == 0)
                def _():
                    acc[:, at] = acc[:, at] + total

                @pl.when(w == 3)
                def _():
                    stash[:, at] = total

                @pl.when((w == 1) | (w == 2))
                def _():
                    xbuf[w, 1, :, at] = total.astype(BF16)

        @pl.when(rc == 1)
        def _():
            partial_send(w).start()

        @pl.when(s == 3)
        def _():
            stage[0].start()
            stage[1].start()

        @pl.when(s == 5)
        def _():
            stage[2].start()
            stage[3].start()

    def blocks_of(k):
        def each(fn):
            @pl.loop(0, half // nb)
            def _(b):
                fn(pl.ds(pl.multiple_of(b * nb, nb), nb), pl.ds(pl.multiple_of(k * half + b * nb, nb), nb))
        return each

    for k in range(2):
        stage[k].wait_recv()

        @blocks_of(k)
        def _(at, to):
            acc[to, :] = acc[to, :] + recv[k, at, :].astype(F32)
    for k in range(2):
        stage[2 + k].wait_recv()

        @blocks_of(k)
        def _(at, to):
            xbuf[3, 1, to, :] = (stash[to, :] + recv[2 + k, at, :].astype(F32)).astype(BF16)
        stage[4 + k].start()
    gather.finish()
    narrow = out_hbm.dtype == BF16
    final = xbuf.at[0, 0] if narrow else acc
    outs = []
    for k in range(2):
        stage[4 + k].wait_recv()

        @blocks_of(k)
        def _(at, to):
            final[to, :] = (acc[to, :] + recv[4 + k, at, :].astype(F32)).astype(final.dtype)
        outs.append(pltpu.make_async_copy(final.at[hs[k]], out_hbm.at[hs[k]], lsem.at[k]))
        outs[k].start()
    for copy in stage:
        copy.wait_send()
    for copy in outs:
        copy.wait()


def mlp(layer, resid, gain, w_gate, w_up, w_down, out_dtype):
    rows, width = resid.shape
    hid = w_gate.shape[1]
    half = rows // 2
    any_spec = pl.BlockSpec(memory_space=pl.ANY)
    dma = pltpu.SemaphoreType.DMA
    return pl.pallas_call(
        functools.partial(mlp_kernel, layer),
        out_shape=jax.ShapeDtypeStruct((rows, width), out_dtype),
        in_specs=[any_spec, pl.BlockSpec(memory_space=pltpu.VMEM), any_spec, any_spec, any_spec],
        out_specs=any_spec,
        scratch_shapes=[
            pltpu.VMEM((hid, width), BF16),
            pltpu.VMEM((hid, width), BF16),
            pltpu.VMEM((hid, width), BF16),
            pltpu.VMEM((4, 2, rows, width), BF16),
            pltpu.VMEM((4, rows, width), BF16),
            pltpu.VMEM((6, half, width), BF16),
            pltpu.VMEM((rows, width), F32),
            pltpu.VMEM((rows, width), F32),
            pltpu.VMEM((rows, hid), BF16),
            dma((4,)),
        ] + gather_sems() + [dma((4,)), dma((4,)), dma((6,)), dma((6,))],
        compiler_params=pltpu.CompilerParams(collective_id=5 + layer, has_side_effects=True, vmem_limit_bytes=VMEM_MAX),
        cost_estimate=pl.CostEstimate(flops=6 * 8 * rows * width * hid, bytes_accessed=6 * width * hid, transcendentals=8 * rows * hid),
        name="mlp" + str(layer),
    )(resid, gain, w_gate, w_up, w_down)


def solution(mesh):
    n_tp = mesh.shape['tp']
    tok_spec = P('dp', 'tp', None)
    in_specs = (tok_spec, P(), P(None, None, 'tp', None), P(), P(None, 'tp', None, None), P(), P(None, None, 'tp'), P(None, None, 'tp'), P(None, 'tp', None))

    def body(hidden, norm_attn, w_q, w_kv, w_o, norm_mlp, w_gate, w_up, w_down):
        n_layers, width, heads, head_dim = w_q.shape
        n_kv = w_kv.shape[3]
        rows = hidden.shape[1]
        kv_head = (lax.axis_index('tp') * n_kv) // n_tp
        cos_t, sin_t = rope_tables(rows * n_tp, head_dim)
        kv = lax.dynamic_index_in_dim(w_kv, kv_head, axis=3, keepdims=False)
        w_qkv = jnp.concatenate([w_q.reshape(n_layers, width, heads * head_dim), kv.reshape(n_layers, width, 2 * head_dim)], axis=2)
        w_o = w_o.reshape(n_layers, heads * head_dim, width)
        w_gate = jnp.swapaxes(w_gate, 1, 2)
        w_up = jnp.swapaxes(w_up, 1, 2)
        resid = hidden[0]
        for layer in range(n_layers):
            qkv_all = qkv(layer, resid, norm_attn[layer][None], w_qkv[layer], cos_t, sin_t, heads, head_dim, n_tp)
            resid = attention(layer, qkv_all, resid, w_o, heads, head_dim, n_tp)
            resid = mlp(layer, resid, norm_mlp[layer][None], w_gate, w_up, w_down, BF16 if layer == n_layers - 1 else F32)
        return resid[None]

    return jax.shard_map(body, mesh=mesh, in_specs=in_specs, out_specs=tok_spec, check_vma=False)
```

```python
import functools
import math
import jax
import jax.numpy as jnp
import numpy as np
from jax import lax
from jax.experimental import pallas as pl
from jax.experimental.pallas import tpu as pltpu
from jax.sharding import PartitionSpec as P

EPS = 1e-5
ROPE_BASE = 10000.0
MESH = pl.DeviceIdType.MESH
VMEM_MAX = 67043328
F32 = jnp.float32
BF16 = jnp.bfloat16


def rope_tables(seq, step, head_dim):
    half_dim = head_dim // 2
    inv_freq = ROPE_BASE ** (-2.0 * np.arange(half_dim, dtype=np.float64) / head_dim)

    def table(positions):
        angles = positions.astype(np.float64)[:, None] * inv_freq[None, :]
        cos_t, sin_t = np.cos(angles), np.sin(angles)
        return np.stack([np.concatenate([cos_t, cos_t], axis=1), np.concatenate([-sin_t, sin_t], axis=1)]).astype(np.float32)

    return table(np.arange(0, seq, step)), table(np.arange(step))


def coords():
    t = lax.axis_index('tp')
    c = lax.rem(t, 2)
    xx = lax.rem(lax.div(t, 2), 2)
    yy = lax.div(t, 4)
    return t, (yy, xx, c), (t + 1 - 2 * c, t + 2 - 4 * xx, t + 4 - 8 * yy)


def rcopy(src, dst, ssem, rsem, dev):
    return pltpu.make_async_remote_copy(src_ref=src, dst_ref=dst, send_sem=ssem, recv_sem=rsem,
                                        device_id={'tp': dev}, device_id_type=MESH)


def greet(devices):
    for dev in devices:
        pl.semaphore_signal(pltpu.get_barrier_semaphore(), inc=1, device_id={'tp': dev}, device_id_type=MESH)


class RowGather:
    def __init__(self, xbuf, sx, sy, ag, fs, fr, partners, greeted=3):
        mate, dev_x, dev_y = partners
        rows = xbuf.shape[2]
        half = rows // 2
        lead = half // 4
        h0, h1 = pl.ds(0, half), pl.ds(half, half)
        own = xbuf.at[0, 0]
        self.xbuf, self.ag, self.fs, self.fr, self.mate = xbuf, ag, fs, fr, mate
        self.halves = (h0, h1)
        self.greeted = greeted

        def piece(k, sem, dev, first, size, window, slot):
            at = pl.ds(first, size)
            return rcopy(own.at[at], xbuf.at[window, 0, at], sem.at[k], ag.at[window, slot], dev)

        self.first = (piece(0, sx, dev_x, 0, half, 1, 0), piece(0, sy, dev_y, half, half, 1, 1))
        self.lead = (piece(1, sx, dev_x, half, lead, 3, 1), piece(1, sy, dev_y, 0, lead, 3, 0))
        self.rest = (piece(2, sx, dev_x, half + lead, half - lead, 3, 1), piece(2, sy, dev_y, lead, half - lead, 3, 0))
        self.relay = (rcopy(xbuf.at[1, 0, h1], xbuf.at[2, 0, h1], sx.at[3], ag.at[2, 1], dev_x),
                      rcopy(xbuf.at[1, 0, h0], xbuf.at[2, 0, h0], sy.at[3], ag.at[2, 0], dev_y))

    def forward(self, w):
        return rcopy(self.xbuf.at[w, 0], self.xbuf.at[w, 1], self.fs.at[w], self.fr.at[w], self.mate)

    def start(self, norm_half):
        norm_half(0)
        pl.semaphore_wait(pltpu.get_barrier_semaphore(), self.greeted)
        self.first[0].start()
        norm_half(1)
        self.first[1].start()
        self.lead[0].start()
        self.lead[1].start()
        self.forward(0).start()

    def arrive(self, w):
        for k in range(2):
            at = self.halves[k]
            pltpu.make_async_copy(self.xbuf.at[0, 0, at], self.xbuf.at[w, 0, at], self.ag.at[w, k]).wait()

        @pl.when(w == 1)
        def _():
            for copy in self.relay + self.rest:
                copy.start()
        self.forward(w).start()

    def finish(self):
        for copy in self.first + self.lead + self.relay + self.rest:
            copy.wait_send()
        for w in range(4):
            self.forward(w).wait_send()


def gather_sems():
    dma = pltpu.SemaphoreType.DMA
    return [dma((4,)), dma((4,)), dma((4, 2)), dma((4,)), dma((4,))]


def norm_rows(src, gain_ref, dst, first, count):
    nb = 64

    @pl.loop(0, count // nb)
    def _(b):
        at = pl.ds(pl.multiple_of(first + b * nb, nb), nb)
        r = src[at, :].astype(F32)
        mean_sq = jnp.mean(r * r, axis=-1, keepdims=True)
        dst[at, :] = (r * lax.rsqrt(mean_sq + EPS) * gain_ref[...]).astype(BF16)


def attend(qkv_ref, block, bq, bk, heads, head_dim):
    scale = math.log2(math.e) / math.sqrt(head_dim)
    mask = lax.broadcasted_iota(jnp.int32, (bq, bq), 0) >= lax.broadcasted_iota(jnp.int32, (bq, bq), 1)
    q_at = pl.ds(pl.multiple_of(block * bq, bq), bq)
    qs = [qkv_ref[q_at, h * head_dim:(h + 1) * head_dim] for h in range(heads)]

    def step(first, count, carry, masked):
        at = pl.ds(pl.multiple_of(first, bq), count)
        k_blk = qkv_ref[at, heads * head_dim:(heads + 1) * head_dim]
        v_blk = qkv_ref[at, (heads + 1) * head_dim:(heads + 2) * head_dim]
        out = []
        for h in range(heads):
            m, l, acc = carry[h]
            s = lax.dot_general(qs[h], k_blk, (((1,), (1,)), ((), ())), preferred_element_type=F32)
            if masked:
                s = jnp.where(mask, s, -jnp.inf)
            m_new = jnp.maximum(m, jnp.max(s, axis=-1, keepdims=True))
            p = jnp.exp2((s - m_new) * scale)
            alpha = jnp.exp2((m - m_new) * scale)
            l = l * alpha + jnp.sum(p, axis=-1, keepdims=True)
            acc = acc * alpha + jnp.dot(p.astype(BF16), v_blk, preferred_element_type=F32)
            out.append((m_new, l, acc))
        return tuple(out)

    carry = tuple((jnp.full((bq, 1), -jnp.inf, F32), jnp.zeros((bq, 1), F32), jnp.zeros((bq, head_dim), F32)) for _ in range(heads))
    carry = step(block * bq, bq, carry, True)
    full = lax.div(block * bq, bk)
    carry = lax.fori_loop(0, full, lambda j, cur: step(j * bk, bk, cur, False), carry)
    carry = lax.fori_loop(full * (bk // bq), block, lambda j, cur: step(j * bq, bq, cur, False), carry)
    return [(acc / l).astype(BF16) for _, l, acc in carry]


def attn_kernel(layer, n_tp, n_kv, heads, head_dim, bk, r_hbm, gain_ref, far_ref, near_ref, wq_hbm, wkv_hbm, wo_hbm, out_hbm,
                xbuf, rin, wq, wkv, wide, w_all, qkv_ref, wo, ctx, ctx_out, res,
                lsem, sx, sy, ag, fs, fr, ox, oy, oz, oa, ob, om, on, cs, cr, es):
    t, (yy, xx, c), partners = coords()
    z = lax.axis_index('dp')
    mate, dev_x, dev_y = partners
    dev_d = dev_x + dev_y - t
    rows, width = res.shape
    half = rows // 2
    cols = heads * head_dim

    load_r = pltpu.make_async_copy(r_hbm, rin, lsem.at[0])
    load_r.start()
    others = [lax.rem(t + k, n_tp) for k in range(1, n_tp)]
    greet(others)
    pl.semaphore_signal(pltpu.get_barrier_semaphore(), inc=1, device_id={'dp': 1 - z, 'tp': t}, device_id_type=MESH)
    own_o = pl.ds(pl.multiple_of(t * cols, cols), cols)
    loads = (pltpu.make_async_copy(wq_hbm.at[layer], wq, lsem.at[1]),
             pltpu.make_async_copy(wkv_hbm.at[layer], wkv, lsem.at[2]),
             pltpu.make_async_copy(wo_hbm.at[layer], wo.at[own_o], lsem.at[3]))
    load_r.wait()
    for copy in loads:
        copy.start()
    gather = RowGather(xbuf, sx, sy, ag, fs, fr, partners, n_tp)
    gather.start(lambda k: norm_rows(rin, gain_ref, xbuf.at[0, 0], k * half, half))
    for copy in loads:
        copy.wait()

    kv_head = lax.div(t * n_kv, n_tp)
    nd = 256

    @pl.loop(0, width // nd)
    def _(b):
        to = pl.ds(pl.multiple_of(b * nd, nd), nd)
        wide[pl.ds(0, heads * nd), :] = wq[pl.ds(pl.multiple_of(b * heads * nd, nd), heads * nd), :].astype(F32)
        for h in range(heads):
            w_all[to, h * head_dim:(h + 1) * head_dim] = wide[pl.ds(h, nd, stride=heads), :].astype(BF16)
        wide[pl.ds(0, 2 * n_kv * nd), :] = wkv[pl.ds(pl.multiple_of(b * 2 * n_kv * nd, nd), 2 * n_kv * nd), :].astype(F32)
        for h in range(2):
            w_all[to, (heads + h) * head_dim:(heads + h + 1) * head_dim] = wide[pl.ds(h * n_kv + kv_head, nd, stride=2 * n_kv), :].astype(BF16)

    @pl.loop(0, 8)
    def _(s):
        w = lax.div(s, 2)
        rc = lax.rem(s, 2)

        @pl.when((rc == 0) & (w >= 1))
        def _():
            gather.arrive(w)

        @pl.when(rc == 1)
        def _():
            gather.forward(w).wait_recv()
        proj = jnp.dot(xbuf[w, rc], w_all[...], preferred_element_type=F32)
        core = c + rc - 2 * c * rc
        one = lax.rem(lax.div(w + 1, 2), 2)
        two = lax.div(w, 2)
        for k in range(2):
            flip_x, flip_y = (one, two) if k == 0 else (two, one)
            chip = 2 * (yy + flip_y - 2 * yy * flip_y) + xx + flip_x - 2 * xx * flip_x
            piece = (chip * 2 + core) * 2 + k
            at = pl.ds(pl.multiple_of(piece * half, half), half)
            part = proj[k * half:(k + 1) * half]
            cos_f, sin_f = far_ref[0, pl.ds(piece, 1), :], far_ref[1, pl.ds(piece, 1), :]
            cos_n, sin_n = near_ref[0], near_ref[1]
            cos_b = cos_f * cos_n - sin_f * sin_n
            sin_b = sin_f * cos_n + cos_f * sin_n
            for h in range(heads + 1):
                at_h = slice(h * head_dim, (h + 1) * head_dim)
                v = part[:, at_h]
                qkv_ref[at, at_h] = (v * cos_b + pltpu.roll(v, head_dim // 2, 1) * sin_b).astype(BF16)
            at_h = slice((heads + 1) * head_dim, (heads + 2) * head_dim)
            qkv_ref[at, at_h] = part[:, at_h].astype(BF16)

    part_rows = head_dim // 2

    def span(dev, k, p):
        return pl.ds(pl.multiple_of(dev * cols + k * head_dim + p * part_rows, part_rows), part_rows)

    def same(at, ssem, rsem, dev):
        return rcopy(wo.at[at], wo.at[at], ssem, rsem, dev)

    def across(at, ssem, rsem):
        return pltpu.make_async_remote_copy(src_ref=wo.at[at], dst_ref=wo.at[at], send_sem=ssem, recv_sem=rsem,
                                            device_id={'dp': 1 - z, 'tp': t}, device_id_type=MESH)

    send = (same(span(t, 0, z), ox.at[0], oa.at[0], dev_x), same(span(t, 1, z), oy.at[0], oa.at[1], dev_y),
            same(span(t, 1, z), ox.at[1], oa.at[2], dev_x), same(span(t, 0, z), oy.at[1], oa.at[3], dev_y))
    relay = (same(span(dev_y, 1, z), ox.at[2], oa.at[4], dev_x), same(span(dev_x, 0, z), oy.at[2], oa.at[5], dev_y))
    from_dev = ((dev_x, 0), (dev_y, 1), (dev_x, 1), (dev_y, 0), (dev_d, 1), (dev_d, 0))
    via_z = [across(span(dev, k, z), oz.at[i], ob.at[i]) for i, (dev, k) in enumerate(from_dev)]
    to_mate = [same(span(dev, k, z), om.at[i], on.at[i], mate) for i, (dev, k) in enumerate(from_dev)]
    to_mate += [same(span(dev, k, 1 - z), om.at[6 + i], on.at[6 + i], mate) for i, (dev, k) in enumerate(from_dev)]
    to_mate.append(same(own_o, om.at[12], on.at[12], mate))

    def take(i, sem, p):
        at = span(from_dev[i][0], from_dev[i][1], p)
        pltpu.make_async_copy(wo.at[at], wo.at[at], sem.at[i]).wait()

    for copy in send:
        copy.start()
    to_mate[12].start()

    def ctx_send(i, dev):
        return rcopy(ctx_out.at[i], ctx.at[:, own_o], cs.at[i], cr.at[t], dev)

    @pl.loop(0, n_tp)
    def _(i):
        block = lax.rem(t + 1 + i, n_tp)

        @pl.when(i == 3)
        def _():
            take(0, oa, z)
            take(1, oa, z)
            for copy in relay:
                copy.start()
            take(2, oa, z)
            take(3, oa, z)
            for k in range(4):
                via_z[k].start()
                to_mate[k].start()

        @pl.when(i == 5)
        def _():
            for k in range(4, 6):
                take(k, oa, z)
                via_z[k].start()
                to_mate[k].start()

        @pl.when(i == 7)
        def _():
            for k in range(6):
                take(k, ob, 1 - z)
                to_mate[6 + k].start()
        for h, val in enumerate(attend(qkv_ref, block, rows, bk, heads, head_dim)):
            ctx_out[i, :, h * head_dim:(h + 1) * head_dim] = val

        @pl.when(i < n_tp - 1)
        def _():
            ctx_send(i, block).start()

    ctx[:, own_o] = ctx_out[n_tp - 1]
    for copy in to_mate:
        copy.wait_recv()
    for dev in others:
        at = pl.ds(pl.multiple_of(dev * cols, cols), cols)
        pltpu.make_async_copy(ctx_out.at[0], ctx.at[:, at], cr.at[dev]).wait()
    nc = 512
    outs = []
    for n in range(width // nc):
        at = pl.ds(n * nc, nc)
        res[:, at] = rin[:, at].astype(F32) + jnp.dot(ctx[...], wo[:, at], preferred_element_type=F32)
        outs.append(pltpu.make_async_copy(res.at[:, at], out_hbm.at[:, at], es.at[n]))
        outs[n].start()
    gather.finish()
    for copy in list(send + relay) + via_z + to_mate:
        copy.wait_send()
    for i in range(n_tp - 1):
        ctx_send(i, mate).wait_send()
    for copy in outs:
        copy.wait()


def attention(layer, resid, gain, far, near, w_q, w_kv, w_o, n_tp, bk=1024):
    rows, width = resid.shape
    cols, head_dim = w_o.shape[1], w_q.shape[2]
    heads = cols // head_dim
    n_kv = w_kv.shape[1] // (2 * width)
    seq = rows * n_tp
    vmem = pl.BlockSpec(memory_space=pltpu.VMEM)
    anywhere = pl.BlockSpec(memory_space=pl.ANY)
    dma = pltpu.SemaphoreType.DMA
    return pl.pallas_call(
        functools.partial(attn_kernel, layer, n_tp, n_kv, heads, head_dim, bk),
        out_shape=jax.ShapeDtypeStruct((rows, width), F32),
        in_specs=[anywhere, vmem, vmem, vmem, anywhere, anywhere, anywhere],
        out_specs=anywhere,
        scratch_shapes=[
            pltpu.VMEM((4, 2, rows, width), BF16),
            pltpu.VMEM((rows, width), resid.dtype),
            pltpu.VMEM(w_q.shape[1:], BF16),
            pltpu.VMEM(w_kv.shape[1:], BF16),
            pltpu.VMEM((256 * max(heads, 2 * n_kv), head_dim), F32),
            pltpu.VMEM((width, cols + 2 * head_dim), BF16),
            pltpu.VMEM((seq, cols + 2 * head_dim), BF16),
            pltpu.VMEM((n_tp * cols, width), BF16),
            pltpu.VMEM((rows, n_tp * cols), BF16),
            pltpu.VMEM((n_tp, rows, cols), BF16),
            pltpu.VMEM((rows, width), F32),
            dma((4,)),
        ] + gather_sems() + [dma((3,)), dma((3,)), dma((6,)), dma((6,)), dma((6,)), dma((13,)), dma((13,)), dma((n_tp,)), dma((n_tp,)), dma((4,))],
        compiler_params=pltpu.CompilerParams(collective_id=1 + layer, has_side_effects=True, vmem_limit_bytes=VMEM_MAX),
        cost_estimate=pl.CostEstimate(flops=2 * seq * seq * cols, bytes_accessed=4 * seq * cols, transcendentals=seq * seq),
        name="attention" + str(layer),
    )(resid, gain, far, near, w_q, w_kv, w_o)


def mlp_kernel(layer, r_hbm, gain_ref, wg_hbm, wu_hbm, wd_hbm, out_hbm,
               wg, wu, wd, xbuf, prec, recv, acc, stash, act,
               lsem, sx, sy, ag, fs, fr, ps, pr, rr, ss):
    _, _, partners = coords()
    mate, dev_x, dev_y = partners
    rows, width = acc.shape
    half = rows // 2
    hid = act.shape[1]
    h0, h1 = pl.ds(0, half), pl.ds(half, half)
    hs = (h0, h1)
    nb = 64

    load_r = pltpu.make_async_copy(r_hbm, acc, lsem.at[0])
    load_r.start()
    greet(partners)
    loads = [pltpu.make_async_copy(src.at[layer], dst, lsem.at[k + 1]) for k, (src, dst) in enumerate(((wg_hbm, wg), (wu_hbm, wu), (wd_hbm, wd)))]
    load_r.wait()
    for copy in loads:
        copy.start()
    gather = RowGather(xbuf, sx, sy, ag, fs, fr, partners)
    gather.start(lambda k: norm_rows(acc, gain_ref, xbuf.at[0, 0], k * half, half))

    def partial_send(w):
        return rcopy(xbuf.at[w, 1], prec.at[w], ps.at[w], pr.at[w], mate)

    stage = (rcopy(xbuf.at[1, 1, h0], recv.at[0], ss.at[0], rr.at[0], dev_x),
             rcopy(xbuf.at[1, 1, h1], recv.at[1], ss.at[1], rr.at[1], dev_y),
             rcopy(xbuf.at[2, 1, h0], recv.at[2], ss.at[2], rr.at[2], dev_x),
             rcopy(xbuf.at[2, 1, h1], recv.at[3], ss.at[3], rr.at[3], dev_y),
             rcopy(xbuf.at[3, 1, h0], recv.at[4], ss.at[4], rr.at[4], dev_y),
             rcopy(xbuf.at[3, 1, h1], recv.at[5], ss.at[5], rr.at[5], dev_x))

    for copy in loads:
        copy.wait()
    cut = 768
    nd = 1024

    def gate_up(x_at, at):
        g = lax.dot_general(x_at[...], wg[at, :], (((1,), (1,)), ((), ())), preferred_element_type=F32)
        u = lax.dot_general(x_at[...], wu[at, :], (((1,), (1,)), ((), ())), preferred_element_type=F32)
        act[:, at] = (g * jax.nn.sigmoid(g) * u).astype(BF16)

    @pl.loop(0, 8)
    def _(s):
        w = lax.div(s, 2)
        rc = 1 - lax.rem(s, 2)

        @pl.when(rc == 1)
        def _():
            gather.forward(w).wait_recv()
        x_at = xbuf.at[w, rc]
        gate_up(x_at, pl.ds(0, cut))
        gate_up(x_at, pl.ds(cut, hid - cut))

        @pl.when(rc == 0)
        def _():
            @pl.when(w < 3)
            def _():
                gather.arrive(w + 1)
            partial_send(w).wait()

        @pl.loop(0, width // nd)
        def _(n):
            at = pl.ds(pl.multiple_of(n * nd, nd), nd)
            val = jnp.dot(act[...], wd[:, at], preferred_element_type=F32)

            @pl.when(rc == 1)
            def _():
                xbuf[w, 1, :, at] = val.astype(BF16)

            @pl.when(rc == 0)
            def _():
                total = val + prec[w, :, at].astype(F32)

                @pl.when(w == 0)
                def _():
                    acc[:, at] = acc[:, at] + total

                @pl.when(w == 3)
                def _():
                    stash[:, at] = total

                @pl.when((w == 1) | (w == 2))
                def _():
                    xbuf[w, 1, :, at] = total.astype(BF16)

        @pl.when(rc == 1)
        def _():
            partial_send(w).start()

        @pl.when(s == 3)
        def _():
            stage[0].start()
            stage[1].start()

        @pl.when(s == 5)
        def _():
            stage[2].start()
            stage[3].start()

    def blocks_of(k):
        def each(fn):
            @pl.loop(0, half // nb)
            def _(b):
                fn(pl.ds(pl.multiple_of(b * nb, nb), nb), pl.ds(pl.multiple_of(k * half + b * nb, nb), nb))
        return each

    for k in range(2):
        stage[k].wait_recv()

        @blocks_of(k)
        def _(at, to):
            acc[to, :] = acc[to, :] + recv[k, at, :].astype(F32)
    for k in range(2):
        stage[2 + k].wait_recv()

        @blocks_of(k)
        def _(at, to):
            xbuf[3, 1, to, :] = (stash[to, :] + recv[2 + k, at, :].astype(F32)).astype(BF16)
        stage[4 + k].start()
    gather.finish()
    narrow = out_hbm.dtype == BF16
    final = xbuf.at[0, 0] if narrow else acc
    outs = []
    for k in range(2):
        stage[4 + k].wait_recv()

        @blocks_of(k)
        def _(at, to):
            final[to, :] = (acc[to, :] + recv[4 + k, at, :].astype(F32)).astype(final.dtype)
        outs.append(pltpu.make_async_copy(final.at[hs[k]], out_hbm.at[hs[k]], lsem.at[k]))
        outs[k].start()
    for copy in stage:
        copy.wait_send()
    for copy in outs:
        copy.wait()


def mlp(layer, resid, gain, w_gate, w_up, w_down, out_dtype):
    rows, width = resid.shape
    hid = w_gate.shape[1]
    half = rows // 2
    any_spec = pl.BlockSpec(memory_space=pl.ANY)
    dma = pltpu.SemaphoreType.DMA
    return pl.pallas_call(
        functools.partial(mlp_kernel, layer),
        out_shape=jax.ShapeDtypeStruct((rows, width), out_dtype),
        in_specs=[any_spec, pl.BlockSpec(memory_space=pltpu.VMEM), any_spec, any_spec, any_spec],
        out_specs=any_spec,
        scratch_shapes=[
            pltpu.VMEM((hid, width), BF16),
            pltpu.VMEM((hid, width), BF16),
            pltpu.VMEM((hid, width), BF16),
            pltpu.VMEM((4, 2, rows, width), BF16),
            pltpu.VMEM((4, rows, width), BF16),
            pltpu.VMEM((6, half, width), BF16),
            pltpu.VMEM((rows, width), F32),
            pltpu.VMEM((rows, width), F32),
            pltpu.VMEM((rows, hid), BF16),
            dma((4,)),
        ] + gather_sems() + [dma((4,)), dma((4,)), dma((6,)), dma((6,))],
        compiler_params=pltpu.CompilerParams(collective_id=5 + layer, has_side_effects=True, vmem_limit_bytes=VMEM_MAX),
        cost_estimate=pl.CostEstimate(flops=6 * 8 * rows * width * hid, bytes_accessed=6 * width * hid, transcendentals=8 * rows * hid),
        name="mlp" + str(layer),
    )(resid, gain, w_gate, w_up, w_down)


def solution(mesh):
    n_tp = mesh.shape['tp']
    tok_spec = P('dp', 'tp', None)
    in_specs = (tok_spec, P(), P(None, None, 'tp', None), P(), P(None, 'tp', None, None), P(), P(None, None, 'tp'), P(None, None, 'tp'), P(None, 'tp', None))

    def body(hidden, norm_attn, w_q, w_kv, w_o, norm_mlp, w_gate, w_up, w_down):
        n_layers, width, heads, head_dim = w_q.shape
        n_kv = w_kv.shape[3]
        rows = hidden.shape[1]
        far, near = rope_tables(rows * n_tp, rows // 2, head_dim)
        w_q = w_q.reshape(n_layers, width * heads, head_dim)
        w_kv = w_kv.reshape(n_layers, width * 2 * n_kv, head_dim)
        w_o = w_o.reshape(n_layers, heads * head_dim, width)
        w_gate = jnp.swapaxes(w_gate, 1, 2)
        w_up = jnp.swapaxes(w_up, 1, 2)
        resid = hidden[0]
        for layer in range(n_layers):
            resid = attention(layer, resid, norm_attn[layer][None], far, near, w_q, w_kv, w_o, n_tp)
            resid = mlp(layer, resid, norm_mlp[layer][None], w_gate, w_up, w_down, BF16 if layer == n_layers - 1 else F32)
        return resid[None]

    return jax.shard_map(body, mesh=mesh, in_specs=in_specs, out_specs=tok_spec, check_vma=False)
```

```python
import functools
import math
import jax
import jax.numpy as jnp
import numpy as np
from jax import lax
from jax.experimental import pallas as pl
from jax.experimental.pallas import tpu as pltpu
from jax.sharding import PartitionSpec as P

EPS = 1e-5
ROPE_BASE = 10000.0
MESH = pl.DeviceIdType.MESH
VMEM_MAX = 67043328
F32 = jnp.float32
BF16 = jnp.bfloat16


def rope_tables(seq, step, head_dim):
    half_dim = head_dim // 2
    inv_freq = ROPE_BASE ** (-2.0 * np.arange(half_dim, dtype=np.float64) / head_dim)

    def table(positions):
        angles = positions.astype(np.float64)[:, None] * inv_freq[None, :]
        cos_t, sin_t = np.cos(angles), np.sin(angles)
        return np.stack([np.concatenate([cos_t, cos_t], axis=1), np.concatenate([-sin_t, sin_t], axis=1)]).astype(np.float32)

    return table(np.arange(0, seq, step)), table(np.arange(step))


def coords():
    t = lax.axis_index('tp')
    c = lax.rem(t, 2)
    xx = lax.rem(lax.div(t, 2), 2)
    yy = lax.div(t, 4)
    return t, (yy, xx, c), (t + 1 - 2 * c, t + 2 - 4 * xx, t + 4 - 8 * yy)


def rcopy(src, dst, ssem, rsem, dev):
    return pltpu.make_async_remote_copy(src_ref=src, dst_ref=dst, send_sem=ssem, recv_sem=rsem,
                                        device_id={'tp': dev}, device_id_type=MESH)


def greet(devices):
    for dev in devices:
        pl.semaphore_signal(pltpu.get_barrier_semaphore(), inc=1, device_id={'tp': dev}, device_id_type=MESH)


class RowGather:
    def __init__(self, xbuf, sx, sy, ag, fs, fr, partners):
        mate, dev_x, dev_y = partners
        rows = xbuf.shape[2]
        half = rows // 2
        lead = half // 4
        h0, h1 = pl.ds(0, half), pl.ds(half, half)
        own = xbuf.at[0, 0]
        self.xbuf, self.ag, self.fs, self.fr, self.mate = xbuf, ag, fs, fr, mate
        self.halves = (h0, h1)

        def piece(k, sem, dev, first, size, window, slot):
            at = pl.ds(first, size)
            return rcopy(own.at[at], xbuf.at[window, 0, at], sem.at[k], ag.at[window, slot], dev)

        self.first = (piece(0, sx, dev_x, 0, half, 1, 0), piece(0, sy, dev_y, half, half, 1, 1))
        self.lead = (piece(1, sx, dev_x, half, lead, 3, 1), piece(1, sy, dev_y, 0, lead, 3, 0))
        self.rest = (piece(2, sx, dev_x, half + lead, half - lead, 3, 1), piece(2, sy, dev_y, lead, half - lead, 3, 0))
        self.relay = (rcopy(xbuf.at[1, 0, h1], xbuf.at[2, 0, h1], sx.at[3], ag.at[2, 1], dev_x),
                      rcopy(xbuf.at[1, 0, h0], xbuf.at[2, 0, h0], sy.at[3], ag.at[2, 0], dev_y))

    def forward(self, w):
        return rcopy(self.xbuf.at[w, 0], self.xbuf.at[w, 1], self.fs.at[w], self.fr.at[w], self.mate)

    def start(self, norm_half):
        norm_half(0)
        pl.semaphore_wait(pltpu.get_barrier_semaphore(), 3)
        self.first[0].start()
        norm_half(1)
        self.first[1].start()
        self.lead[0].start()
        self.lead[1].start()
        self.forward(0).start()

    def arrive(self, w):
        for k in range(2):
            at = self.halves[k]
            pltpu.make_async_copy(self.xbuf.at[0, 0, at], self.xbuf.at[w, 0, at], self.ag.at[w, k]).wait()

        @pl.when(w == 1)
        def _():
            for copy in self.relay + self.rest:
                copy.start()
        self.forward(w).start()

    def finish(self):
        for copy in self.first + self.lead + self.relay + self.rest:
            copy.wait_send()
        for w in range(4):
            self.forward(w).wait_send()


def gather_sems():
    dma = pltpu.SemaphoreType.DMA
    return [dma((4,)), dma((4,)), dma((4, 2)), dma((4,)), dma((4,))]


def norm_rows(src, gain_ref, dst, first, count):
    nb = 64

    @pl.loop(0, count // nb)
    def _(b):
        at = pl.ds(pl.multiple_of(first + b * nb, nb), nb)
        r = src[at, :].astype(F32)
        mean_sq = jnp.mean(r * r, axis=-1, keepdims=True)
        dst[at, :] = (r * lax.rsqrt(mean_sq + EPS) * gain_ref[...]).astype(BF16)


class BlockGather:
    def __init__(self, xbuf, sf, ag, fs, fr, mate, dev_f, dev_s):
        rows = xbuf.shape[2]
        half = rows // 2
        self.halves = (pl.ds(0, half), pl.ds(half, half))
        self.xbuf, self.ag, self.fs, self.fr, self.mate = xbuf, ag, fs, fr, mate

        def copies(source, target, sem, dev):
            return [rcopy(xbuf.at[source, 0, at], xbuf.at[target, 0, at], sf.at[sem + k], ag.at[target, k], dev)
                    for k, at in enumerate(self.halves)]

        self.first = copies(0, 1, 0, dev_f)
        self.relay = copies(1, 2, 2, dev_s)
        self.second = copies(0, 3, 4, dev_s)

    def forward(self, w):
        return rcopy(self.xbuf.at[w, 0], self.xbuf.at[w, 1], self.fs.at[w], self.fr.at[w], self.mate)

    def arrive(self, w, between):
        for k, at in enumerate(self.halves):
            pltpu.make_async_copy(self.xbuf.at[0, 0, at], self.xbuf.at[w, 0, at], self.ag.at[w, k]).wait()

            @pl.when(w == 1)
            def _():
                self.relay[k].start()
        self.forward(w).start()

        @pl.when(w == 1)
        def _():
            between()
            for copy in self.second:
                copy.start()

    def finish(self):
        for copy in self.first + self.relay + self.second:
            copy.wait_send()
        for w in range(4):
            self.forward(w).wait_send()


def attn_kernel(layer, n_tp, n_kv, heads, head_dim, r_hbm, gain_ref, far_ref, near_ref, wq_hbm, wkv_hbm, wo_hbm, out_hbm,
                xbuf, rin, wq, wkv, wide, w_all, qkv_ref, wo, ctx, ctx_out, res, stat, total,
                lsem, sf, ag, fs, fr, of, oz, oa, ob, om, on, cs, cr, es):
    t, (yy, xx, c), (mate, dev_x, dev_y) = coords()
    z = lax.axis_index('dp')
    dev_d = dev_x + dev_y - t
    dev_f = dev_x + c * (dev_y - dev_x)
    dev_s = dev_y + c * (dev_x - dev_y)
    rows, width = res.shape
    half = rows // 2
    cols = heads * head_dim

    load_r = pltpu.make_async_copy(r_hbm, rin, lsem.at[0])
    load_r.start()
    others = [lax.rem(t + k, n_tp) for k in range(1, n_tp)]
    greet(others)
    pl.semaphore_signal(pltpu.get_barrier_semaphore(), inc=1, device_id={'dp': 1 - z, 'tp': t}, device_id_type=MESH)
    own_o = pl.ds(pl.multiple_of(t * cols, cols), cols)
    loads = (pltpu.make_async_copy(wo_hbm.at[layer], wo.at[own_o], lsem.at[3]),
             pltpu.make_async_copy(wq_hbm.at[layer], wq, lsem.at[1]),
             pltpu.make_async_copy(wkv_hbm.at[layer], wkv, lsem.at[2]))
    load_r.wait()
    for copy in loads:
        copy.start()
    gather = BlockGather(xbuf, sf, ag, fs, fr, mate, dev_f, dev_s)
    norm_rows(rin, gain_ref, xbuf.at[0, 0], 0, half)
    pl.semaphore_wait(pltpu.get_barrier_semaphore(), n_tp)
    gather.first[0].start()
    norm_rows(rin, gain_ref, xbuf.at[0, 0], half, half)
    gather.first[1].start()
    gather.forward(0).start()

    part_rows = head_dim // 2

    def span(dev, k, p):
        return pl.ds(pl.multiple_of(dev * cols + k * head_dim + p * part_rows, part_rows), part_rows)

    def same(at, ssem, rsem, dev):
        return rcopy(wo.at[at], wo.at[at], ssem, rsem, dev)

    def across(at, ssem, rsem):
        return pltpu.make_async_remote_copy(src_ref=wo.at[at], dst_ref=wo.at[at], send_sem=ssem, recv_sem=rsem,
                                            device_id={'dp': 1 - z, 'tp': t}, device_id_type=MESH)

    from_dev = ((dev_f, 0), (dev_s, 1), (dev_f, 1), (dev_s, 0), (dev_d, 1), (dev_d, 0))
    send = (same(span(t, 0, z), of.at[0], oa.at[0], dev_f), same(span(t, 1, z), of.at[1], oa.at[1], dev_s),
            same(span(t, 1, z), of.at[2], oa.at[2], dev_f), same(span(t, 0, z), of.at[3], oa.at[3], dev_s))
    relay = (same(span(dev_s, 1, z), of.at[4], oa.at[4], dev_f), same(span(dev_f, 0, z), of.at[5], oa.at[5], dev_s))
    via_z = [across(span(dev, k, z), oz.at[i], ob.at[i]) for i, (dev, k) in enumerate(from_dev)]
    to_mate = [same(span(dev, k, z), om.at[i], on.at[i], mate) for i, (dev, k) in enumerate(from_dev)]
    to_mate += [same(span(dev, k, 1 - z), om.at[6 + i], on.at[6 + i], mate) for i, (dev, k) in enumerate(from_dev)]
    to_mate.append(same(own_o, om.at[12], on.at[12], mate))

    def take(i, sem, p):
        at = span(from_dev[i][0], from_dev[i][1], p)
        pltpu.make_async_copy(wo.at[at], wo.at[at], sem.at[i]).wait()

    def pass_on(i):
        take(i, oa, z)
        via_z[i].start()
        to_mate[i].start()

    def from_z(i):
        take(i, ob, 1 - z)
        to_mate[6 + i].start()

    for copy in loads:
        copy.wait()
    send[0].start()
    send[2].start()
    to_mate[12].start()

    kv_head = lax.div(t * n_kv, n_tp)
    nd = 256

    @pl.loop(0, width // nd)
    def _(b):
        to = pl.ds(pl.multiple_of(b * nd, nd), nd)
        wide[pl.ds(0, heads * nd), :] = wq[pl.ds(pl.multiple_of(b * heads * nd, nd), heads * nd), :].astype(F32)
        for h in range(heads):
            w_all[to, h * head_dim:(h + 1) * head_dim] = wide[pl.ds(h, nd, stride=heads), :].astype(BF16)
        wide[pl.ds(0, 2 * n_kv * nd), :] = wkv[pl.ds(pl.multiple_of(b * 2 * n_kv * nd, nd), 2 * n_kv * nd), :].astype(F32)
        for h in range(2):
            w_all[to, (heads + h) * head_dim:(heads + h + 1) * head_dim] = wide[pl.ds(h * n_kv + kv_head, nd, stride=2 * n_kv), :].astype(BF16)

    def block_of(i):
        w = lax.div(i, 2)
        j = lax.rem(i, 2)
        core = c + j - 2 * c * j
        one = lax.rem(lax.div(w + 1, 2), 2)
        two = lax.div(w, 2)
        flip_x = one + core * (two - one)
        flip_y = two + core * (one - two)
        return (2 * (yy + flip_y - 2 * yy * flip_y) + xx + flip_x - 2 * xx * flip_x) * 2 + core

    def project(i):
        block = block_of(i)
        proj = jnp.dot(xbuf[lax.div(i, 2), lax.rem(i, 2)], w_all[...], preferred_element_type=F32)
        cos_n, sin_n = near_ref[0], near_ref[1]
        for k in range(2):
            piece = block * 2 + k
            at = pl.ds(pl.multiple_of(piece * half, half), half)
            part = proj[k * half:(k + 1) * half]
            cos_f, sin_f = far_ref[0, pl.ds(piece, 1), :], far_ref[1, pl.ds(piece, 1), :]
            cos_b = cos_f * cos_n - sin_f * sin_n
            sin_b = sin_f * cos_n + cos_f * sin_n
            for h in range(heads + 1):
                at_h = slice(h * head_dim, (h + 1) * head_dim)
                v = part[:, at_h]
                qkv_ref[at, at_h] = (v * cos_b + pltpu.roll(v, head_dim // 2, 1) * sin_b).astype(BF16)
            at_h = slice((heads + 1) * head_dim, (heads + 2) * head_dim)
            qkv_ref[at, at_h] = part[:, at_h].astype(BF16)
        stat[i] = jnp.where(lax.rem(lax.broadcasted_iota(jnp.int32, (rows, head_dim), 1), 2) == 0, -jnp.inf, 0.0)
        total[i] = jnp.zeros((heads, rows, head_dim), F32)

    scale = math.log2(math.e) / math.sqrt(head_dim)

    def tile(i, q_block, k_block, masked):
        q_at = pl.ds(pl.multiple_of(q_block * rows, rows), rows)
        k_at = pl.ds(pl.multiple_of(k_block * rows, rows), rows)
        k_blk = qkv_ref[k_at, heads * head_dim:(heads + 1) * head_dim]
        v_blk = qkv_ref[k_at, (heads + 1) * head_dim:(heads + 2) * head_dim]
        for h in range(heads):
            s = lax.dot_general(qkv_ref[q_at, h * head_dim:(h + 1) * head_dim], k_blk, (((1,), (1,)), ((), ())), preferred_element_type=F32)
            if masked:
                s = jnp.where(lax.broadcasted_iota(jnp.int32, (rows, rows), 0) >= lax.broadcasted_iota(jnp.int32, (rows, rows), 1), s, -jnp.inf)
            m = stat[i, :, 2 * h:2 * h + 1]
            m_new = jnp.maximum(m, jnp.max(s, axis=-1, keepdims=True))
            p = jnp.exp2((s - m_new) * scale)
            alpha = jnp.exp2((m - m_new) * scale)
            stat[i, :, 2 * h:2 * h + 1] = m_new
            stat[i, :, 2 * h + 1:2 * h + 2] = stat[i, :, 2 * h + 1:2 * h + 2] * alpha + jnp.sum(p, axis=-1, keepdims=True)
            total[i, h] = total[i, h] * alpha + jnp.dot(p.astype(BF16), v_blk, preferred_element_type=F32)

    def ctx_send(i, dev):
        return rcopy(ctx_out.at[i], ctx.at[:, own_o], cs.at[i], cr.at[t], dev)

    def second_sends():
        send[1].start()
        send[3].start()

    @pl.loop(0, 4)
    def _(w):
        @pl.when(w >= 1)
        def _():
            gather.arrive(w, second_sends)

        @pl.when(w == 2)
        def _():
            take(0, oa, z)
            relay[1].start()
            via_z[0].start()
            to_mate[0].start()
            pass_on(2)

        @pl.when(w == 3)
        def _():
            take(1, oa, z)
            relay[0].start()
            via_z[1].start()
            to_mate[1].start()
            pass_on(3)
            from_z(0)
            from_z(2)

        @pl.loop(0, 2)
        def _(j):
            @pl.when(j == 1)
            def _():
                gather.forward(w).wait_recv()
            project(2 * w + j)
        count = 2 * w + 2

        @pl.loop(0, count)
        def _(n):
            i = lax.rem(n + 1, count)
            q_block = block_of(i)

            @pl.when((w == 3) & (n == 3))
            def _():
                pass_on(4)
                pass_on(5)

            @pl.when((w == 3) & (n == 5))
            def _():
                from_z(1)
                from_z(3)

            def one_tile(k, _):
                k_block = block_of(k)

                @pl.when(k_block < q_block)
                def _():
                    tile(i, q_block, k_block, False)

                @pl.when(k_block == q_block)
                def _():
                    tile(i, q_block, k_block, True)
                return 0

            lax.fori_loop(jnp.where(i >= 2 * w, 0, 2 * w), count, one_tile, 0)

            @pl.when(w == 3)
            def _():
                for h in range(heads):
                    ctx_out[i, :, h * head_dim:(h + 1) * head_dim] = (total[i, h] / stat[i, :, 2 * h + 1:2 * h + 2]).astype(BF16)

                @pl.when(i >= 1)
                def _():
                    ctx_send(i, q_block).start()

    from_z(4)
    from_z(5)
    ctx[:, own_o] = ctx_out[0]
    for copy in to_mate:
        copy.wait_recv()
    for dev in others:
        at = pl.ds(pl.multiple_of(dev * cols, cols), cols)
        pltpu.make_async_copy(ctx_out.at[0], ctx.at[:, at], cr.at[dev]).wait()
    nc = 512
    outs = []
    for n in range(width // nc):
        at = pl.ds(n * nc, nc)
        res[:, at] = rin[:, at].astype(F32) + jnp.dot(ctx[...], wo[:, at], preferred_element_type=F32)
        outs.append(pltpu.make_async_copy(res.at[:, at], out_hbm.at[:, at], es.at[n]))
        outs[n].start()
    gather.finish()
    for copy in list(send + relay) + via_z + to_mate:
        copy.wait_send()
    for i in range(1, n_tp):
        ctx_send(i, mate).wait_send()
    for copy in outs:
        copy.wait()


def attention(layer, resid, gain, far, near, w_q, w_kv, w_o, n_tp):
    rows, width = resid.shape
    cols, head_dim = w_o.shape[1], w_q.shape[2]
    heads = cols // head_dim
    n_kv = w_kv.shape[1] // (2 * width)
    seq = rows * n_tp
    vmem = pl.BlockSpec(memory_space=pltpu.VMEM)
    anywhere = pl.BlockSpec(memory_space=pl.ANY)
    dma = pltpu.SemaphoreType.DMA
    return pl.pallas_call(
        functools.partial(attn_kernel, layer, n_tp, n_kv, heads, head_dim),
        out_shape=jax.ShapeDtypeStruct((rows, width), F32),
        in_specs=[anywhere, vmem, vmem, vmem, anywhere, anywhere, anywhere],
        out_specs=anywhere,
        scratch_shapes=[
            pltpu.VMEM((4, 2, rows, width), BF16),
            pltpu.VMEM((rows, width), resid.dtype),
            pltpu.VMEM(w_q.shape[1:], BF16),
            pltpu.VMEM(w_kv.shape[1:], BF16),
            pltpu.VMEM((256 * max(heads, 2 * n_kv), head_dim), F32),
            pltpu.VMEM((width, cols + 2 * head_dim), BF16),
            pltpu.VMEM((seq, cols + 2 * head_dim), BF16),
            pltpu.VMEM((n_tp * cols, width), BF16),
            pltpu.VMEM((rows, n_tp * cols), BF16),
            pltpu.VMEM((n_tp, rows, cols), BF16),
            pltpu.VMEM((rows, width), F32),
            pltpu.VMEM((n_tp, rows, head_dim), F32),
            pltpu.VMEM((n_tp, heads, rows, head_dim), F32),
            dma((4,)), dma((6,)), dma((4, 2)), dma((4,)), dma((4,)), dma((6,)), dma((6,)), dma((6,)), dma((6,)), dma((13,)), dma((13,)), dma((n_tp,)), dma((n_tp,)), dma((4,)),
        ],
        compiler_params=pltpu.CompilerParams(collective_id=1 + layer, has_side_effects=True, vmem_limit_bytes=VMEM_MAX),
        cost_estimate=pl.CostEstimate(flops=2 * seq * seq * cols, bytes_accessed=4 * seq * cols, transcendentals=seq * seq),
        name="attention" + str(layer),
    )(resid, gain, far, near, w_q, w_kv, w_o)


def mlp_kernel(layer, r_hbm, gain_ref, wg_hbm, wu_hbm, wd_hbm, out_hbm,
               wg, wu, wd, xbuf, prec, recv, acc, stash, act,
               lsem, sx, sy, ag, fs, fr, ps, pr, rr, ss):
    _, _, partners = coords()
    mate, dev_x, dev_y = partners
    rows, width = acc.shape
    half = rows // 2
    hid = act.shape[1]
    h0, h1 = pl.ds(0, half), pl.ds(half, half)
    hs = (h0, h1)
    nb = 64

    load_r = pltpu.make_async_copy(r_hbm, acc, lsem.at[0])
    load_r.start()
    greet(partners)
    loads = [pltpu.make_async_copy(src.at[layer], dst, lsem.at[k + 1]) for k, (src, dst) in enumerate(((wg_hbm, wg), (wu_hbm, wu), (wd_hbm, wd)))]
    load_r.wait()
    for copy in loads:
        copy.start()
    gather = RowGather(xbuf, sx, sy, ag, fs, fr, partners)
    gather.start(lambda k: norm_rows(acc, gain_ref, xbuf.at[0, 0], k * half, half))

    def partial_send(w):
        return rcopy(xbuf.at[w, 1], prec.at[w], ps.at[w], pr.at[w], mate)

    stage = (rcopy(xbuf.at[1, 1, h0], recv.at[0], ss.at[0], rr.at[0], dev_x),
             rcopy(xbuf.at[1, 1, h1], recv.at[1], ss.at[1], rr.at[1], dev_y),
             rcopy(xbuf.at[2, 1, h0], recv.at[2], ss.at[2], rr.at[2], dev_x),
             rcopy(xbuf.at[2, 1, h1], recv.at[3], ss.at[3], rr.at[3], dev_y),
             rcopy(xbuf.at[3, 1, h0], recv.at[4], ss.at[4], rr.at[4], dev_y),
             rcopy(xbuf.at[3, 1, h1], recv.at[5], ss.at[5], rr.at[5], dev_x))

    for copy in loads:
        copy.wait()
    cut = 768
    nd = 1024

    def gate_up(x_at, at):
        g = lax.dot_general(x_at[...], wg[at, :], (((1,), (1,)), ((), ())), preferred_element_type=F32)
        u = lax.dot_general(x_at[...], wu[at, :], (((1,), (1,)), ((), ())), preferred_element_type=F32)
        act[:, at] = (g * jax.nn.sigmoid(g) * u).astype(BF16)

    @pl.loop(0, 8)
    def _(s):
        w = lax.div(s, 2)
        rc = 1 - lax.rem(s, 2)

        @pl.when(rc == 1)
        def _():
            gather.forward(w).wait_recv()
        x_at = xbuf.at[w, rc]
        gate_up(x_at, pl.ds(0, cut))
        gate_up(x_at, pl.ds(cut, hid - cut))

        @pl.when(rc == 0)
        def _():
            @pl.when(w < 3)
            def _():
                gather.arrive(w + 1)
            partial_send(w).wait()

        @pl.loop(0, width // nd)
        def _(n):
            at = pl.ds(pl.multiple_of(n * nd, nd), nd)
            val = jnp.dot(act[...], wd[:, at], preferred_element_type=F32)

            @pl.when(rc == 1)
            def _():
                xbuf[w, 1, :, at] = val.astype(BF16)

            @pl.when(rc == 0)
            def _():
                total = val + prec[w, :, at].astype(F32)

                @pl.when(w == 0)
                def _():
                    acc[:, at] = acc[:, at] + total

                @pl.when(w == 3)
                def _():
                    stash[:, at] = total

                @pl.when((w == 1) | (w == 2))
                def _():
                    xbuf[w, 1, :, at] = total.astype(BF16)

        @pl.when(rc == 1)
        def _():
            partial_send(w).start()

        @pl.when(s == 3)
        def _():
            stage[0].start()
            stage[1].start()

        @pl.when(s == 5)
        def _():
            stage[2].start()
            stage[3].start()

    def blocks_of(k):
        def each(fn):
            @pl.loop(0, half // nb)
            def _(b):
                fn(pl.ds(pl.multiple_of(b * nb, nb), nb), pl.ds(pl.multiple_of(k * half + b * nb, nb), nb))
        return each

    for k in range(2):
        stage[k].wait_recv()

        @blocks_of(k)
        def _(at, to):
            acc[to, :] = acc[to, :] + recv[k, at, :].astype(F32)
    for k in range(2):
        stage[2 + k].wait_recv()

        @blocks_of(k)
        def _(at, to):
            xbuf[3, 1, to, :] = (stash[to, :] + recv[2 + k, at, :].astype(F32)).astype(BF16)
        stage[4 + k].start()
    gather.finish()
    narrow = out_hbm.dtype == BF16
    final = xbuf.at[0, 0] if narrow else acc
    outs = []
    for k in range(2):
        stage[4 + k].wait_recv()

        @blocks_of(k)
        def _(at, to):
            final[to, :] = (acc[to, :] + recv[4 + k, at, :].astype(F32)).astype(final.dtype)
        outs.append(pltpu.make_async_copy(final.at[hs[k]], out_hbm.at[hs[k]], lsem.at[k]))
        outs[k].start()
    for copy in stage:
        copy.wait_send()
    for copy in outs:
        copy.wait()


def mlp(layer, resid, gain, w_gate, w_up, w_down, out_dtype):
    rows, width = resid.shape
    hid = w_gate.shape[1]
    half = rows // 2
    any_spec = pl.BlockSpec(memory_space=pl.ANY)
    dma = pltpu.SemaphoreType.DMA
    return pl.pallas_call(
        functools.partial(mlp_kernel, layer),
        out_shape=jax.ShapeDtypeStruct((rows, width), out_dtype),
        in_specs=[any_spec, pl.BlockSpec(memory_space=pltpu.VMEM), any_spec, any_spec, any_spec],
        out_specs=any_spec,
        scratch_shapes=[
            pltpu.VMEM((hid, width), BF16),
            pltpu.VMEM((hid, width), BF16),
            pltpu.VMEM((hid, width), BF16),
            pltpu.VMEM((4, 2, rows, width), BF16),
            pltpu.VMEM((4, rows, width), BF16),
            pltpu.VMEM((6, half, width), BF16),
            pltpu.VMEM((rows, width), F32),
            pltpu.VMEM((rows, width), F32),
            pltpu.VMEM((rows, hid), BF16),
            dma((4,)),
        ] + gather_sems() + [dma((4,)), dma((4,)), dma((6,)), dma((6,))],
        compiler_params=pltpu.CompilerParams(collective_id=5 + layer, has_side_effects=True, vmem_limit_bytes=VMEM_MAX),
        cost_estimate=pl.CostEstimate(flops=6 * 8 * rows * width * hid, bytes_accessed=6 * width * hid, transcendentals=8 * rows * hid),
        name="mlp" + str(layer),
    )(resid, gain, w_gate, w_up, w_down)


def solution(mesh):
    n_tp = mesh.shape['tp']
    tok_spec = P('dp', 'tp', None)
    in_specs = (tok_spec, P(), P(None, None, 'tp', None), P(), P(None, 'tp', None, None), P(), P(None, None, 'tp'), P(None, None, 'tp'), P(None, 'tp', None))

    def body(hidden, norm_attn, w_q, w_kv, w_o, norm_mlp, w_gate, w_up, w_down):
        n_layers, width, heads, head_dim = w_q.shape
        n_kv = w_kv.shape[3]
        rows = hidden.shape[1]
        far, near = rope_tables(rows * n_tp, rows // 2, head_dim)
        w_q = w_q.reshape(n_layers, width * heads, head_dim)
        w_kv = w_kv.reshape(n_layers, width * 2 * n_kv, head_dim)
        w_o = w_o.reshape(n_layers, heads * head_dim, width)
        w_gate = jnp.swapaxes(w_gate, 1, 2)
        w_up = jnp.swapaxes(w_up, 1, 2)
        resid = hidden[0]
        for layer in range(n_layers):
            resid = attention(layer, resid, norm_attn[layer][None], far, near, w_q, w_kv, w_o, n_tp)
            resid = mlp(layer, resid, norm_mlp[layer][None], w_gate, w_up, w_down, BF16 if layer == n_layers - 1 else F32)
        return resid[None]

    return jax.shard_map(body, mesh=mesh, in_specs=in_specs, out_specs=tok_spec, check_vma=False)
```

```python
import functools
import math
import jax
import jax.numpy as jnp
import numpy as np
from jax import lax
from jax.experimental import pallas as pl
from jax.experimental.pallas import tpu as pltpu
from jax.sharding import PartitionSpec as P

EPS = 1e-5
ROPE_BASE = 10000.0
MESH = pl.DeviceIdType.MESH
VMEM_MAX = 67043328
F32 = jnp.float32
BF16 = jnp.bfloat16


def rope_tables(seq, step, head_dim):
    half_dim = head_dim // 2
    inv_freq = ROPE_BASE ** (-2.0 * np.arange(half_dim, dtype=np.float64) / head_dim)

    def table(positions):
        angles = positions.astype(np.float64)[:, None] * inv_freq[None, :]
        cos_t, sin_t = np.cos(angles), np.sin(angles)
        return np.stack([np.concatenate([cos_t, cos_t], axis=1), np.concatenate([-sin_t, sin_t], axis=1)]).astype(np.float32)

    return table(np.arange(0, seq, step)), table(np.arange(step))


def coords():
    t = lax.axis_index('tp')
    c = lax.rem(t, 2)
    xx = lax.rem(lax.div(t, 2), 2)
    yy = lax.div(t, 4)
    return t, (yy, xx, c), (t + 1 - 2 * c, t + 2 - 4 * xx, t + 4 - 8 * yy)


def rcopy(src, dst, ssem, rsem, dev):
    return pltpu.make_async_remote_copy(src_ref=src, dst_ref=dst, send_sem=ssem, recv_sem=rsem,
                                        device_id={'tp': dev}, device_id_type=MESH)


def greet(devices):
    for dev in devices:
        pl.semaphore_signal(pltpu.get_barrier_semaphore(), inc=1, device_id={'tp': dev}, device_id_type=MESH)


class RowGather:
    def __init__(self, xbuf, sx, sy, ag, fs, fr, partners):
        mate, dev_x, dev_y = partners
        rows = xbuf.shape[2]
        half = rows // 2
        lead = half // 4
        h0, h1 = pl.ds(0, half), pl.ds(half, half)
        own = xbuf.at[0, 0]
        self.xbuf, self.ag, self.fs, self.fr, self.mate = xbuf, ag, fs, fr, mate
        self.halves = (h0, h1)

        def piece(k, sem, dev, first, size, window, slot):
            at = pl.ds(first, size)
            return rcopy(own.at[at], xbuf.at[window, 0, at], sem.at[k], ag.at[window, slot], dev)

        self.first = (piece(0, sx, dev_x, 0, half, 1, 0), piece(0, sy, dev_y, half, half, 1, 1))
        self.lead = (piece(1, sx, dev_x, half, lead, 3, 1), piece(1, sy, dev_y, 0, lead, 3, 0))
        self.rest = (piece(2, sx, dev_x, half + lead, half - lead, 3, 1), piece(2, sy, dev_y, lead, half - lead, 3, 0))
        self.relay = (rcopy(xbuf.at[1, 0, h1], xbuf.at[2, 0, h1], sx.at[3], ag.at[2, 1], dev_x),
                      rcopy(xbuf.at[1, 0, h0], xbuf.at[2, 0, h0], sy.at[3], ag.at[2, 0], dev_y))

    def forward(self, w):
        return rcopy(self.xbuf.at[w, 0], self.xbuf.at[w, 1], self.fs.at[w], self.fr.at[w], self.mate)

    def start(self, norm_half):
        norm_half(0)
        pl.semaphore_wait(pltpu.get_barrier_semaphore(), 3)
        self.first[0].start()
        norm_half(1)
        self.first[1].start()
        self.lead[0].start()
        self.lead[1].start()
        self.forward(0).start()

    def arrive(self, w):
        for k in range(2):
            at = self.halves[k]
            pltpu.make_async_copy(self.xbuf.at[0, 0, at], self.xbuf.at[w, 0, at], self.ag.at[w, k]).wait()

        @pl.when(w == 1)
        def _():
            for copy in self.relay + self.rest:
                copy.start()
        self.forward(w).start()

    def finish(self):
        for copy in self.first + self.lead + self.relay + self.rest:
            copy.wait_send()
        for w in range(4):
            self.forward(w).wait_send()


def gather_sems():
    dma = pltpu.SemaphoreType.DMA
    return [dma((4,)), dma((4,)), dma((4, 2)), dma((4,)), dma((4,))]


def norm_rows(src, gain_ref, dst, first, count):
    nb = 64

    @pl.loop(0, count // nb)
    def _(b):
        at = pl.ds(pl.multiple_of(first + b * nb, nb), nb)
        r = src[at, :].astype(F32)
        mean_sq = jnp.mean(r * r, axis=-1, keepdims=True)
        dst[at, :] = (r * lax.rsqrt(mean_sq + EPS) * gain_ref[...]).astype(BF16)


class BlockGather:
    def __init__(self, xbuf, sf, ag, fs, fr, mate, dev_f, dev_s):
        rows = xbuf.shape[2]
        half = rows // 2
        self.halves = (pl.ds(0, half), pl.ds(half, half))
        self.xbuf, self.ag, self.fs, self.fr, self.mate = xbuf, ag, fs, fr, mate

        def copies(source, target, sem, dev):
            return [rcopy(xbuf.at[source, 0, at], xbuf.at[target, 0, at], sf.at[sem + k], ag.at[target, k], dev)
                    for k, at in enumerate(self.halves)]

        self.first = copies(0, 1, 0, dev_f)
        self.relay = copies(1, 2, 2, dev_s)
        self.second = copies(0, 3, 4, dev_s)

    def forward(self, w):
        return rcopy(self.xbuf.at[w, 0], self.xbuf.at[w, 1], self.fs.at[w], self.fr.at[w], self.mate)

    def arrive(self, w, between):
        for k, at in enumerate(self.halves):
            pltpu.make_async_copy(self.xbuf.at[0, 0, at], self.xbuf.at[w, 0, at], self.ag.at[w, k]).wait()

            @pl.when(w == 1)
            def _():
                self.relay[k].start()
        self.forward(w).start()

        @pl.when(w == 1)
        def _():
            between()
            for copy in self.second:
                copy.start()

    def finish(self):
        for copy in self.first + self.relay + self.second:
            copy.wait_send()
        for w in range(4):
            self.forward(w).wait_send()


def attn_kernel(layer, n_tp, n_kv, heads, head_dim, r_hbm, gain_ref, far_ref, near_ref, wq_hbm, wkv_hbm, wo_hbm, out_hbm,
                xbuf, rin, wq, wkv, wide, w_all, qkv_ref, wo, ctx, ctx_out, res, stat, total,
                lsem, sf, ag, fs, fr, of, oz, oa, ob, om, on, cs, cr, es):
    t, (yy, xx, c), (mate, dev_x, dev_y) = coords()
    z = lax.axis_index('dp')
    dev_d = dev_x + dev_y - t
    dev_f = dev_x + c * (dev_y - dev_x)
    dev_s = dev_y + c * (dev_x - dev_y)
    rows, width = res.shape
    half = rows // 2
    cols = heads * head_dim

    load_r = pltpu.make_async_copy(r_hbm, rin, lsem.at[0])
    load_r.start()
    others = [lax.rem(t + k, n_tp) for k in range(1, n_tp)]
    greet(others)
    pl.semaphore_signal(pltpu.get_barrier_semaphore(), inc=1, device_id={'dp': 1 - z, 'tp': t}, device_id_type=MESH)
    own_o = pl.ds(pl.multiple_of(t * cols, cols), cols)
    loads = (pltpu.make_async_copy(wo_hbm.at[layer], wo.at[own_o], lsem.at[3]),
             pltpu.make_async_copy(wq_hbm.at[layer], wq, lsem.at[1]),
             pltpu.make_async_copy(wkv_hbm.at[layer], wkv, lsem.at[2]))
    load_r.wait()
    for copy in loads:
        copy.start()
    gather = BlockGather(xbuf, sf, ag, fs, fr, mate, dev_f, dev_s)
    norm_rows(rin, gain_ref, xbuf.at[0, 0], 0, half)
    pl.semaphore_wait(pltpu.get_barrier_semaphore(), n_tp)
    gather.first[0].start()
    norm_rows(rin, gain_ref, xbuf.at[0, 0], half, half)
    gather.first[1].start()
    gather.forward(0).start()

    part_rows = head_dim // 2

    def span(dev, k, p):
        return pl.ds(pl.multiple_of(dev * cols + k * head_dim + p * part_rows, part_rows), part_rows)

    def same(at, ssem, rsem, dev):
        return rcopy(wo.at[at], wo.at[at], ssem, rsem, dev)

    def across(at, ssem, rsem):
        return pltpu.make_async_remote_copy(src_ref=wo.at[at], dst_ref=wo.at[at], send_sem=ssem, recv_sem=rsem,
                                            device_id={'dp': 1 - z, 'tp': t}, device_id_type=MESH)

    from_dev = ((dev_f, 0), (dev_s, 1), (dev_f, 1), (dev_s, 0), (dev_d, 1), (dev_d, 0))
    send = (same(span(t, 0, z), of.at[0], oa.at[0], dev_f), same(span(t, 1, z), of.at[1], oa.at[1], dev_s),
            same(span(t, 1, z), of.at[2], oa.at[2], dev_f), same(span(t, 0, z), of.at[3], oa.at[3], dev_s))
    relay = (same(span(dev_s, 1, z), of.at[4], oa.at[4], dev_f), same(span(dev_f, 0, z), of.at[5], oa.at[5], dev_s))
    via_z = [across(span(dev, k, z), oz.at[i], ob.at[i]) for i, (dev, k) in enumerate(from_dev)]
    to_mate = [same(span(dev, k, z), om.at[i], on.at[i], mate) for i, (dev, k) in enumerate(from_dev)]
    to_mate += [same(span(dev, k, 1 - z), om.at[6 + i], on.at[6 + i], mate) for i, (dev, k) in enumerate(from_dev)]
    to_mate.append(same(own_o, om.at[12], on.at[12], mate))

    def take(i, sem, p):
        at = span(from_dev[i][0], from_dev[i][1], p)
        pltpu.make_async_copy(wo.at[at], wo.at[at], sem.at[i]).wait()

    def pass_on(i):
        take(i, oa, z)
        via_z[i].start()
        to_mate[i].start()

    def from_z(i):
        take(i, ob, 1 - z)
        to_mate[6 + i].start()

    for copy in loads:
        copy.wait()
    send[0].start()
    send[2].start()
    to_mate[12].start()

    kv_head = lax.div(t * n_kv, n_tp)
    nd = 256

    @pl.loop(0, width // nd)
    def _(b):
        to = pl.ds(pl.multiple_of(b * nd, nd), nd)
        wide[pl.ds(0, heads * nd), :] = wq[pl.ds(pl.multiple_of(b * heads * nd, nd), heads * nd), :].astype(F32)
        for h in range(heads):
            w_all[to, h * head_dim:(h + 1) * head_dim] = wide[pl.ds(h, nd, stride=heads), :].astype(BF16)
        wide[pl.ds(0, 2 * n_kv * nd), :] = wkv[pl.ds(pl.multiple_of(b * 2 * n_kv * nd, nd), 2 * n_kv * nd), :].astype(F32)
        for h in range(2):
            w_all[to, (heads + h) * head_dim:(heads + h + 1) * head_dim] = wide[pl.ds(h * n_kv + kv_head, nd, stride=2 * n_kv), :].astype(BF16)

    def block_of(i):
        w = lax.div(i, 2)
        j = lax.rem(i, 2)
        core = c + j - 2 * c * j
        one = lax.rem(lax.div(w + 1, 2), 2)
        two = lax.div(w, 2)
        flip_x = one + core * (two - one)
        flip_y = two + core * (one - two)
        return (2 * (yy + flip_y - 2 * yy * flip_y) + xx + flip_x - 2 * xx * flip_x) * 2 + core

    def project(i):
        block = block_of(i)
        proj = jnp.dot(xbuf[lax.div(i, 2), lax.rem(i, 2)], w_all[...], preferred_element_type=F32)
        cos_n, sin_n = near_ref[0], near_ref[1]
        for k in range(2):
            piece = block * 2 + k
            at = pl.ds(pl.multiple_of(piece * half, half), half)
            part = proj[k * half:(k + 1) * half]
            cos_f, sin_f = far_ref[0, pl.ds(piece, 1), :], far_ref[1, pl.ds(piece, 1), :]
            cos_b = cos_f * cos_n - sin_f * sin_n
            sin_b = sin_f * cos_n + cos_f * sin_n
            for h in range(heads + 1):
                at_h = slice(h * head_dim, (h + 1) * head_dim)
                v = part[:, at_h]
                qkv_ref[at, at_h] = (v * cos_b + pltpu.roll(v, head_dim // 2, 1) * sin_b).astype(BF16)
            at_h = slice((heads + 1) * head_dim, (heads + 2) * head_dim)
            qkv_ref[at, at_h] = part[:, at_h].astype(BF16)
        stat[i] = jnp.where(lax.rem(lax.broadcasted_iota(jnp.int32, (2 * heads, rows), 0), 2) == 0, -jnp.inf, 0.0)
        total[i] = jnp.zeros((heads, head_dim, rows), F32)

    scale = math.log2(math.e) / math.sqrt(head_dim)

    def tile(i, q_block, k_block, masked):
        q_at = pl.ds(pl.multiple_of(q_block * rows, rows), rows)
        k_at = pl.ds(pl.multiple_of(k_block * rows, rows), rows)
        k_blk = qkv_ref[k_at, heads * head_dim:(heads + 1) * head_dim]
        v_blk = qkv_ref[k_at, (heads + 1) * head_dim:(heads + 2) * head_dim]
        qs = [qkv_ref[q_at, h * head_dim:(h + 1) * head_dim] for h in range(heads)]
        old = [(stat[i, 2 * h:2 * h + 1, :], stat[i, 2 * h + 1:2 * h + 2, :], total[i, h]) for h in range(heads)]
        out = []
        for h in range(heads):
            m, l, acc = old[h]
            s = lax.dot_general(k_blk, qs[h], (((1,), (1,)), ((), ())), preferred_element_type=F32)
            if masked:
                s = jnp.where(lax.broadcasted_iota(jnp.int32, (rows, rows), 0) <= lax.broadcasted_iota(jnp.int32, (rows, rows), 1), s, -jnp.inf)
            m_new = jnp.maximum(m, jnp.max(s, axis=0, keepdims=True))
            p = jnp.exp2((s - m_new) * scale)
            alpha = jnp.exp2((m - m_new) * scale)
            l = l * alpha + jnp.sum(p, axis=0, keepdims=True)
            acc = acc * alpha + lax.dot_general(v_blk, p.astype(BF16), (((0,), (0,)), ((), ())), preferred_element_type=F32)
            out.append((m_new, l, acc))
        for h in range(heads):
            stat[i, 2 * h:2 * h + 1, :], stat[i, 2 * h + 1:2 * h + 2, :], total[i, h] = out[h]

    def ctx_send(i, dev):
        return rcopy(ctx_out.at[i], ctx.at[:, own_o], cs.at[i], cr.at[t], dev)

    def second_sends():
        send[1].start()
        send[3].start()

    @pl.loop(0, 4)
    def _(w):
        @pl.when(w >= 1)
        def _():
            gather.arrive(w, second_sends)

        @pl.when(w == 2)
        def _():
            take(0, oa, z)
            relay[1].start()
            via_z[0].start()
            to_mate[0].start()
            pass_on(2)

        @pl.when(w == 3)
        def _():
            take(1, oa, z)
            relay[0].start()
            via_z[1].start()
            to_mate[1].start()
            pass_on(3)
            from_z(0)
            from_z(2)

        @pl.loop(0, 2)
        def _(j):
            @pl.when(j == 1)
            def _():
                gather.forward(w).wait_recv()
            project(2 * w + j)
        count = 2 * w + 2

        @pl.loop(0, count)
        def _(n):
            i = lax.rem(n + 1, count)
            q_block = block_of(i)

            @pl.when((w == 3) & (n == 3))
            def _():
                pass_on(4)
                pass_on(5)

            @pl.when((w == 3) & (n == 5))
            def _():
                from_z(1)
                from_z(3)

            def one_tile(k, _):
                k_block = block_of(k)

                @pl.when(k_block < q_block)
                def _():
                    tile(i, q_block, k_block, False)

                @pl.when(k_block == q_block)
                def _():
                    tile(i, q_block, k_block, True)
                return 0

            lax.fori_loop(jnp.where(i >= 2 * w, 0, 2 * w), count, one_tile, 0)

            @pl.when(w == 3)
            def _():
                for h in range(heads):
                    ctx_out[i, :, h * head_dim:(h + 1) * head_dim] = (total[i, h] / stat[i, 2 * h + 1:2 * h + 2, :]).T.astype(BF16)

                @pl.when(i >= 1)
                def _():
                    ctx_send(i, q_block).start()

    from_z(4)
    from_z(5)
    ctx[:, own_o] = ctx_out[0]
    for copy in to_mate:
        copy.wait_recv()
    for dev in others:
        at = pl.ds(pl.multiple_of(dev * cols, cols), cols)
        pltpu.make_async_copy(ctx_out.at[0], ctx.at[:, at], cr.at[dev]).wait()
    nc = 512
    outs = []
    for n in range(width // nc):
        at = pl.ds(n * nc, nc)
        res[:, at] = rin[:, at].astype(F32) + jnp.dot(ctx[...], wo[:, at], preferred_element_type=F32)
        outs.append(pltpu.make_async_copy(res.at[:, at], out_hbm.at[:, at], es.at[n]))
        outs[n].start()
    gather.finish()
    for copy in list(send + relay) + via_z + to_mate:
        copy.wait_send()
    for i in range(1, n_tp):
        ctx_send(i, mate).wait_send()
    for copy in outs:
        copy.wait()


def attention(layer, resid, gain, far, near, w_q, w_kv, w_o, n_tp):
    rows, width = resid.shape
    cols, head_dim = w_o.shape[1], w_q.shape[2]
    heads = cols // head_dim
    n_kv = w_kv.shape[1] // (2 * width)
    seq = rows * n_tp
    vmem = pl.BlockSpec(memory_space=pltpu.VMEM)
    anywhere = pl.BlockSpec(memory_space=pl.ANY)
    dma = pltpu.SemaphoreType.DMA
    return pl.pallas_call(
        functools.partial(attn_kernel, layer, n_tp, n_kv, heads, head_dim),
        out_shape=jax.ShapeDtypeStruct((rows, width), F32),
        in_specs=[anywhere, vmem, vmem, vmem, anywhere, anywhere, anywhere],
        out_specs=anywhere,
        scratch_shapes=[
            pltpu.VMEM((4, 2, rows, width), BF16),
            pltpu.VMEM((rows, width), resid.dtype),
            pltpu.VMEM(w_q.shape[1:], BF16),
            pltpu.VMEM(w_kv.shape[1:], BF16),
            pltpu.VMEM((256 * max(heads, 2 * n_kv), head_dim), F32),
            pltpu.VMEM((width, cols + 2 * head_dim), BF16),
            pltpu.VMEM((seq, cols + 2 * head_dim), BF16),
            pltpu.VMEM((n_tp * cols, width), BF16),
            pltpu.VMEM((rows, n_tp * cols), BF16),
            pltpu.VMEM((n_tp, rows, cols), BF16),
            pltpu.VMEM((rows, width), F32),
            pltpu.VMEM((n_tp, 2 * heads, rows), F32),
            pltpu.VMEM((n_tp, heads, head_dim, rows), F32),
            dma((4,)), dma((6,)), dma((4, 2)), dma((4,)), dma((4,)), dma((6,)), dma((6,)), dma((6,)), dma((6,)), dma((13,)), dma((13,)), dma((n_tp,)), dma((n_tp,)), dma((4,)),
        ],
        compiler_params=pltpu.CompilerParams(collective_id=1 + layer, has_side_effects=True, vmem_limit_bytes=VMEM_MAX),
        cost_estimate=pl.CostEstimate(flops=2 * seq * seq * cols, bytes_accessed=4 * seq * cols, transcendentals=seq * seq),
        name="attention" + str(layer),
    )(resid, gain, far, near, w_q, w_kv, w_o)


def mlp_kernel(layer, r_hbm, gain_ref, wg_hbm, wu_hbm, wd_hbm, out_hbm,
               wg, wu, wd, xbuf, prec, recv, acc, stash, act,
               lsem, sx, sy, ag, fs, fr, ps, pr, rr, ss):
    _, _, partners = coords()
    mate, dev_x, dev_y = partners
    rows, width = acc.shape
    half = rows // 2
    hid = act.shape[1]
    h0, h1 = pl.ds(0, half), pl.ds(half, half)
    hs = (h0, h1)
    nb = 64

    load_r = pltpu.make_async_copy(r_hbm, acc, lsem.at[0])
    load_r.start()
    greet(partners)
    loads = [pltpu.make_async_copy(src.at[layer], dst, lsem.at[k + 1]) for k, (src, dst) in enumerate(((wg_hbm, wg), (wu_hbm, wu), (wd_hbm, wd)))]
    load_r.wait()
    for copy in loads:
        copy.start()
    gather = RowGather(xbuf, sx, sy, ag, fs, fr, partners)
    gather.start(lambda k: norm_rows(acc, gain_ref, xbuf.at[0, 0], k * half, half))

    def partial_send(w):
        return rcopy(xbuf.at[w, 1], prec.at[w], ps.at[w], pr.at[w], mate)

    stage = (rcopy(xbuf.at[1, 1, h0], recv.at[0], ss.at[0], rr.at[0], dev_x),
             rcopy(xbuf.at[1, 1, h1], recv.at[1], ss.at[1], rr.at[1], dev_y),
             rcopy(xbuf.at[2, 1, h0], recv.at[2], ss.at[2], rr.at[2], dev_x),
             rcopy(xbuf.at[2, 1, h1], recv.at[3], ss.at[3], rr.at[3], dev_y),
             rcopy(xbuf.at[3, 1, h0], recv.at[4], ss.at[4], rr.at[4], dev_y),
             rcopy(xbuf.at[3, 1, h1], recv.at[5], ss.at[5], rr.at[5], dev_x))

    for copy in loads:
        copy.wait()
    cut = 768
    nd = 1024

    def gate_up(x_at, at):
        g = lax.dot_general(x_at[...], wg[at, :], (((1,), (1,)), ((), ())), preferred_element_type=F32)
        u = lax.dot_general(x_at[...], wu[at, :], (((1,), (1,)), ((), ())), preferred_element_type=F32)
        act[:, at] = (g * jax.nn.sigmoid(g) * u).astype(BF16)

    @pl.loop(0, 8)
    def _(s):
        w = lax.div(s, 2)
        rc = 1 - lax.rem(s, 2)

        @pl.when(rc == 1)
        def _():
            gather.forward(w).wait_recv()
        x_at = xbuf.at[w, rc]
        gate_up(x_at, pl.ds(0, cut))
        gate_up(x_at, pl.ds(cut, hid - cut))

        @pl.when(rc == 0)
        def _():
            @pl.when(w < 3)
            def _():
                gather.arrive(w + 1)
            partial_send(w).wait()

        @pl.loop(0, width // nd)
        def _(n):
            at = pl.ds(pl.multiple_of(n * nd, nd), nd)
            val = jnp.dot(act[...], wd[:, at], preferred_element_type=F32)

            @pl.when(rc == 1)
            def _():
                xbuf[w, 1, :, at] = val.astype(BF16)

            @pl.when(rc == 0)
            def _():
                total = val + prec[w, :, at].astype(F32)

                @pl.when(w == 0)
                def _():
                    acc[:, at] = acc[:, at] + total

                @pl.when(w == 3)
                def _():
                    stash[:, at] = total

                @pl.when((w == 1) | (w == 2))
                def _():
                    xbuf[w, 1, :, at] = total.astype(BF16)

        @pl.when(rc == 1)
        def _():
            partial_send(w).start()

        @pl.when(s == 3)
        def _():
            stage[0].start()
            stage[1].start()

        @pl.when(s == 5)
        def _():
            stage[2].start()
            stage[3].start()

    def blocks_of(k):
        def each(fn):
            @pl.loop(0, half // nb)
            def _(b):
                fn(pl.ds(pl.multiple_of(b * nb, nb), nb), pl.ds(pl.multiple_of(k * half + b * nb, nb), nb))
        return each

    for k in range(2):
        stage[k].wait_recv()

        @blocks_of(k)
        def _(at, to):
            acc[to, :] = acc[to, :] + recv[k, at, :].astype(F32)
    for k in range(2):
        stage[2 + k].wait_recv()

        @blocks_of(k)
        def _(at, to):
            xbuf[3, 1, to, :] = (stash[to, :] + recv[2 + k, at, :].astype(F32)).astype(BF16)
        stage[4 + k].start()
    gather.finish()
    narrow = out_hbm.dtype == BF16
    final = xbuf.at[0, 0] if narrow else acc
    outs = []
    for k in range(2):
        stage[4 + k].wait_recv()

        @blocks_of(k)
        def _(at, to):
            final[to, :] = (acc[to, :] + recv[4 + k, at, :].astype(F32)).astype(final.dtype)
        outs.append(pltpu.make_async_copy(final.at[hs[k]], out_hbm.at[hs[k]], lsem.at[k]))
        outs[k].start()
    for copy in stage:
        copy.wait_send()
    for copy in outs:
        copy.wait()


def mlp(layer, resid, gain, w_gate, w_up, w_down, out_dtype):
    rows, width = resid.shape
    hid = w_gate.shape[1]
    half = rows // 2
    any_spec = pl.BlockSpec(memory_space=pl.ANY)
    dma = pltpu.SemaphoreType.DMA
    return pl.pallas_call(
        functools.partial(mlp_kernel, layer),
        out_shape=jax.ShapeDtypeStruct((rows, width), out_dtype),
        in_specs=[any_spec, pl.BlockSpec(memory_space=pltpu.VMEM), any_spec, any_spec, any_spec],
        out_specs=any_spec,
        scratch_shapes=[
            pltpu.VMEM((hid, width), BF16),
            pltpu.VMEM((hid, width), BF16),
            pltpu.VMEM((hid, width), BF16),
            pltpu.VMEM((4, 2, rows, width), BF16),
            pltpu.VMEM((4, rows, width), BF16),
            pltpu.VMEM((6, half, width), BF16),
            pltpu.VMEM((rows, width), F32),
            pltpu.VMEM((rows, width), F32),
            pltpu.VMEM((rows, hid), BF16),
            dma((4,)),
        ] + gather_sems() + [dma((4,)), dma((4,)), dma((6,)), dma((6,))],
        compiler_params=pltpu.CompilerParams(collective_id=5 + layer, has_side_effects=True, vmem_limit_bytes=VMEM_MAX),
        cost_estimate=pl.CostEstimate(flops=6 * 8 * rows * width * hid, bytes_accessed=6 * width * hid, transcendentals=8 * rows * hid),
        name="mlp" + str(layer),
    )(resid, gain, w_gate, w_up, w_down)


def solution(mesh):
    n_tp = mesh.shape['tp']
    tok_spec = P('dp', 'tp', None)
    in_specs = (tok_spec, P(), P(None, None, 'tp', None), P(), P(None, 'tp', None, None), P(), P(None, None, 'tp'), P(None, None, 'tp'), P(None, 'tp', None))

    def body(hidden, norm_attn, w_q, w_kv, w_o, norm_mlp, w_gate, w_up, w_down):
        n_layers, width, heads, head_dim = w_q.shape
        n_kv = w_kv.shape[3]
        rows = hidden.shape[1]
        far, near = rope_tables(rows * n_tp, rows // 2, head_dim)
        w_q = w_q.reshape(n_layers, width * heads, head_dim)
        w_kv = w_kv.reshape(n_layers, width * 2 * n_kv, head_dim)
        w_o = w_o.reshape(n_layers, heads * head_dim, width)
        w_gate = jnp.swapaxes(w_gate, 1, 2)
        w_up = jnp.swapaxes(w_up, 1, 2)
        resid = hidden[0]
        for layer in range(n_layers):
            resid = attention(layer, resid, norm_attn[layer][None], far, near, w_q, w_kv, w_o, n_tp)
            resid = mlp(layer, resid, norm_mlp[layer][None], w_gate, w_up, w_down, BF16 if layer == n_layers - 1 else F32)
        return resid[None]

    return jax.shard_map(body, mesh=mesh, in_specs=in_specs, out_specs=tok_spec, check_vma=False)
```

```python
import functools
import math
import jax
import jax.numpy as jnp
import numpy as np
from jax import lax
from jax.experimental import pallas as pl
from jax.experimental.pallas import tpu as pltpu
from jax.sharding import PartitionSpec as P

EPS = 1e-5
ROPE_BASE = 10000.0
MESH = pl.DeviceIdType.MESH
VMEM_MAX = 67043328
F32 = jnp.float32
BF16 = jnp.bfloat16


def rope_tables(seq, step, head_dim):
    half_dim = head_dim // 2
    inv_freq = ROPE_BASE ** (-2.0 * np.arange(half_dim, dtype=np.float64) / head_dim)

    def table(positions):
        angles = positions.astype(np.float64)[:, None] * inv_freq[None, :]
        cos_t, sin_t = np.cos(angles), np.sin(angles)
        return np.stack([np.concatenate([cos_t, cos_t], axis=1), np.concatenate([-sin_t, sin_t], axis=1)]).astype(np.float32)

    return table(np.arange(0, seq, step)), table(np.arange(step))


def coords():
    t = lax.axis_index('tp')
    c = lax.rem(t, 2)
    xx = lax.rem(lax.div(t, 2), 2)
    yy = lax.div(t, 4)
    return t, (yy, xx, c), (t + 1 - 2 * c, t + 2 - 4 * xx, t + 4 - 8 * yy)


def rcopy(src, dst, ssem, rsem, dev):
    return pltpu.make_async_remote_copy(src_ref=src, dst_ref=dst, send_sem=ssem, recv_sem=rsem,
                                        device_id={'tp': dev}, device_id_type=MESH)


def greet(devices):
    for dev in devices:
        pl.semaphore_signal(pltpu.get_barrier_semaphore(), inc=1, device_id={'tp': dev}, device_id_type=MESH)


class RowGather:
    def __init__(self, xbuf, sx, sy, ag, fs, fr, partners):
        mate, dev_x, dev_y = partners
        rows = xbuf.shape[2]
        half = rows // 2
        lead = half // 4
        h0, h1 = pl.ds(0, half), pl.ds(half, half)
        own = xbuf.at[0, 0]
        self.xbuf, self.ag, self.fs, self.fr, self.mate = xbuf, ag, fs, fr, mate
        self.halves = (h0, h1)

        def piece(k, sem, dev, first, size, window, slot):
            at = pl.ds(first, size)
            return rcopy(own.at[at], xbuf.at[window, 0, at], sem.at[k], ag.at[window, slot], dev)

        self.first = (piece(0, sx, dev_x, 0, half, 1, 0), piece(0, sy, dev_y, half, half, 1, 1))
        self.lead = (piece(1, sx, dev_x, half, lead, 3, 1), piece(1, sy, dev_y, 0, lead, 3, 0))
        self.rest = (piece(2, sx, dev_x, half + lead, half - lead, 3, 1), piece(2, sy, dev_y, lead, half - lead, 3, 0))
        self.relay = (rcopy(xbuf.at[1, 0, h1], xbuf.at[2, 0, h1], sx.at[3], ag.at[2, 1], dev_x),
                      rcopy(xbuf.at[1, 0, h0], xbuf.at[2, 0, h0], sy.at[3], ag.at[2, 0], dev_y))

    def forward(self, w):
        return rcopy(self.xbuf.at[w, 0], self.xbuf.at[w, 1], self.fs.at[w], self.fr.at[w], self.mate)

    def start(self, norm_half):
        norm_half(0)
        pl.semaphore_wait(pltpu.get_barrier_semaphore(), 3)
        self.first[0].start()
        norm_half(1)
        self.first[1].start()
        self.lead[0].start()
        self.lead[1].start()
        self.forward(0).start()

    def arrive(self, w):
        for k in range(2):
            at = self.halves[k]
            pltpu.make_async_copy(self.xbuf.at[0, 0, at], self.xbuf.at[w, 0, at], self.ag.at[w, k]).wait()

        @pl.when(w == 1)
        def _():
            for copy in self.relay + self.rest:
                copy.start()
        self.forward(w).start()

    def finish(self):
        for copy in self.first + self.lead + self.relay + self.rest:
            copy.wait_send()
        for w in range(4):
            self.forward(w).wait_send()


def gather_sems():
    dma = pltpu.SemaphoreType.DMA
    return [dma((4,)), dma((4,)), dma((4, 2)), dma((4,)), dma((4,))]


def norm_rows(src, gain, dst, first, count):
    nb = 64

    @pl.loop(0, count // nb)
    def _(b):
        at = pl.ds(pl.multiple_of(first + b * nb, nb), nb)
        r = src[at, :].astype(F32)
        mean_sq = jnp.mean(r * r, axis=-1, keepdims=True)
        dst[at, :] = (r * lax.rsqrt(mean_sq + EPS) * gain).astype(BF16)


class WeightGather:
    def __init__(self, buf, unit, sems, t, z, mate, dev_f, dev_s, dev_d):
        so, sz, oa, ob, om, on = sems
        part = unit // 4
        self.buf, self.oa, self.ob, self.z = buf, oa, ob, z
        self.from_dev = ((dev_f, 0), (dev_s, 1), (dev_f, 1), (dev_s, 0), (dev_d, 1), (dev_d, 0))

        def span(dev, k, p):
            return pl.ds(pl.multiple_of(dev * unit + (2 * k + p) * part, part), part)

        def same(at, ssem, rsem, dev):
            return rcopy(buf.at[at], buf.at[at], ssem, rsem, dev)

        def across(at, ssem, rsem):
            return pltpu.make_async_remote_copy(src_ref=buf.at[at], dst_ref=buf.at[at], send_sem=ssem, recv_sem=rsem,
                                                device_id={'dp': 1 - z, 'tp': t}, device_id_type=MESH)

        self.span = span
        self.send = (same(span(t, 0, z), so.at[0], oa.at[0], dev_f), same(span(t, 1, z), so.at[1], oa.at[1], dev_s),
                     same(span(t, 1, z), so.at[2], oa.at[2], dev_f), same(span(t, 0, z), so.at[3], oa.at[3], dev_s))
        self.relay = (same(span(dev_s, 1, z), so.at[4], oa.at[4], dev_f), same(span(dev_f, 0, z), so.at[5], oa.at[5], dev_s))
        self.via_z = [across(span(dev, k, z), sz.at[i], ob.at[i]) for i, (dev, k) in enumerate(self.from_dev)]
        self.to_mate = [same(span(dev, k, z), om.at[i], on.at[i], mate) for i, (dev, k) in enumerate(self.from_dev)]
        self.to_mate += [same(span(dev, k, 1 - z), om.at[6 + i], on.at[6 + i], mate) for i, (dev, k) in enumerate(self.from_dev)]
        own = pl.ds(pl.multiple_of(t * unit, unit), unit)
        self.to_mate.append(same(own, om.at[12], on.at[12], mate))

    def take(self, i, sem, p):
        at = self.span(self.from_dev[i][0], self.from_dev[i][1], p)
        pltpu.make_async_copy(self.buf.at[at], self.buf.at[at], sem.at[i]).wait()

    def start(self):
        for copy in self.send:
            copy.start()
        self.to_mate[12].start()

    def received(self, pieces):
        for i in pieces:
            self.take(i, self.oa, self.z)
            if i < 2:
                self.relay[1 - i].start()
            self.via_z[i].start()
            self.to_mate[i].start()

    def from_z(self, pieces):
        for i in pieces:
            self.take(i, self.ob, 1 - self.z)
            self.to_mate[6 + i].start()

    def from_mate(self, pieces):
        for i in pieces:
            self.to_mate[i].wait_recv()

    def finish(self):
        for copy in list(self.send + self.relay) + self.via_z + self.to_mate:
            copy.wait_send()


def weight_sems():
    dma = pltpu.SemaphoreType.DMA
    return [dma((6,)), dma((6,)), dma((6,)), dma((6,)), dma((13,)), dma((13,))]


def attend(qkv_ref, block, bq, bk, heads, head_dim):
    scale = math.log2(math.e) / math.sqrt(head_dim)
    mask = lax.broadcasted_iota(jnp.int32, (bq, bq), 0) >= lax.broadcasted_iota(jnp.int32, (bq, bq), 1)
    q_at = pl.ds(pl.multiple_of(block * bq, bq), bq)
    qs = [qkv_ref[q_at, h * head_dim:(h + 1) * head_dim] for h in range(heads)]

    def step(first, count, carry, masked):
        at = pl.ds(pl.multiple_of(first, bq), count)
        k_blk = qkv_ref[at, heads * head_dim:(heads + 1) * head_dim]
        v_blk = qkv_ref[at, (heads + 1) * head_dim:(heads + 2) * head_dim]
        out = []
        for h in range(heads):
            m, l, acc = carry[h]
            s = lax.dot_general(qs[h], k_blk, (((1,), (1,)), ((), ())), preferred_element_type=F32)
            if masked:
                s = jnp.where(mask, s, -jnp.inf)
            m_new = jnp.maximum(m, jnp.max(s, axis=-1, keepdims=True))
            p = jnp.exp2((s - m_new) * scale)
            alpha = jnp.exp2((m - m_new) * scale)
            l = l * alpha + jnp.sum(p, axis=-1, keepdims=True)
            acc = acc * alpha + jnp.dot(p.astype(BF16), v_blk, preferred_element_type=F32)
            out.append((m_new, l, acc))
        return tuple(out)

    carry = tuple((jnp.full((bq, 1), -jnp.inf, F32), jnp.zeros((bq, 1), F32), jnp.zeros((bq, head_dim), F32)) for _ in range(heads))
    carry = step(block * bq, bq, carry, True)
    full = lax.div(block * bq, bk)
    carry = lax.fori_loop(0, full, lambda j, cur: step(j * bk, bk, cur, False), carry)
    carry = lax.fori_loop(full * (bk // bq), block, lambda j, cur: step(j * bq, bq, cur, False), carry)
    return [(acc / l).astype(BF16) for _, l, acc in carry]


def attn_kernel(layer, n_tp, n_kv, heads, head_dim, bk, r_hbm, gain_ref, far_ref, near_ref, wq_hbm, wkv_hbm, wo_hbm, out_hbm,
                x, rin, wq, wkv, wide, w_kv, w_q, rope, kv_out, q_out, qkv_ref, wo, ctx, ctx_out, res,
                lsem, ks, kr, km, kn, qs, qr, cs, cr, es, *gather_sem):
    t, (yy, xx, c), (mate, dev_x, dev_y) = coords()
    z = lax.axis_index('dp')
    dev_d = dev_x + dev_y - t
    dev_f = dev_x + c * (dev_y - dev_x)
    dev_s = dev_y + c * (dev_x - dev_y)
    rows, width = res.shape
    half = rows // 2
    cols = heads * head_dim

    load_r = pltpu.make_async_copy(r_hbm, rin, lsem.at[0])
    load_q = pltpu.make_async_copy(wq_hbm.at[layer], wq, lsem.at[1])
    load_r.start()
    load_q.start()
    others = [lax.rem(t + k, n_tp) for k in range(1, n_tp)]
    greet(others)
    pl.semaphore_signal(pltpu.get_barrier_semaphore(), inc=1, device_id={'dp': 1 - z, 'tp': t}, device_id_type=MESH)
    own_o = pl.ds(pl.multiple_of(t * cols, cols), cols)
    load_kv = pltpu.make_async_copy(wkv_hbm.at[layer], wkv, lsem.at[2])
    load_o = pltpu.make_async_copy(wo_hbm.at[layer], wo.at[own_o], lsem.at[3])
    load_kv.start()
    load_o.start()
    place = (t, z, mate, dev_f, dev_s, dev_d)
    get_q = WeightGather(w_q, width, gather_sem[:6], *place)
    get_o = WeightGather(wo, cols, gather_sem[6:], *place)
    nd = 256

    def deinterleave(raw, count, dst, first):
        @pl.loop(0, width // nd)
        def _(b):
            wide[pl.ds(0, count * nd), :] = raw[pl.ds(pl.multiple_of(b * count * nd, nd), count * nd), :].astype(F32)
            for h in range(count):
                dst[pl.ds(pl.multiple_of(first + b * nd, nd), nd), h * head_dim:(h + 1) * head_dim] = wide[pl.ds(h, nd, stride=count), :].astype(BF16)

    load_q.wait()
    deinterleave(wq, heads, w_q, t * width)
    pl.semaphore_wait(pltpu.get_barrier_semaphore(), n_tp)
    get_q.start()

    load_r.wait()
    norm_rows(rin, gain_ref[layer:layer + 1], x, 0, rows)
    for k in range(2):
        at = slice(k * half, (k + 1) * half)
        cos_f, sin_f = far_ref[0, pl.ds(t * 2 + k, 1), :], far_ref[1, pl.ds(t * 2 + k, 1), :]
        rope[0, at] = cos_f * near_ref[0] - sin_f * near_ref[1]
        rope[1, at] = sin_f * near_ref[0] + cos_f * near_ref[1]

    def rotate(v):
        return (v * rope[0] + pltpu.roll(v, head_dim // 2, 1) * rope[1]).astype(BF16)

    own = pl.ds(pl.multiple_of(t * rows, rows), rows)
    kv_cols = pl.ds(cols, 2 * head_dim)
    q_cols = pl.ds(0, cols)
    load_kv.wait()
    deinterleave(wkv, 2 * n_kv, w_kv, 0)
    for g in range(n_kv):
        proj = jnp.dot(x[...], w_kv[:, g * head_dim:(g + 1) * head_dim], preferred_element_type=F32)
        kv_out[g, :, 0:head_dim] = rotate(proj)
        proj = jnp.dot(x[...], w_kv[:, (n_kv + g) * head_dim:(n_kv + g + 1) * head_dim], preferred_element_type=F32)
        kv_out[g, :, head_dim:2 * head_dim] = proj.astype(BF16)

    def kv_send(k, dev):
        return rcopy(kv_out.at[lax.div(dev * n_kv, n_tp)], qkv_ref.at[own, kv_cols], ks.at[k], kr.at[k], dev)

    def kv_mate(k, dev):
        at = pl.ds(pl.multiple_of(dev * rows, rows), rows)
        return rcopy(qkv_ref.at[at, kv_cols], qkv_ref.at[at, kv_cols], km.at[k], kn.at[k], mate)

    near = (dev_x, dev_y, dev_d)
    sends = [kv_send(k, dev) for k, dev in enumerate(near)]
    for copy in sends:
        copy.start()
    qkv_ref[own, kv_cols] = kv_out[lax.div(t * n_kv, n_tp)]
    hand_on = [kv_mate(k, dev) for k, dev in enumerate(near)] + [
        rcopy(kv_out.at[lax.div(t * n_kv, n_tp)], qkv_ref.at[own, kv_cols], km.at[3], kn.at[3], mate)]
    hand_on[3].start()

    def block_of(i):
        w = lax.div(i, 2)
        j = lax.rem(i, 2)
        core = c + j - 2 * c * j
        one = lax.rem(lax.div(w + 1, 2), 2)
        two = lax.div(w, 2)
        flip_x = one + core * (two - one)
        flip_y = two + core * (one - two)
        return (2 * (yy + flip_y - 2 * yy * flip_y) + xx + flip_x - 2 * xx * flip_x) * 2 + core

    def project(i):
        dev = block_of(i)
        proj = jnp.dot(x[...], w_q[pl.ds(pl.multiple_of(dev * width, width), width), :], preferred_element_type=F32)
        for h in range(heads):
            at_h = slice(h * head_dim, (h + 1) * head_dim)
            q_out[i, :, at_h] = rotate(proj[:, at_h])

    def q_send(i):
        return rcopy(q_out.at[i], qkv_ref.at[own, q_cols], qs.at[i], qr.at[t], block_of(i))

    def project_all(first, last):
        @pl.loop(first, last)
        def _(i):
            project(i)

            @pl.when(i >= 1)
            def _():
                q_send(i).start()

    get_q.from_mate([12])
    project_all(0, 2)
    qkv_ref[own, q_cols] = q_out[0]
    get_q.received(range(4))
    for k in range(3):
        pltpu.make_async_copy(kv_out.at[0], qkv_ref.at[pl.ds(pl.multiple_of(near[k] * rows, rows), rows), kv_cols], kr.at[k]).wait()
        hand_on[k].start()
    for copy in hand_on:
        copy.wait_recv()

    def ctx_send(i, dev):
        return rcopy(ctx_out.at[i], ctx.at[t], cs.at[i], cr.at[t], dev)

    load_o.wait()

    @pl.loop(0, n_tp)
    def _(n):
        i = n + jnp.where(n < 4, 0, jnp.where(n < 6, 2, -2))
        block = block_of(i)

        @pl.when(n == 0)
        def _():
            get_o.start()

        @pl.when(n == 1)
        def _():
            get_q.received((4, 5))

        @pl.when(n == 2)
        def _():
            get_q.from_z(range(4))
            get_q.from_mate((0, 1, 2, 3, 6, 7, 8, 9))
            project_all(2, 4)
            project_all(6, 8)
            get_o.received(range(4))

        @pl.when(n == 4)
        def _():
            get_q.from_z((4, 5))
            get_q.from_mate((4, 5, 10, 11))
            project_all(4, 6)
            get_o.received((4, 5))

        @pl.when(n == 7)
        def _():
            get_o.from_z(range(4))

        @pl.when(n >= 1)
        def _():
            pltpu.make_async_copy(q_out.at[0], qkv_ref.at[pl.ds(pl.multiple_of(block * rows, rows), rows), q_cols], qr.at[block]).wait()
        for h, val in enumerate(attend(qkv_ref, block, rows, bk, heads, head_dim)):
            ctx_out[i, :, h * head_dim:(h + 1) * head_dim] = val

        @pl.when(n >= 1)
        def _():
            ctx_send(i, block).start()

    get_o.from_z((4, 5))
    get_o.from_mate(range(13))
    nc = 512
    chunks = [pl.ds(n * nc, nc) for n in range(width // nc)]
    for at in chunks:
        res[:, at] = rin[:, at].astype(F32) + jnp.dot(ctx_out[0], wo[own_o, at], preferred_element_type=F32)

    def from_sender(n):
        dev = block_of(n + jnp.where(n < 4, 0, jnp.where(n < 6, 2, -2)))
        pltpu.make_async_copy(ctx_out.at[0], ctx.at[dev], cr.at[dev]).wait()
        return dev, pl.ds(pl.multiple_of(dev * cols, cols), cols)

    @pl.loop(1, n_tp - 1)
    def _(n):
        dev, rows_o = from_sender(n)
        for at in chunks:
            res[:, at] = res[:, at] + jnp.dot(ctx[dev], wo[rows_o, at], preferred_element_type=F32)

    dev, rows_o = from_sender(jnp.int32(n_tp - 1))
    outs = []
    for n, at in enumerate(chunks):
        res[:, at] = res[:, at] + jnp.dot(ctx[dev], wo[rows_o, at], preferred_element_type=F32)
        outs.append(pltpu.make_async_copy(res.at[:, at], out_hbm.at[:, at], es.at[n]))
        outs[n].start()
    get_q.finish()
    get_o.finish()
    for copy in sends + hand_on:
        copy.wait_send()
    for i in range(1, n_tp):
        q_send(jnp.int32(i)).wait_send()
        ctx_send(i, mate).wait_send()
    for copy in outs:
        copy.wait()


def attention(layer, resid, gain, far, near, w_q, w_kv, w_o, n_tp, bk=1024):
    rows, width = resid.shape
    cols, head_dim = w_o.shape[1], w_q.shape[2]
    heads = cols // head_dim
    n_kv = w_kv.shape[1] // (2 * width)
    seq = rows * n_tp
    vmem = pl.BlockSpec(memory_space=pltpu.VMEM)
    anywhere = pl.BlockSpec(memory_space=pl.ANY)
    dma = pltpu.SemaphoreType.DMA
    return pl.pallas_call(
        functools.partial(attn_kernel, layer, n_tp, n_kv, heads, head_dim, bk),
        out_shape=jax.ShapeDtypeStruct((rows, width), F32),
        in_specs=[anywhere, vmem, vmem, vmem, anywhere, anywhere, anywhere],
        out_specs=anywhere,
        scratch_shapes=[
            pltpu.VMEM((rows, width), BF16),
            pltpu.VMEM((rows, width), resid.dtype),
            pltpu.VMEM(w_q.shape[1:], BF16),
            pltpu.VMEM(w_kv.shape[1:], BF16),
            pltpu.VMEM((256 * max(heads, 2 * n_kv), head_dim), F32),
            pltpu.VMEM((width, 2 * n_kv * head_dim), BF16),
            pltpu.VMEM((n_tp * width, cols), BF16),
            pltpu.VMEM((2, rows, head_dim), F32),
            pltpu.VMEM((n_kv, rows, 2 * head_dim), BF16),
            pltpu.VMEM((n_tp, rows, cols), BF16),
            pltpu.VMEM((seq, cols + 2 * head_dim), BF16),
            pltpu.VMEM((n_tp * cols, width), BF16),
            pltpu.VMEM((n_tp, rows, cols), BF16),
            pltpu.VMEM((n_tp, rows, cols), BF16),
            pltpu.VMEM((rows, width), F32),
            dma((4,)), dma((3,)), dma((3,)), dma((4,)), dma((4,)), dma((n_tp,)), dma((n_tp,)), dma((n_tp,)), dma((n_tp,)), dma((4,)),
        ] + weight_sems() + weight_sems(),
        compiler_params=pltpu.CompilerParams(collective_id=1 + layer, has_side_effects=True, vmem_limit_bytes=VMEM_MAX),
        cost_estimate=pl.CostEstimate(flops=2 * seq * seq * cols, bytes_accessed=4 * seq * cols, transcendentals=seq * seq),
        name="attention" + str(layer),
    )(resid, gain, far, near, w_q, w_kv, w_o)


def mlp_kernel(layer, r_hbm, gain_ref, wg_hbm, wu_hbm, wd_hbm, out_hbm,
               wg, wu, wd, xbuf, prec, recv, acc, stash, act,
               lsem, sx, sy, ag, fs, fr, ps, pr, rr, ss):
    _, _, partners = coords()
    mate, dev_x, dev_y = partners
    rows, width = acc.shape
    half = rows // 2
    hid = act.shape[1]
    h0, h1 = pl.ds(0, half), pl.ds(half, half)
    hs = (h0, h1)
    nb = 64

    load_r = pltpu.make_async_copy(r_hbm, acc, lsem.at[0])
    load_r.start()
    greet(partners)
    loads = [pltpu.make_async_copy(src.at[layer], dst, lsem.at[k + 1]) for k, (src, dst) in enumerate(((wg_hbm, wg), (wu_hbm, wu), (wd_hbm, wd)))]
    load_r.wait()
    for copy in loads:
        copy.start()
    gather = RowGather(xbuf, sx, sy, ag, fs, fr, partners)
    gather.start(lambda k: norm_rows(acc, gain_ref[layer:layer + 1], xbuf.at[0, 0], k * half, half))

    def partial_send(w):
        return rcopy(xbuf.at[w, 1], prec.at[w], ps.at[w], pr.at[w], mate)

    stage = (rcopy(xbuf.at[1, 1, h0], recv.at[0], ss.at[0], rr.at[0], dev_x),
             rcopy(xbuf.at[1, 1, h1], recv.at[1], ss.at[1], rr.at[1], dev_y),
             rcopy(xbuf.at[2, 1, h0], recv.at[2], ss.at[2], rr.at[2], dev_x),
             rcopy(xbuf.at[2, 1, h1], recv.at[3], ss.at[3], rr.at[3], dev_y),
             rcopy(xbuf.at[3, 1, h0], recv.at[4], ss.at[4], rr.at[4], dev_y),
             rcopy(xbuf.at[3, 1, h1], recv.at[5], ss.at[5], rr.at[5], dev_x))

    for copy in loads:
        copy.wait()
    cut = 768
    nd = 1024

    def gate_up(x_at, at):
        g = lax.dot_general(x_at[...], wg[at, :], (((1,), (1,)), ((), ())), preferred_element_type=F32)
        u = lax.dot_general(x_at[...], wu[at, :], (((1,), (1,)), ((), ())), preferred_element_type=F32)
        act[:, at] = (g * jax.nn.sigmoid(g) * u).astype(BF16)

    @pl.loop(0, 8)
    def _(s):
        w = lax.div(s, 2)
        rc = 1 - lax.rem(s, 2)

        @pl.when(rc == 1)
        def _():
            gather.forward(w).wait_recv()
        x_at = xbuf.at[w, rc]
        gate_up(x_at, pl.ds(0, cut))
        gate_up(x_at, pl.ds(cut, hid - cut))

        @pl.when(rc == 0)
        def _():
            @pl.when(w < 3)
            def _():
                gather.arrive(w + 1)
            partial_send(w).wait()

        @pl.loop(0, width // nd)
        def _(n):
            at = pl.ds(pl.multiple_of(n * nd, nd), nd)
            val = jnp.dot(act[...], wd[:, at], preferred_element_type=F32)

            @pl.when(rc == 1)
            def _():
                xbuf[w, 1, :, at] = val.astype(BF16)

            @pl.when(rc == 0)
            def _():
                total = val + prec[w, :, at].astype(F32)

                @pl.when(w == 0)
                def _():
                    acc[:, at] = acc[:, at] + total

                @pl.when(w == 3)
                def _():
                    stash[:, at] = total

                @pl.when((w == 1) | (w == 2))
                def _():
                    xbuf[w, 1, :, at] = total.astype(BF16)

        @pl.when(rc == 1)
        def _():
            partial_send(w).start()

        @pl.when(s == 3)
        def _():
            stage[0].start()
            stage[1].start()

        @pl.when(s == 5)
        def _():
            stage[2].start()
            stage[3].start()

    def blocks_of(k):
        def each(fn):
            @pl.loop(0, half // nb)
            def _(b):
                fn(pl.ds(pl.multiple_of(b * nb, nb), nb), pl.ds(pl.multiple_of(k * half + b * nb, nb), nb))
        return each

    for k in range(2):
        stage[k].wait_recv()

        @blocks_of(k)
        def _(at, to):
            acc[to, :] = acc[to, :] + recv[k, at, :].astype(F32)
    for k in range(2):
        stage[2 + k].wait_recv()

        @blocks_of(k)
        def _(at, to):
            xbuf[3, 1, to, :] = (stash[to, :] + recv[2 + k, at, :].astype(F32)).astype(BF16)
        stage[4 + k].start()
    gather.finish()
    narrow = out_hbm.dtype == BF16
    final = xbuf.at[0, 0] if narrow else acc
    outs = []
    for k in range(2):
        stage[4 + k].wait_recv()

        @blocks_of(k)
        def _(at, to):
            final[to, :] = (acc[to, :] + recv[4 + k, at, :].astype(F32)).astype(final.dtype)
        outs.append(pltpu.make_async_copy(final.at[hs[k]], out_hbm.at[hs[k]], lsem.at[k]))
        outs[k].start()
    for copy in stage:
        copy.wait_send()
    for copy in outs:
        copy.wait()


def mlp(layer, resid, gain, w_gate, w_up, w_down, out_dtype):
    rows, width = resid.shape
    hid = w_gate.shape[1]
    half = rows // 2
    any_spec = pl.BlockSpec(memory_space=pl.ANY)
    dma = pltpu.SemaphoreType.DMA
    return pl.pallas_call(
        functools.partial(mlp_kernel, layer),
        out_shape=jax.ShapeDtypeStruct((rows, width), out_dtype),
        in_specs=[any_spec, pl.BlockSpec(memory_space=pltpu.VMEM), any_spec, any_spec, any_spec],
        out_specs=any_spec,
        scratch_shapes=[
            pltpu.VMEM((hid, width), BF16),
            pltpu.VMEM((hid, width), BF16),
            pltpu.VMEM((hid, width), BF16),
            pltpu.VMEM((4, 2, rows, width), BF16),
            pltpu.VMEM((4, rows, width), BF16),
            pltpu.VMEM((6, half, width), BF16),
            pltpu.VMEM((rows, width), F32),
            pltpu.VMEM((rows, width), F32),
            pltpu.VMEM((rows, hid), BF16),
            dma((4,)),
        ] + gather_sems() + [dma((4,)), dma((4,)), dma((6,)), dma((6,))],
        compiler_params=pltpu.CompilerParams(collective_id=5 + layer, has_side_effects=True, vmem_limit_bytes=VMEM_MAX),
        cost_estimate=pl.CostEstimate(flops=6 * 8 * rows * width * hid, bytes_accessed=6 * width * hid, transcendentals=8 * rows * hid),
        name="mlp" + str(layer),
    )(resid, gain, w_gate, w_up, w_down)


def solution(mesh):
    n_tp = mesh.shape['tp']
    tok_spec = P('dp', 'tp', None)
    in_specs = (tok_spec, P(), P(None, None, 'tp', None), P(), P(None, 'tp', None, None), P(), P(None, None, 'tp'), P(None, None, 'tp'), P(None, 'tp', None))

    def body(hidden, norm_attn, w_q, w_kv, w_o, norm_mlp, w_gate, w_up, w_down):
        n_layers, width, heads, head_dim = w_q.shape
        n_kv = w_kv.shape[3]
        rows = hidden.shape[1]
        far, near = rope_tables(rows * n_tp, rows // 2, head_dim)
        w_q = w_q.reshape(n_layers, width * heads, head_dim)
        w_kv = w_kv.reshape(n_layers, width * 2 * n_kv, head_dim)
        w_o = w_o.reshape(n_layers, heads * head_dim, width)
        w_gate = jnp.swapaxes(w_gate, 1, 2)
        w_up = jnp.swapaxes(w_up, 1, 2)
        resid = hidden[0]
        for layer in range(n_layers):
            resid = attention(layer, resid, norm_attn, far, near, w_q, w_kv, w_o, n_tp)
            resid = mlp(layer, resid, norm_mlp, w_gate, w_up, w_down, BF16 if layer == n_layers - 1 else F32)
        return resid[None]

    return jax.shard_map(body, mesh=mesh, in_specs=in_specs, out_specs=tok_spec, check_vma=False)
```

```python
import functools
import math
import jax
import jax.numpy as jnp
import numpy as np
from jax import lax
from jax.experimental import pallas as pl
from jax.experimental.pallas import tpu as pltpu
from jax.sharding import PartitionSpec as P

EPS = 1e-5
ROPE_BASE = 10000.0
MESH = pl.DeviceIdType.MESH
VMEM_MAX = 67043328
F32 = jnp.float32
BF16 = jnp.bfloat16


def rope_tables(seq, step, head_dim):
    half_dim = head_dim // 2
    inv_freq = ROPE_BASE ** (-2.0 * np.arange(half_dim, dtype=np.float64) / head_dim)

    def table(positions):
        angles = positions.astype(np.float64)[:, None] * inv_freq[None, :]
        cos_t, sin_t = np.cos(angles), np.sin(angles)
        return np.stack([np.concatenate([cos_t, cos_t], axis=1), np.concatenate([-sin_t, sin_t], axis=1)]).astype(np.float32)

    return table(np.arange(0, seq, step)), table(np.arange(step))


def coords():
    t = lax.axis_index('tp')
    c = lax.rem(t, 2)
    xx = lax.rem(lax.div(t, 2), 2)
    yy = lax.div(t, 4)
    return t, (yy, xx, c), (t + 1 - 2 * c, t + 2 - 4 * xx, t + 4 - 8 * yy)


def rcopy(src, dst, ssem, rsem, dev):
    return pltpu.make_async_remote_copy(src_ref=src, dst_ref=dst, send_sem=ssem, recv_sem=rsem,
                                        device_id={'tp': dev}, device_id_type=MESH)


def greet(devices):
    for dev in devices:
        pl.semaphore_signal(pltpu.get_barrier_semaphore(), inc=1, device_id={'tp': dev}, device_id_type=MESH)


class RowGather:
    def __init__(self, xbuf, sx, sy, ag, fs, fr, partners):
        mate, dev_x, dev_y = partners
        rows = xbuf.shape[2]
        half = rows // 2
        lead = half // 4
        h0, h1 = pl.ds(0, half), pl.ds(half, half)
        own = xbuf.at[0, 0]
        self.xbuf, self.ag, self.fs, self.fr, self.mate = xbuf, ag, fs, fr, mate
        self.halves = (h0, h1)

        def piece(k, sem, dev, first, size, window, slot):
            at = pl.ds(first, size)
            return rcopy(own.at[at], xbuf.at[window, 0, at], sem.at[k], ag.at[window, slot], dev)

        self.first = (piece(0, sx, dev_x, 0, half, 1, 0), piece(0, sy, dev_y, half, half, 1, 1))
        self.lead = (piece(1, sx, dev_x, half, lead, 3, 1), piece(1, sy, dev_y, 0, lead, 3, 0))
        self.rest = (piece(2, sx, dev_x, half + lead, half - lead, 3, 1), piece(2, sy, dev_y, lead, half - lead, 3, 0))
        self.relay = (rcopy(xbuf.at[1, 0, h1], xbuf.at[2, 0, h1], sx.at[3], ag.at[2, 1], dev_x),
                      rcopy(xbuf.at[1, 0, h0], xbuf.at[2, 0, h0], sy.at[3], ag.at[2, 0], dev_y))

    def forward(self, w):
        return rcopy(self.xbuf.at[w, 0], self.xbuf.at[w, 1], self.fs.at[w], self.fr.at[w], self.mate)

    def start(self, norm_half):
        norm_half(0)
        pl.semaphore_wait(pltpu.get_barrier_semaphore(), 3)
        self.first[0].start()
        norm_half(1)
        self.first[1].start()
        self.lead[0].start()
        self.lead[1].start()
        self.forward(0).start()

    def arrive(self, w):
        for k in range(2):
            at = self.halves[k]
            pltpu.make_async_copy(self.xbuf.at[0, 0, at], self.xbuf.at[w, 0, at], self.ag.at[w, k]).wait()

        @pl.when(w == 1)
        def _():
            for copy in self.relay + self.rest:
                copy.start()
        self.forward(w).start()

    def finish(self):
        for copy in self.first + self.lead + self.relay + self.rest:
            copy.wait_send()
        for w in range(4):
            self.forward(w).wait_send()


def gather_sems():
    dma = pltpu.SemaphoreType.DMA
    return [dma((4,)), dma((4,)), dma((4, 2)), dma((4,)), dma((4,))]


def norm_rows(src, gain, dst, first, count):
    nb = 64

    @pl.loop(0, count // nb)
    def _(b):
        at = pl.ds(pl.multiple_of(first + b * nb, nb), nb)
        r = src[at, :].astype(F32)
        mean_sq = jnp.mean(r * r, axis=-1, keepdims=True)
        dst[at, :] = (r * lax.rsqrt(mean_sq + EPS) * gain).astype(BF16)


class WeightGather:
    def __init__(self, buf, unit, sems, t, z, mate, dev_f, dev_s, dev_d):
        so, sz, oa, ob, om, on = sems
        part = unit // 4
        self.buf, self.oa, self.ob, self.z = buf, oa, ob, z
        self.from_dev = ((dev_f, 0), (dev_s, 1), (dev_f, 1), (dev_s, 0), (dev_d, 1), (dev_d, 0))

        def span(dev, k, p):
            return pl.ds(pl.multiple_of(dev * unit + (2 * k + p) * part, part), part)

        def same(at, ssem, rsem, dev):
            return rcopy(buf.at[at], buf.at[at], ssem, rsem, dev)

        def across(at, ssem, rsem):
            return pltpu.make_async_remote_copy(src_ref=buf.at[at], dst_ref=buf.at[at], send_sem=ssem, recv_sem=rsem,
                                                device_id={'dp': 1 - z, 'tp': t}, device_id_type=MESH)

        self.span = span
        self.send = (same(span(t, 0, z), so.at[0], oa.at[0], dev_f), same(span(t, 1, z), so.at[1], oa.at[1], dev_s),
                     same(span(t, 1, z), so.at[2], oa.at[2], dev_f), same(span(t, 0, z), so.at[3], oa.at[3], dev_s))
        self.relay = (same(span(dev_s, 1, z), so.at[4], oa.at[4], dev_f), same(span(dev_f, 0, z), so.at[5], oa.at[5], dev_s))
        self.via_z = [across(span(dev, k, z), sz.at[i], ob.at[i]) for i, (dev, k) in enumerate(self.from_dev)]
        self.to_mate = [same(span(dev, k, z), om.at[i], on.at[i], mate) for i, (dev, k) in enumerate(self.from_dev)]
        self.to_mate += [same(span(dev, k, 1 - z), om.at[6 + i], on.at[6 + i], mate) for i, (dev, k) in enumerate(self.from_dev)]
        own = pl.ds(pl.multiple_of(t * unit, unit), unit)
        self.to_mate.append(same(own, om.at[12], on.at[12], mate))

    def take(self, i, sem, p):
        at = self.span(self.from_dev[i][0], self.from_dev[i][1], p)
        pltpu.make_async_copy(self.buf.at[at], self.buf.at[at], sem.at[i]).wait()

    def start(self):
        for copy in self.send:
            copy.start()
        self.to_mate[12].start()

    def received(self, pieces):
        for i in pieces:
            self.take(i, self.oa, self.z)
            if i < 2:
                self.relay[1 - i].start()
            self.via_z[i].start()
            self.to_mate[i].start()

    def from_z(self, pieces):
        for i in pieces:
            self.take(i, self.ob, 1 - self.z)
            self.to_mate[6 + i].start()

    def from_mate(self, pieces):
        for i in pieces:
            self.to_mate[i].wait_recv()

    def finish(self):
        for copy in list(self.send + self.relay) + self.via_z + self.to_mate:
            copy.wait_send()


def weight_sems():
    dma = pltpu.SemaphoreType.DMA
    return [dma((6,)), dma((6,)), dma((6,)), dma((6,)), dma((13,)), dma((13,))]


def attend(qkv_ref, block, bq, bk, heads, head_dim):
    scale = math.log2(math.e) / math.sqrt(head_dim)
    mask = lax.broadcasted_iota(jnp.int32, (bq, bq), 0) >= lax.broadcasted_iota(jnp.int32, (bq, bq), 1)
    q_at = pl.ds(pl.multiple_of(block * bq, bq), bq)
    qs = [qkv_ref[q_at, h * head_dim:(h + 1) * head_dim] for h in range(heads)]

    def step(first, count, carry, masked):
        at = pl.ds(pl.multiple_of(first, bq), count)
        k_blk = qkv_ref[at, heads * head_dim:(heads + 1) * head_dim]
        v_blk = qkv_ref[at, (heads + 1) * head_dim:(heads + 2) * head_dim]
        out = []
        for h in range(heads):
            m, l, acc = carry[h]
            s = lax.dot_general(qs[h], k_blk, (((1,), (1,)), ((), ())), preferred_element_type=F32)
            if masked:
                s = jnp.where(mask, s, -jnp.inf)
            m_new = jnp.maximum(m, jnp.max(s, axis=-1, keepdims=True))
            p = jnp.exp2((s - m_new) * scale)
            alpha = jnp.exp2((m - m_new) * scale)
            l = l * alpha + jnp.sum(p, axis=-1, keepdims=True)
            acc = acc * alpha + jnp.dot(p.astype(BF16), v_blk, preferred_element_type=F32)
            out.append((m_new, l, acc))
        return tuple(out)

    carry = tuple((jnp.full((bq, 1), -jnp.inf, F32), jnp.zeros((bq, 1), F32), jnp.zeros((bq, head_dim), F32)) for _ in range(heads))
    carry = step(block * bq, bq, carry, True)
    full = lax.div(block * bq, bk)
    carry = lax.fori_loop(0, full, lambda j, cur: step(j * bk, bk, cur, False), carry)
    carry = lax.fori_loop(full * (bk // bq), block, lambda j, cur: step(j * bq, bq, cur, False), carry)
    return [(acc / l).astype(BF16) for _, l, acc in carry]


def attn_kernel(layer, n_tp, n_kv, heads, head_dim, bk, r_hbm, gain_ref, far_ref, near_ref, wq_hbm, wkv_hbm, wo_hbm, out_hbm,
                x, rin, wq, wkv, wide, w_kv, w_q, rope, kv_out, q_out, qkv_ref, wo, ctx, ctx_out, res,
                lsem, ks, kr, km, kn, qs, qr, cs, cr, es, *gather_sem):
    t, (yy, xx, c), (mate, dev_x, dev_y) = coords()
    z = lax.axis_index('dp')
    dev_d = dev_x + dev_y - t
    dev_f = dev_x + c * (dev_y - dev_x)
    dev_s = dev_y + c * (dev_x - dev_y)
    rows, width = res.shape
    half = rows // 2
    cols = heads * head_dim

    load_r = pltpu.make_async_copy(r_hbm, rin, lsem.at[0])
    load_q = pltpu.make_async_copy(wq_hbm.at[layer], wq, lsem.at[1])
    load_r.start()
    load_q.start()
    others = [lax.rem(t + k, n_tp) for k in range(1, n_tp)]
    greet(others)
    pl.semaphore_signal(pltpu.get_barrier_semaphore(), inc=1, device_id={'dp': 1 - z, 'tp': t}, device_id_type=MESH)
    own_o = pl.ds(pl.multiple_of(t * cols, cols), cols)
    load_kv = pltpu.make_async_copy(wkv_hbm.at[layer], wkv, lsem.at[2])
    load_o = pltpu.make_async_copy(wo_hbm.at[layer], wo.at[own_o], lsem.at[3])
    load_kv.start()
    load_o.start()
    place = (t, z, mate, dev_f, dev_s, dev_d)
    get_q = WeightGather(w_q, width, gather_sem[:6], *place)
    get_o = WeightGather(wo, cols, gather_sem[6:], *place)
    nd = 256

    def deinterleave(raw, count, dst, first, order):
        @pl.loop(0, width // nd)
        def _(b):
            wide[pl.ds(0, count * nd), :] = raw[pl.ds(pl.multiple_of(b * count * nd, nd), count * nd), :].astype(F32)
            for h in range(count):
                dst[pl.ds(pl.multiple_of(first + b * nd, nd), nd), h * head_dim:(h + 1) * head_dim] = wide[pl.ds(order[h], nd, stride=count), :].astype(BF16)

    load_q.wait()
    deinterleave(wq, heads, w_q, t * width, range(heads))
    pl.semaphore_wait(pltpu.get_barrier_semaphore(), n_tp)
    get_q.start()

    load_r.wait()
    norm_rows(rin, gain_ref[layer:layer + 1], x, 0, rows)
    for k in range(2):
        at = slice(k * half, (k + 1) * half)
        cos_f, sin_f = far_ref[0, pl.ds(t * 2 + k, 1), :], far_ref[1, pl.ds(t * 2 + k, 1), :]
        rope[0, at] = cos_f * near_ref[0] - sin_f * near_ref[1]
        rope[1, at] = sin_f * near_ref[0] + cos_f * near_ref[1]

    def rotate(v):
        return (v * rope[0] + pltpu.roll(v, head_dim // 2, 1) * rope[1]).astype(BF16)

    own = pl.ds(pl.multiple_of(t * rows, rows), rows)
    kv_cols = pl.ds(cols, 2 * head_dim)
    q_cols = pl.ds(0, cols)
    load_kv.wait()
    deinterleave(wkv, 2 * n_kv, w_kv, 0, [g + n_kv * k for g in range(n_kv) for k in range(2)])

    @pl.loop(0, n_kv)
    def _(g):
        at = pl.ds(pl.multiple_of(g * 2 * head_dim, 2 * head_dim), 2 * head_dim)
        proj = jnp.dot(x[...], w_kv[:, at], preferred_element_type=F32)
        kv_out[g, :, 0:head_dim] = rotate(proj[:, 0:head_dim])
        kv_out[g, :, head_dim:2 * head_dim] = proj[:, head_dim:2 * head_dim].astype(BF16)

    def kv_send(k, dev):
        return rcopy(kv_out.at[lax.div(dev * n_kv, n_tp)], qkv_ref.at[own, kv_cols], ks.at[k], kr.at[k], dev)

    def kv_mate(k, dev):
        at = pl.ds(pl.multiple_of(dev * rows, rows), rows)
        return rcopy(qkv_ref.at[at, kv_cols], qkv_ref.at[at, kv_cols], km.at[k], kn.at[k], mate)

    near = (dev_x, dev_y, dev_d)
    sends = [kv_send(k, dev) for k, dev in enumerate(near)]
    for copy in sends:
        copy.start()
    qkv_ref[own, kv_cols] = kv_out[lax.div(t * n_kv, n_tp)]
    hand_on = [kv_mate(k, dev) for k, dev in enumerate(near)] + [
        rcopy(kv_out.at[lax.div(t * n_kv, n_tp)], qkv_ref.at[own, kv_cols], km.at[3], kn.at[3], mate)]
    hand_on[3].start()

    def block_of(i):
        w = lax.div(i, 2)
        j = lax.rem(i, 2)
        core = c + j - 2 * c * j
        one = lax.rem(lax.div(w + 1, 2), 2)
        two = lax.div(w, 2)
        flip_x = one + core * (two - one)
        flip_y = two + core * (one - two)
        return (2 * (yy + flip_y - 2 * yy * flip_y) + xx + flip_x - 2 * xx * flip_x) * 2 + core

    def project(i):
        dev = block_of(i)
        proj = jnp.dot(x[...], w_q[pl.ds(pl.multiple_of(dev * width, width), width), :], preferred_element_type=F32)
        for h in range(heads):
            at_h = slice(h * head_dim, (h + 1) * head_dim)
            q_out[i, :, at_h] = rotate(proj[:, at_h])

    def q_send(i):
        return rcopy(q_out.at[i], qkv_ref.at[own, q_cols], qs.at[i], qr.at[t], block_of(i))

    def take_kv():
        for k in range(3):
            at = pl.ds(pl.multiple_of(near[k] * rows, rows), rows)
            pltpu.make_async_copy(kv_out.at[0], qkv_ref.at[at, kv_cols], kr.at[k]).wait()
            hand_on[k].start()
        for copy in hand_on:
            copy.wait_recv()

    def ctx_send(i, dev):
        return rcopy(ctx_out.at[i], ctx.at[t], cs.at[i], cr.at[t], dev)

    load_o.wait()

    @pl.loop(0, n_tp)
    def _(n):
        i = n + jnp.where(n < 4, 0, jnp.where(n < 6, 2, -2))
        block = block_of(i)

        @pl.when(n == 0)
        def _():
            get_q.from_mate([12])

        @pl.when(n == 1)
        def _():
            get_q.received((4, 5))

        @pl.when(n == 2)
        def _():
            get_q.from_z(range(4))
            get_q.from_mate((0, 1, 2, 3, 6, 7, 8, 9))

        @pl.when(n == 4)
        def _():
            get_q.from_z((4, 5))
            get_q.from_mate((4, 5, 10, 11))

        @pl.when((n == 0) | (n == 2) | (n == 4))
        def _():
            @pl.loop(0, jnp.where(n == 2, 4, 2))
            def _(m):
                which = n + m + jnp.where(m < 2, 0, 2)
                project(which)

                @pl.when(which >= 1)
                def _():
                    q_send(which).start()

        @pl.when(n == 0)
        def _():
            qkv_ref[own, q_cols] = q_out[0]
            get_q.received(range(4))
            take_kv()
            get_o.start()

        @pl.when(n == 2)
        def _():
            get_o.received(range(4))

        @pl.when(n == 4)
        def _():
            get_o.received((4, 5))

        @pl.when(n == 7)
        def _():
            get_o.from_z(range(4))

        @pl.when(n >= 1)
        def _():
            pltpu.make_async_copy(q_out.at[0], qkv_ref.at[pl.ds(pl.multiple_of(block * rows, rows), rows), q_cols], qr.at[block]).wait()
        for h, val in enumerate(attend(qkv_ref, block, rows, bk, heads, head_dim)):
            ctx_out[i, :, h * head_dim:(h + 1) * head_dim] = val

        @pl.when(n >= 1)
        def _():
            ctx_send(i, block).start()

    ctx[t] = ctx_out[0]
    res[...] = rin[...].astype(F32)
    get_o.from_z((4, 5))
    get_o.from_mate(range(13))
    nc = 512

    @pl.loop(0, n_tp)
    def _(n):
        dev = block_of(n + jnp.where(n < 4, 0, jnp.where(n < 6, 2, -2)))

        @pl.when(n >= 1)
        def _():
            pltpu.make_async_copy(ctx_out.at[0], ctx.at[dev], cr.at[dev]).wait()
        rows_o = pl.ds(pl.multiple_of(dev * cols, cols), cols)

        @pl.loop(0, width // nc)
        def _(k):
            at = pl.ds(pl.multiple_of(k * nc, nc), nc)
            res[:, at] = res[:, at] + jnp.dot(ctx[dev], wo[rows_o, at], preferred_element_type=F32)

            @pl.when(n == n_tp - 1)
            def _():
                pltpu.make_async_copy(res.at[:, at], out_hbm.at[:, at], es.at[k]).start()

    get_q.finish()
    get_o.finish()
    for copy in sends + hand_on:
        copy.wait_send()
    for i in range(1, n_tp):
        q_send(jnp.int32(i)).wait_send()
        ctx_send(i, mate).wait_send()
    for k in range(width // nc):
        at = pl.ds(k * nc, nc)
        pltpu.make_async_copy(res.at[:, at], out_hbm.at[:, at], es.at[k]).wait()


def attention(layer, resid, gain, far, near, w_q, w_kv, w_o, n_tp, bk=1024):
    rows, width = resid.shape
    cols, head_dim = w_o.shape[1], w_q.shape[2]
    heads = cols // head_dim
    n_kv = w_kv.shape[1] // (2 * width)
    seq = rows * n_tp
    vmem = pl.BlockSpec(memory_space=pltpu.VMEM)
    anywhere = pl.BlockSpec(memory_space=pl.ANY)
    dma = pltpu.SemaphoreType.DMA
    return pl.pallas_call(
        functools.partial(attn_kernel, layer, n_tp, n_kv, heads, head_dim, bk),
        out_shape=jax.ShapeDtypeStruct((rows, width), F32),
        in_specs=[anywhere, vmem, vmem, vmem, anywhere, anywhere, anywhere],
        out_specs=anywhere,
        scratch_shapes=[
            pltpu.VMEM((rows, width), BF16),
            pltpu.VMEM((rows, width), resid.dtype),
            pltpu.VMEM(w_q.shape[1:], BF16),
            pltpu.VMEM(w_kv.shape[1:], BF16),
            pltpu.VMEM((256 * max(heads, 2 * n_kv), head_dim), F32),
            pltpu.VMEM((width, 2 * n_kv * head_dim), BF16),
            pltpu.VMEM((n_tp * width, cols), BF16),
            pltpu.VMEM((2, rows, head_dim), F32),
            pltpu.VMEM((n_kv, rows, 2 * head_dim), BF16),
            pltpu.VMEM((n_tp, rows, cols), BF16),
            pltpu.VMEM((seq, cols + 2 * head_dim), BF16),
            pltpu.VMEM((n_tp * cols, width), BF16),
            pltpu.VMEM((n_tp, rows, cols), BF16),
            pltpu.VMEM((n_tp, rows, cols), BF16),
            pltpu.VMEM((rows, width), F32),
            dma((4,)), dma((3,)), dma((3,)), dma((4,)), dma((4,)), dma((n_tp,)), dma((n_tp,)), dma((n_tp,)), dma((n_tp,)), dma((4,)),
        ] + weight_sems() + weight_sems(),
        compiler_params=pltpu.CompilerParams(collective_id=1 + layer, has_side_effects=True, vmem_limit_bytes=VMEM_MAX),
        cost_estimate=pl.CostEstimate(flops=2 * seq * seq * cols, bytes_accessed=4 * seq * cols, transcendentals=seq * seq),
        name="attention" + str(layer),
    )(resid, gain, far, near, w_q, w_kv, w_o)


def mlp_kernel(layer, r_hbm, gain_ref, wg_hbm, wu_hbm, wd_hbm, out_hbm,
               wg, wu, wd, xbuf, prec, recv, acc, stash, act,
               lsem, sx, sy, ag, fs, fr, ps, pr, rr, ss):
    _, _, partners = coords()
    mate, dev_x, dev_y = partners
    rows, width = acc.shape
    half = rows // 2
    hid = act.shape[1]
    h0, h1 = pl.ds(0, half), pl.ds(half, half)
    nb = 64

    load_r = pltpu.make_async_copy(r_hbm, acc, lsem.at[0])
    load_r.start()
    greet(partners)
    loads = [pltpu.make_async_copy(src.at[layer], dst, lsem.at[k + 1]) for k, (src, dst) in enumerate(((wg_hbm, wg), (wu_hbm, wu), (wd_hbm, wd)))]
    load_r.wait()
    for copy in loads:
        copy.start()
    gather = RowGather(xbuf, sx, sy, ag, fs, fr, partners)
    gather.start(lambda k: norm_rows(acc, gain_ref[layer:layer + 1], xbuf.at[0, 0], k * half, half))

    def partial_send(w):
        return rcopy(xbuf.at[w, 1], prec.at[w], ps.at[w], pr.at[w], mate)

    stage = (rcopy(xbuf.at[1, 1, h0], recv.at[0], ss.at[0], rr.at[0], dev_x),
             rcopy(xbuf.at[1, 1, h1], recv.at[1], ss.at[1], rr.at[1], dev_y))
    quarter = half // 2
    cuts = [(k, m, pl.ds(m * quarter, quarter), pl.ds(k * half + m * quarter, quarter)) for m in range(2) for k in range(2)]
    to_first, to_second = (dev_x, dev_y), (dev_y, dev_x)
    stage_two = [rcopy(xbuf.at[2, 1, to], recv.at[2 + k, at], ss.at[2 + k + 2 * m], rr.at[2 + k + 2 * m], to_first[k]) for k, m, at, to in cuts]
    stage_three = [rcopy(xbuf.at[3, 1, to], recv.at[4 + k, at], ss.at[6 + k + 2 * m], rr.at[6 + k + 2 * m], to_second[k]) for k, m, at, to in cuts]

    for copy in loads:
        copy.wait()
    cut = 768
    nd = 1024

    def gate_up(x_at, at):
        g = lax.dot_general(x_at[...], wg[at, :], (((1,), (1,)), ((), ())), preferred_element_type=F32)
        u = lax.dot_general(x_at[...], wu[at, :], (((1,), (1,)), ((), ())), preferred_element_type=F32)
        act[:, at] = (g * jax.nn.sigmoid(g) * u).astype(BF16)

    @pl.loop(0, 8)
    def _(s):
        w = lax.div(s, 2)
        rc = 1 - lax.rem(s, 2)

        @pl.when(rc == 1)
        def _():
            gather.forward(w).wait_recv()
        x_at = xbuf.at[w, rc]
        gate_up(x_at, pl.ds(0, cut))
        gate_up(x_at, pl.ds(cut, hid - cut))

        @pl.when(rc == 0)
        def _():
            @pl.when(w < 3)
            def _():
                gather.arrive(w + 1)
            partial_send(w).wait()

        @pl.loop(0, width // nd)
        def _(n):
            at = pl.ds(pl.multiple_of(n * nd, nd), nd)
            val = jnp.dot(act[...], wd[:, at], preferred_element_type=F32)

            @pl.when(rc == 1)
            def _():
                xbuf[w, 1, :, at] = val.astype(BF16)

            @pl.when(rc == 0)
            def _():
                total = val + prec[w, :, at].astype(F32)

                @pl.when(w == 0)
                def _():
                    acc[:, at] = acc[:, at] + total

                @pl.when(w == 3)
                def _():
                    stash[:, at] = total

                @pl.when((w == 1) | (w == 2))
                def _():
                    xbuf[w, 1, :, at] = total.astype(BF16)

        @pl.when(rc == 1)
        def _():
            partial_send(w).start()

        @pl.when(s == 3)
        def _():
            stage[0].start()
            stage[1].start()

        @pl.when(s == 5)
        def _():
            for copy in stage_two:
                copy.start()

    def rows_from(first, count):
        def each(fn):
            @pl.loop(0, count // nb)
            def _(b):
                fn(pl.multiple_of(b * nb, nb), pl.ds(pl.multiple_of(first + b * nb, nb), nb))
        return each

    for k in range(2):
        stage[k].wait_recv()

        @rows_from(k * half, half)
        def _(at, to):
            acc[to, :] = acc[to, :] + recv[k, pl.ds(at, nb), :].astype(F32)
    for copy, send, (k, m, _, _) in zip(stage_two, stage_three, cuts):
        copy.wait_recv()

        @rows_from(k * half + m * quarter, quarter)
        def _(at, to):
            xbuf[3, 1, to, :] = (stash[to, :] + recv[2 + k, pl.ds(m * quarter + at, nb), :].astype(F32)).astype(BF16)
        send.start()
    gather.finish()
    narrow = out_hbm.dtype == BF16
    final = xbuf.at[0, 0] if narrow else acc
    outs = []
    for copy, (k, m, _, out_at) in zip(stage_three, cuts):
        copy.wait_recv()

        @rows_from(k * half + m * quarter, quarter)
        def _(at, to):
            final[to, :] = (acc[to, :] + recv[4 + k, pl.ds(m * quarter + at, nb), :].astype(F32)).astype(final.dtype)
        outs.append(pltpu.make_async_copy(final.at[out_at], out_hbm.at[out_at], lsem.at[k + 2 * m]))
        outs[-1].start()
    for copy in list(stage) + stage_two + stage_three:
        copy.wait_send()
    for copy in outs:
        copy.wait()


def mlp(layer, resid, gain, w_gate, w_up, w_down, out_dtype):
    rows, width = resid.shape
    hid = w_gate.shape[1]
    half = rows // 2
    any_spec = pl.BlockSpec(memory_space=pl.ANY)
    dma = pltpu.SemaphoreType.DMA
    return pl.pallas_call(
        functools.partial(mlp_kernel, layer),
        out_shape=jax.ShapeDtypeStruct((rows, width), out_dtype),
        in_specs=[any_spec, pl.BlockSpec(memory_space=pltpu.VMEM), any_spec, any_spec, any_spec],
        out_specs=any_spec,
        scratch_shapes=[
            pltpu.VMEM((hid, width), BF16),
            pltpu.VMEM((hid, width), BF16),
            pltpu.VMEM((hid, width), BF16),
            pltpu.VMEM((4, 2, rows, width), BF16),
            pltpu.VMEM((4, rows, width), BF16),
            pltpu.VMEM((6, half, width), BF16),
            pltpu.VMEM((rows, width), F32),
            pltpu.VMEM((rows, width), F32),
            pltpu.VMEM((rows, hid), BF16),
            dma((4,)),
        ] + gather_sems() + [dma((4,)), dma((4,)), dma((10,)), dma((10,))],
        compiler_params=pltpu.CompilerParams(collective_id=5 + layer, has_side_effects=True, vmem_limit_bytes=VMEM_MAX),
        cost_estimate=pl.CostEstimate(flops=6 * 8 * rows * width * hid, bytes_accessed=6 * width * hid, transcendentals=8 * rows * hid),
        name="mlp" + str(layer),
    )(resid, gain, w_gate, w_up, w_down)


def solution(mesh):
    n_tp = mesh.shape['tp']
    tok_spec = P('dp', 'tp', None)
    in_specs = (tok_spec, P(), P(None, None, 'tp', None), P(), P(None, 'tp', None, None), P(), P(None, None, 'tp'), P(None, None, 'tp'), P(None, 'tp', None))

    def body(hidden, norm_attn, w_q, w_kv, w_o, norm_mlp, w_gate, w_up, w_down):
        n_layers, width, heads, head_dim = w_q.shape
        n_kv = w_kv.shape[3]
        rows = hidden.shape[1]
        far, near = rope_tables(rows * n_tp, rows // 2, head_dim)
        w_q = w_q.reshape(n_layers, width * heads, head_dim)
        w_kv = w_kv.reshape(n_layers, width * 2 * n_kv, head_dim)
        w_o = w_o.reshape(n_layers, heads * head_dim, width)
        w_gate = jnp.swapaxes(w_gate, 1, 2)
        w_up = jnp.swapaxes(w_up, 1, 2)
        resid = hidden[0]
        for layer in range(n_layers):
            resid = attention(layer, resid, norm_attn, far, near, w_q, w_kv, w_o, n_tp)
            resid = mlp(layer, resid, norm_mlp, w_gate, w_up, w_down, BF16 if layer == n_layers - 1 else F32)
        return resid[None]

    return jax.shard_map(body, mesh=mesh, in_specs=in_specs, out_specs=tok_spec, check_vma=False)
```

```python
import functools
import math
import jax
import jax.numpy as jnp
import numpy as np
from jax import lax
from jax.experimental import pallas as pl
from jax.experimental.pallas import tpu as pltpu
from jax.sharding import PartitionSpec as P

EPS = 1e-5
ROPE_BASE = 10000.0
MESH = pl.DeviceIdType.MESH
VMEM_MAX = 67043328
F32 = jnp.float32
BF16 = jnp.bfloat16


def rope_tables(seq, step, head_dim):
    half_dim = head_dim // 2
    inv_freq = ROPE_BASE ** (-2.0 * np.arange(half_dim, dtype=np.float64) / head_dim)

    def table(positions):
        angles = positions.astype(np.float64)[:, None] * inv_freq[None, :]
        cos_t, sin_t = np.cos(angles), np.sin(angles)
        return np.stack([np.concatenate([cos_t, cos_t], axis=1), np.concatenate([-sin_t, sin_t], axis=1)]).astype(np.float32)

    return table(np.arange(0, seq, step)), table(np.arange(step))


def coords():
    t = lax.axis_index('tp')
    c = lax.rem(t, 2)
    xx = lax.rem(lax.div(t, 2), 2)
    yy = lax.div(t, 4)
    return t, (yy, xx, c), (t + 1 - 2 * c, t + 2 - 4 * xx, t + 4 - 8 * yy)


def rcopy(src, dst, ssem, rsem, dev):
    return pltpu.make_async_remote_copy(src_ref=src, dst_ref=dst, send_sem=ssem, recv_sem=rsem,
                                        device_id={'tp': dev}, device_id_type=MESH)


def greet(devices):
    for dev in devices:
        pl.semaphore_signal(pltpu.get_barrier_semaphore(), inc=1, device_id={'tp': dev}, device_id_type=MESH)


class RowGather:
    def __init__(self, xbuf, sx, sy, ag, fs, fr, partners):
        mate, dev_x, dev_y = partners
        rows = xbuf.shape[2]
        half = rows // 2
        lead = half // 4
        h0, h1 = pl.ds(0, half), pl.ds(half, half)
        own = xbuf.at[0, 0]
        self.xbuf, self.ag, self.fs, self.fr, self.mate = xbuf, ag, fs, fr, mate
        self.halves = (h0, h1)

        def piece(k, sem, dev, first, size, window, slot):
            at = pl.ds(first, size)
            return rcopy(own.at[at], xbuf.at[window, 0, at], sem.at[k], ag.at[window, slot], dev)

        self.first = (piece(0, sx, dev_x, 0, half, 1, 0), piece(0, sy, dev_y, half, half, 1, 1))
        self.lead = (piece(1, sx, dev_x, half, lead, 3, 1), piece(1, sy, dev_y, 0, lead, 3, 0))
        self.rest = (piece(2, sx, dev_x, half + lead, half - lead, 3, 1), piece(2, sy, dev_y, lead, half - lead, 3, 0))
        self.relay = (rcopy(xbuf.at[1, 0, h1], xbuf.at[2, 0, h1], sx.at[3], ag.at[2, 1], dev_x),
                      rcopy(xbuf.at[1, 0, h0], xbuf.at[2, 0, h0], sy.at[3], ag.at[2, 0], dev_y))

    def forward(self, w):
        return rcopy(self.xbuf.at[w, 0], self.xbuf.at[w, 1], self.fs.at[w], self.fr.at[w], self.mate)

    def start(self, norm_half):
        norm_half(0)
        pl.semaphore_wait(pltpu.get_barrier_semaphore(), 3)
        self.first[0].start()
        norm_half(1)
        self.first[1].start()
        self.lead[0].start()
        self.lead[1].start()
        self.forward(0).start()

    def arrive(self, w):
        for k in range(2):
            at = self.halves[k]
            pltpu.make_async_copy(self.xbuf.at[0, 0, at], self.xbuf.at[w, 0, at], self.ag.at[w, k]).wait()

        @pl.when(w == 1)
        def _():
            for copy in self.relay + self.rest:
                copy.start()
        self.forward(w).start()

    def finish(self):
        for copy in self.first + self.lead + self.relay + self.rest:
            copy.wait_send()
        for w in range(4):
            self.forward(w).wait_send()


def gather_sems():
    dma = pltpu.SemaphoreType.DMA
    return [dma((4,)), dma((4,)), dma((4, 2)), dma((4,)), dma((4,))]


def norm_rows(src, gain, dst, first, count):
    nb = 64

    @pl.loop(0, count // nb)
    def _(b):
        at = pl.ds(pl.multiple_of(first + b * nb, nb), nb)
        r = src[at, :].astype(F32)
        mean_sq = jnp.mean(r * r, axis=-1, keepdims=True)
        dst[at, :] = (r * lax.rsqrt(mean_sq + EPS) * gain).astype(BF16)


class WeightGather:
    def __init__(self, buf, unit, sems, t, z, mate, dev_f, dev_s, dev_d):
        so, sz, oa, ob, om, on = sems
        part = unit // 4
        self.buf, self.oa, self.ob, self.z = buf, oa, ob, z
        self.from_dev = ((dev_f, 0), (dev_s, 1), (dev_f, 1), (dev_s, 0), (dev_d, 1), (dev_d, 0))

        def span(dev, k, p):
            return pl.ds(pl.multiple_of(dev * unit + (2 * k + p) * part, part), part)

        def same(at, ssem, rsem, dev):
            return rcopy(buf.at[at], buf.at[at], ssem, rsem, dev)

        def across(at, ssem, rsem):
            return pltpu.make_async_remote_copy(src_ref=buf.at[at], dst_ref=buf.at[at], send_sem=ssem, recv_sem=rsem,
                                                device_id={'dp': 1 - z, 'tp': t}, device_id_type=MESH)

        self.span = span
        self.send = (same(span(t, 0, z), so.at[0], oa.at[0], dev_f), same(span(t, 1, z), so.at[1], oa.at[1], dev_s),
                     same(span(t, 1, z), so.at[2], oa.at[2], dev_f), same(span(t, 0, z), so.at[3], oa.at[3], dev_s))
        self.relay = (same(span(dev_s, 1, z), so.at[4], oa.at[4], dev_f), same(span(dev_f, 0, z), so.at[5], oa.at[5], dev_s))
        self.via_z = [across(span(dev, k, z), sz.at[i], ob.at[i]) for i, (dev, k) in enumerate(self.from_dev)]
        self.to_mate = [same(span(dev, k, z), om.at[i], on.at[i], mate) for i, (dev, k) in enumerate(self.from_dev)]
        self.to_mate += [same(span(dev, k, 1 - z), om.at[6 + i], on.at[6 + i], mate) for i, (dev, k) in enumerate(self.from_dev)]
        own = pl.ds(pl.multiple_of(t * unit, unit), unit)
        self.to_mate.append(same(own, om.at[12], on.at[12], mate))

    def take(self, i, sem, p):
        at = self.span(self.from_dev[i][0], self.from_dev[i][1], p)
        pltpu.make_async_copy(self.buf.at[at], self.buf.at[at], sem.at[i]).wait()

    def start(self):
        for copy in self.send:
            copy.start()
        self.to_mate[12].start()

    def received(self, pieces):
        for i in pieces:
            self.take(i, self.oa, self.z)
            if i < 2:
                self.relay[1 - i].start()
            self.via_z[i].start()
            self.to_mate[i].start()

    def from_z(self, pieces):
        for i in pieces:
            self.take(i, self.ob, 1 - self.z)
            self.to_mate[6 + i].start()

    def from_mate(self, pieces):
        for i in pieces:
            self.to_mate[i].wait_recv()

    def finish(self):
        for copy in list(self.send + self.relay) + self.via_z + self.to_mate:
            copy.wait_send()


def weight_sems():
    dma = pltpu.SemaphoreType.DMA
    return [dma((6,)), dma((6,)), dma((6,)), dma((6,)), dma((13,)), dma((13,))]


def attend(qkv_ref, block, bq, bk, heads, head_dim):
    scale = math.log2(math.e) / math.sqrt(head_dim)
    mask = lax.broadcasted_iota(jnp.int32, (bq, bq), 0) <= lax.broadcasted_iota(jnp.int32, (bq, bq), 1)
    q_at = pl.ds(pl.multiple_of(block * bq, bq), bq)
    qs = [qkv_ref[q_at, h * head_dim:(h + 1) * head_dim] for h in range(heads)]

    def step(first, count, carry, masked):
        at = pl.ds(pl.multiple_of(first, bq), count)
        k_blk = qkv_ref[at, heads * head_dim:(heads + 1) * head_dim]
        v_blk = qkv_ref[at, (heads + 1) * head_dim:(heads + 2) * head_dim]
        out = []
        for h in range(heads):
            m, l, acc = carry[h]
            s = lax.dot_general(k_blk, qs[h], (((1,), (1,)), ((), ())), preferred_element_type=F32)
            if masked:
                s = jnp.where(mask, s, -jnp.inf)
            m_new = jnp.maximum(m, jnp.max(s, axis=0, keepdims=True))
            p = jnp.exp2((s - m_new) * scale)
            alpha = jnp.exp2((m - m_new) * scale)
            l = l * alpha + jnp.sum(p, axis=0, keepdims=True)
            acc = acc * alpha + lax.dot_general(v_blk, p.astype(BF16), (((0,), (0,)), ((), ())), preferred_element_type=F32)
            out.append((m_new, l, acc))
        return tuple(out)

    carry = tuple((jnp.full((1, bq), -jnp.inf, F32), jnp.zeros((1, bq), F32), jnp.zeros((head_dim, bq), F32)) for _ in range(heads))
    carry = step(block * bq, bq, carry, True)
    full = lax.div(block * bq, bk)
    carry = lax.fori_loop(0, full, lambda j, cur: step(j * bk, bk, cur, False), carry)
    carry = lax.fori_loop(full * (bk // bq), block, lambda j, cur: step(j * bq, bq, cur, False), carry)
    return [(acc / l).T.astype(BF16) for _, l, acc in carry]


def attn_kernel(layer, n_tp, n_kv, heads, head_dim, bk, r_hbm, gain_ref, far_ref, near_ref, wq_hbm, wkv_hbm, wo_hbm, out_hbm,
                x, rin, wq, wkv, wide, w_kv, w_q, rope, kv_out, q_out, qkv_ref, wo, ctx, ctx_out, res,
                lsem, ks, kr, km, kn, qs, qr, cs, cr, es, *gather_sem):
    t, (yy, xx, c), (mate, dev_x, dev_y) = coords()
    z = lax.axis_index('dp')
    dev_d = dev_x + dev_y - t
    dev_f = dev_x + c * (dev_y - dev_x)
    dev_s = dev_y + c * (dev_x - dev_y)
    rows, width = res.shape
    half = rows // 2
    cols = heads * head_dim

    load_r = pltpu.make_async_copy(r_hbm, rin, lsem.at[0])
    load_q = pltpu.make_async_copy(wq_hbm.at[layer], wq, lsem.at[1])
    load_r.start()
    load_q.start()
    others = [lax.rem(t + k, n_tp) for k in range(1, n_tp)]
    greet(others)
    pl.semaphore_signal(pltpu.get_barrier_semaphore(), inc=1, device_id={'dp': 1 - z, 'tp': t}, device_id_type=MESH)
    own_o = pl.ds(pl.multiple_of(t * cols, cols), cols)
    load_kv = pltpu.make_async_copy(wkv_hbm.at[layer], wkv, lsem.at[2])
    load_o = pltpu.make_async_copy(wo_hbm.at[layer], wo.at[own_o], lsem.at[3])
    load_kv.start()
    load_o.start()
    place = (t, z, mate, dev_f, dev_s, dev_d)
    get_q = WeightGather(w_q, width, gather_sem[:6], *place)
    get_o = WeightGather(wo, cols, gather_sem[6:], *place)
    nd = 256

    def deinterleave(raw, count, dst, first, order):
        @pl.loop(0, width // nd)
        def _(b):
            wide[pl.ds(0, count * nd), :] = raw[pl.ds(pl.multiple_of(b * count * nd, nd), count * nd), :].astype(F32)
            for h in range(count):
                dst[pl.ds(pl.multiple_of(first + b * nd, nd), nd), h * head_dim:(h + 1) * head_dim] = wide[pl.ds(order[h], nd, stride=count), :].astype(BF16)

    load_q.wait()
    deinterleave(wq, heads, w_q, t * width, range(heads))
    pl.semaphore_wait(pltpu.get_barrier_semaphore(), n_tp)
    get_q.start()

    load_r.wait()
    norm_rows(rin, gain_ref[layer:layer + 1], x, 0, rows)
    for k in range(2):
        at = slice(k * half, (k + 1) * half)
        cos_f, sin_f = far_ref[0, pl.ds(t * 2 + k, 1), :], far_ref[1, pl.ds(t * 2 + k, 1), :]
        rope[0, at] = cos_f * near_ref[0] - sin_f * near_ref[1]
        rope[1, at] = sin_f * near_ref[0] + cos_f * near_ref[1]

    def rotate(v):
        return (v * rope[0] + pltpu.roll(v, head_dim // 2, 1) * rope[1]).astype(BF16)

    own = pl.ds(pl.multiple_of(t * rows, rows), rows)
    kv_cols = pl.ds(cols, 2 * head_dim)
    q_cols = pl.ds(0, cols)
    load_kv.wait()
    deinterleave(wkv, 2 * n_kv, w_kv, 0, [g + n_kv * k for g in range(n_kv) for k in range(2)])

    @pl.loop(0, n_kv)
    def _(g):
        at = pl.ds(pl.multiple_of(g * 2 * head_dim, 2 * head_dim), 2 * head_dim)
        proj = jnp.dot(x[...], w_kv[:, at], preferred_element_type=F32)
        kv_out[g, :, 0:head_dim] = rotate(proj[:, 0:head_dim])
        kv_out[g, :, head_dim:2 * head_dim] = proj[:, head_dim:2 * head_dim].astype(BF16)

    def kv_send(k, dev):
        return rcopy(kv_out.at[lax.div(dev * n_kv, n_tp)], qkv_ref.at[own, kv_cols], ks.at[k], kr.at[k], dev)

    def kv_mate(k, dev):
        at = pl.ds(pl.multiple_of(dev * rows, rows), rows)
        return rcopy(qkv_ref.at[at, kv_cols], qkv_ref.at[at, kv_cols], km.at[k], kn.at[k], mate)

    near = (dev_x, dev_y, dev_d)
    sends = [kv_send(k, dev) for k, dev in enumerate(near)]
    for copy in sends:
        copy.start()
    qkv_ref[own, kv_cols] = kv_out[lax.div(t * n_kv, n_tp)]
    hand_on = [kv_mate(k, dev) for k, dev in enumerate(near)] + [
        rcopy(kv_out.at[lax.div(t * n_kv, n_tp)], qkv_ref.at[own, kv_cols], km.at[3], kn.at[3], mate)]
    hand_on[3].start()

    def block_of(i):
        w = lax.div(i, 2)
        j = lax.rem(i, 2)
        core = c + j - 2 * c * j
        one = lax.rem(lax.div(w + 1, 2), 2)
        two = lax.div(w, 2)
        flip_x = one + core * (two - one)
        flip_y = two + core * (one - two)
        return (2 * (yy + flip_y - 2 * yy * flip_y) + xx + flip_x - 2 * xx * flip_x) * 2 + core

    def project(i):
        dev = block_of(i)
        proj = jnp.dot(x[...], w_q[pl.ds(pl.multiple_of(dev * width, width), width), :], preferred_element_type=F32)
        for h in range(heads):
            at_h = slice(h * head_dim, (h + 1) * head_dim)
            q_out[i, :, at_h] = rotate(proj[:, at_h])

    def q_send(i):
        return rcopy(q_out.at[i], qkv_ref.at[own, q_cols], qs.at[i], qr.at[t], block_of(i))

    def take_kv():
        for k in range(3):
            at = pl.ds(pl.multiple_of(near[k] * rows, rows), rows)
            pltpu.make_async_copy(kv_out.at[0], qkv_ref.at[at, kv_cols], kr.at[k]).wait()
            hand_on[k].start()
        for copy in hand_on:
            copy.wait_recv()

    def ctx_send(i, dev):
        return rcopy(ctx_out.at[i], ctx.at[t], cs.at[i], cr.at[t], dev)

    load_o.wait()

    @pl.loop(0, n_tp)
    def _(n):
        i = n + jnp.where(n < 4, 0, jnp.where(n < 6, 2, -2))
        block = block_of(i)

        @pl.when(n == 0)
        def _():
            get_q.from_mate([12])

        @pl.when(n == 1)
        def _():
            get_q.received((4, 5))

        @pl.when(n == 2)
        def _():
            get_q.from_z(range(4))
            get_q.from_mate((0, 1, 2, 3, 6, 7, 8, 9))

        @pl.when(n == 4)
        def _():
            get_q.from_z((4, 5))
            get_q.from_mate((4, 5, 10, 11))

        @pl.when((n == 0) | (n == 2) | (n == 4))
        def _():
            @pl.loop(0, jnp.where(n == 2, 4, 2))
            def _(m):
                which = n + m + jnp.where(m < 2, 0, 2)
                project(which)

                @pl.when(which >= 1)
                def _():
                    q_send(which).start()

        @pl.when(n == 0)
        def _():
            qkv_ref[own, q_cols] = q_out[0]
            get_q.received(range(4))
            get_o.start()
            take_kv()

        @pl.when(n == 2)
        def _():
            get_o.received(range(4))

        @pl.when(n == 4)
        def _():
            get_o.received((4, 5))

        @pl.when(n == 7)
        def _():
            get_o.from_z(range(4))

        @pl.when(n >= 1)
        def _():
            pltpu.make_async_copy(q_out.at[0], qkv_ref.at[pl.ds(pl.multiple_of(block * rows, rows), rows), q_cols], qr.at[block]).wait()
        for h, val in enumerate(attend(qkv_ref, block, rows, bk, heads, head_dim)):
            ctx_out[i, :, h * head_dim:(h + 1) * head_dim] = val

        @pl.when(n >= 1)
        def _():
            ctx_send(i, block).start()

    ctx[t] = ctx_out[0]
    res[...] = rin[...].astype(F32)
    get_o.from_z((4, 5))
    get_o.from_mate(range(13))
    nc = 512

    @pl.loop(0, n_tp)
    def _(n):
        dev = block_of(n + jnp.where(n < 4, 0, jnp.where(n < 6, 2, -2)))

        @pl.when(n >= 1)
        def _():
            pltpu.make_async_copy(ctx_out.at[0], ctx.at[dev], cr.at[dev]).wait()
        rows_o = pl.ds(pl.multiple_of(dev * cols, cols), cols)

        @pl.loop(0, width // nc)
        def _(k):
            at = pl.ds(pl.multiple_of(k * nc, nc), nc)
            res[:, at] = res[:, at] + jnp.dot(ctx[dev], wo[rows_o, at], preferred_element_type=F32)

            @pl.when(n == n_tp - 1)
            def _():
                pltpu.make_async_copy(res.at[:, at], out_hbm.at[:, at], es.at[k]).start()

    get_q.finish()
    get_o.finish()
    for copy in sends + hand_on:
        copy.wait_send()
    for i in range(1, n_tp):
        q_send(jnp.int32(i)).wait_send()
        ctx_send(i, mate).wait_send()
    for k in range(width // nc):
        at = pl.ds(k * nc, nc)
        pltpu.make_async_copy(res.at[:, at], out_hbm.at[:, at], es.at[k]).wait()


def attention(layer, resid, gain, far, near, w_q, w_kv, w_o, n_tp, bk=1024):
    rows, width = resid.shape
    cols, head_dim = w_o.shape[1], w_q.shape[2]
    heads = cols // head_dim
    n_kv = w_kv.shape[1] // (2 * width)
    seq = rows * n_tp
    vmem = pl.BlockSpec(memory_space=pltpu.VMEM)
    anywhere = pl.BlockSpec(memory_space=pl.ANY)
    dma = pltpu.SemaphoreType.DMA
    return pl.pallas_call(
        functools.partial(attn_kernel, layer, n_tp, n_kv, heads, head_dim, bk),
        out_shape=jax.ShapeDtypeStruct((rows, width), F32),
        in_specs=[anywhere, vmem, vmem, vmem, anywhere, anywhere, anywhere],
        out_specs=anywhere,
        scratch_shapes=[
            pltpu.VMEM((rows, width), BF16),
            pltpu.VMEM((rows, width), resid.dtype),
            pltpu.VMEM(w_q.shape[1:], BF16),
            pltpu.VMEM(w_kv.shape[1:], BF16),
            pltpu.VMEM((256 * max(heads, 2 * n_kv), head_dim), F32),
            pltpu.VMEM((width, 2 * n_kv * head_dim), BF16),
            pltpu.VMEM((n_tp * width, cols), BF16),
            pltpu.VMEM((2, rows, head_dim), F32),
            pltpu.VMEM((n_kv, rows, 2 * head_dim), BF16),
            pltpu.VMEM((n_tp, rows, cols), BF16),
            pltpu.VMEM((seq, cols + 2 * head_dim), BF16),
            pltpu.VMEM((n_tp * cols, width), BF16),
            pltpu.VMEM((n_tp, rows, cols), BF16),
            pltpu.VMEM((n_tp, rows, cols), BF16),
            pltpu.VMEM((rows, width), F32),
            dma((4,)), dma((3,)), dma((3,)), dma((4,)), dma((4,)), dma((n_tp,)), dma((n_tp,)), dma((n_tp,)), dma((n_tp,)), dma((4,)),
        ] + weight_sems() + weight_sems(),
        compiler_params=pltpu.CompilerParams(collective_id=1 + layer, has_side_effects=True, vmem_limit_bytes=VMEM_MAX),
        cost_estimate=pl.CostEstimate(flops=2 * seq * seq * cols, bytes_accessed=4 * seq * cols, transcendentals=seq * seq),
        name="attention" + str(layer),
    )(resid, gain, far, near, w_q, w_kv, w_o)


def mlp_kernel(layer, r_hbm, gain_ref, wg_hbm, wu_hbm, wd_hbm, out_hbm,
               wg, wu, wd, xbuf, prec, recv, acc, stash, act,
               lsem, sx, sy, ag, fs, fr, ps, pr, rr, ss):
    _, _, partners = coords()
    mate, dev_x, dev_y = partners
    rows, width = acc.shape
    half = rows // 2
    hid = act.shape[1]
    h0, h1 = pl.ds(0, half), pl.ds(half, half)
    nb = 64

    load_r = pltpu.make_async_copy(r_hbm, acc, lsem.at[0])
    load_r.start()
    greet(partners)
    loads = [pltpu.make_async_copy(src.at[layer], dst, lsem.at[k + 1]) for k, (src, dst) in enumerate(((wg_hbm, wg), (wu_hbm, wu), (wd_hbm, wd)))]
    load_r.wait()
    for copy in loads:
        copy.start()
    gather = RowGather(xbuf, sx, sy, ag, fs, fr, partners)
    gather.start(lambda k: norm_rows(acc, gain_ref[layer:layer + 1], xbuf.at[0, 0], k * half, half))

    def partial_send(w):
        return rcopy(xbuf.at[w, 1], prec.at[w], ps.at[w], pr.at[w], mate)

    stage = (rcopy(xbuf.at[1, 1, h0], recv.at[0], ss.at[0], rr.at[0], dev_x),
             rcopy(xbuf.at[1, 1, h1], recv.at[1], ss.at[1], rr.at[1], dev_y))
    quarter = half // 2
    cuts = [(k, m, pl.ds(m * quarter, quarter), pl.ds(k * half + m * quarter, quarter)) for m in range(2) for k in range(2)]
    to_first, to_second = (dev_x, dev_y), (dev_y, dev_x)
    stage_two = [rcopy(xbuf.at[2, 1, to], recv.at[2 + k, at], ss.at[2 + k + 2 * m], rr.at[2 + k + 2 * m], to_first[k]) for k, m, at, to in cuts]
    stage_three = [rcopy(xbuf.at[3, 1, to], recv.at[4 + k, at], ss.at[6 + k + 2 * m], rr.at[6 + k + 2 * m], to_second[k]) for k, m, at, to in cuts]

    for copy in loads:
        copy.wait()
    cut = 768
    nd = 1024

    def gate_up(x_at, at):
        g = lax.dot_general(x_at[...], wg[at, :], (((1,), (1,)), ((), ())), preferred_element_type=F32)
        u = lax.dot_general(x_at[...], wu[at, :], (((1,), (1,)), ((), ())), preferred_element_type=F32)
        act[:, at] = (g * jax.nn.sigmoid(g) * u).astype(BF16)

    @pl.loop(0, 8)
    def _(s):
        w = lax.div(s, 2)
        rc = 1 - lax.rem(s, 2)

        @pl.when(rc == 1)
        def _():
            gather.forward(w).wait_recv()
        x_at = xbuf.at[w, rc]
        gate_up(x_at, pl.ds(0, cut))
        gate_up(x_at, pl.ds(cut, hid - cut))

        @pl.when(rc == 0)
        def _():
            @pl.when(w < 3)
            def _():
                gather.arrive(w + 1)
            partial_send(w).wait()

        @pl.loop(0, width // nd)
        def _(n):
            at = pl.ds(pl.multiple_of(n * nd, nd), nd)
            val = jnp.dot(act[...], wd[:, at], preferred_element_type=F32)

            @pl.when(rc == 1)
            def _():
                xbuf[w, 1, :, at] = val.astype(BF16)

            @pl.when(rc == 0)
            def _():
                total = val + prec[w, :, at].astype(F32)

                @pl.when(w == 0)
                def _():
                    acc[:, at] = acc[:, at] + total

                @pl.when(w == 3)
                def _():
                    stash[:, at] = total

                @pl.when((w == 1) | (w == 2))
                def _():
                    xbuf[w, 1, :, at] = total.astype(BF16)

        @pl.when(rc == 1)
        def _():
            partial_send(w).start()

        @pl.when(s == 3)
        def _():
            stage[0].start()
            stage[1].start()

        @pl.when(s == 5)
        def _():
            for copy in stage_two:
                copy.start()

    def rows_from(first, count):
        def each(fn):
            @pl.loop(0, count // nb)
            def _(b):
                fn(pl.multiple_of(b * nb, nb), pl.ds(pl.multiple_of(first + b * nb, nb), nb))
        return each

    for k in range(2):
        stage[k].wait_recv()

        @rows_from(k * half, half)
        def _(at, to):
            acc[to, :] = acc[to, :] + recv[k, pl.ds(at, nb), :].astype(F32)
    for copy, send, (k, m, _, _) in zip(stage_two, stage_three, cuts):
        copy.wait_recv()

        @rows_from(k * half + m * quarter, quarter)
        def _(at, to):
            xbuf[3, 1, to, :] = (stash[to, :] + recv[2 + k, pl.ds(m * quarter + at, nb), :].astype(F32)).astype(BF16)
        send.start()
    gather.finish()
    narrow = out_hbm.dtype == BF16
    final = xbuf.at[0, 0] if narrow else acc
    outs = []
    for copy, (k, m, _, out_at) in zip(stage_three, cuts):
        copy.wait_recv()

        @rows_from(k * half + m * quarter, quarter)
        def _(at, to):
            final[to, :] = (acc[to, :] + recv[4 + k, pl.ds(m * quarter + at, nb), :].astype(F32)).astype(final.dtype)
        outs.append(pltpu.make_async_copy(final.at[out_at], out_hbm.at[out_at], lsem.at[k + 2 * m]))
        outs[-1].start()
    for copy in list(stage) + stage_two + stage_three:
        copy.wait_send()
    for copy in outs:
        copy.wait()


def mlp(layer, resid, gain, w_gate, w_up, w_down, out_dtype):
    rows, width = resid.shape
    hid = w_gate.shape[1]
    half = rows // 2
    any_spec = pl.BlockSpec(memory_space=pl.ANY)
    dma = pltpu.SemaphoreType.DMA
    return pl.pallas_call(
        functools.partial(mlp_kernel, layer),
        out_shape=jax.ShapeDtypeStruct((rows, width), out_dtype),
        in_specs=[any_spec, pl.BlockSpec(memory_space=pltpu.VMEM), any_spec, any_spec, any_spec],
        out_specs=any_spec,
        scratch_shapes=[
            pltpu.VMEM((hid, width), BF16),
            pltpu.VMEM((hid, width), BF16),
            pltpu.VMEM((hid, width), BF16),
            pltpu.VMEM((4, 2, rows, width), BF16),
            pltpu.VMEM((4, rows, width), BF16),
            pltpu.VMEM((6, half, width), BF16),
            pltpu.VMEM((rows, width), F32),
            pltpu.VMEM((rows, width), F32),
            pltpu.VMEM((rows, hid), BF16),
            dma((4,)),
        ] + gather_sems() + [dma((4,)), dma((4,)), dma((10,)), dma((10,))],
        compiler_params=pltpu.CompilerParams(collective_id=5 + layer, has_side_effects=True, vmem_limit_bytes=VMEM_MAX),
        cost_estimate=pl.CostEstimate(flops=6 * 8 * rows * width * hid, bytes_accessed=6 * width * hid, transcendentals=8 * rows * hid),
        name="mlp" + str(layer),
    )(resid, gain, w_gate, w_up, w_down)


def solution(mesh):
    n_tp = mesh.shape['tp']
    tok_spec = P('dp', 'tp', None)
    in_specs = (tok_spec, P(), P(None, None, 'tp', None), P(), P(None, 'tp', None, None), P(), P(None, None, 'tp'), P(None, None, 'tp'), P(None, 'tp', None))

    def body(hidden, norm_attn, w_q, w_kv, w_o, norm_mlp, w_gate, w_up, w_down):
        n_layers, width, heads, head_dim = w_q.shape
        n_kv = w_kv.shape[3]
        rows = hidden.shape[1]
        far, near = rope_tables(rows * n_tp, rows // 2, head_dim)
        w_q = w_q.reshape(n_layers, width * heads, head_dim)
        w_kv = w_kv.reshape(n_layers, width * 2 * n_kv, head_dim)
        w_o = w_o.reshape(n_layers, heads * head_dim, width)
        w_gate = jnp.swapaxes(w_gate, 1, 2)
        w_up = jnp.swapaxes(w_up, 1, 2)
        resid = hidden[0]
        for layer in range(n_layers):
            resid = attention(layer, resid, norm_attn, far, near, w_q, w_kv, w_o, n_tp)
            resid = mlp(layer, resid, norm_mlp, w_gate, w_up, w_down, BF16 if layer == n_layers - 1 else F32)
        return resid[None]

    return jax.shard_map(body, mesh=mesh, in_specs=in_specs, out_specs=tok_spec, check_vma=False)
```
